32 devices in a mesh: dp: 4 (over z), w: 2 (over y), h: 4 (over x, core).
Axes of the slice: x: 2, y: 2, z: 4, core: 2. Of those that a mesh axis runs over, the one named last changes fastest.
Arguments:
- field: float32 [12, 64, 256, 512], P('dp', None, 'h', 'w')
- target: float32 [12, 64, 256, 512], P('dp', None, 'h', 'w')
- lat_weight: float32 [256], P('h')
- leg_fwd: float32 [128, 128, 256], P('w', None, 'h')
- leg_inv: float32 [128, 128, 256], P('w', None, 'h')
- spec_w: float32 [2, 128, 64, 64], replicated
- w_in: bfloat16 [64, 128], replicated
- w_out: bfloat16 [128, 64], replicated
Outputs:
- output 1: float32 [], replicated
- output 2: float32 [12, 64, 256, 512], P('dp', None, 'h', 'w')
- output 3: float32 [2, 128, 64, 64], P(None, 'h')
- output 4: float32 [64, 128], replicated
- output 5: float32 [128, 64], replicated
All inputs are finite; a program needn't handle non-finite values.
Results may differ from the reference program's by a relative error of at most 0.00126581.
Values sent between devices are 32-bit elements.
A program may use at most 1 GiB of HBM per device.

```python
import functools
import jax
import jax.numpy as jnp
from jax import lax

BATCH = 12
CHANNELS = 64
NLAT = 256
NLON = 512
LMAX = 128
NORM_EPS = 1e-5
TOTAL = BATCH * CHANNELS * NLAT * NLON


def setup_inputs(seed: int = 0) -> dict:
    keys = jax.random.split(jax.random.key(seed), 12)
    lat_angle = (jnp.arange(NLAT, dtype=jnp.float32) + 0.5) * (jnp.pi / NLAT) - 0.5 * jnp.pi
    lon_angle = jnp.arange(NLON, dtype=jnp.float32) * (2.0 * jnp.pi / NLON)
    grid_shape = (BATCH, CHANNELS, NLAT, NLON)
    chan_mean = jax.random.normal(keys[0], (1, CHANNELS, 1, 1))
    chan_scale = 0.5 + jax.random.uniform(keys[1], (1, CHANNELS, 1, 1))
    wave_amp = jax.random.normal(keys[2], (BATCH, CHANNELS, 1, 1))
    wave_phase = 2.0 * jnp.pi * jax.random.uniform(keys[3], (BATCH, CHANNELS, 1, 1))
    wave = wave_amp * jnp.sin(2.0 * lat_angle)[:, None] * jnp.cos(lon_angle + wave_phase)
    field = chan_mean + chan_scale * (jax.random.normal(keys[4], grid_shape) + wave)
    target = chan_mean + 0.7 * jax.random.normal(keys[5], grid_shape)
    lat_weight = jnp.cos(lat_angle) * (0.5 + jax.random.uniform(keys[6], (NLAT,)))
    degrees = jnp.arange(LMAX)
    tri_mask = (degrees[None, :, None] >= degrees[:, None, None]).astype(jnp.float32)
    leg_fwd = jax.random.normal(keys[7], (LMAX, LMAX, NLAT)) * tri_mask * (NLAT ** -0.5)
    leg_inv = jax.random.normal(keys[8], (LMAX, LMAX, NLAT)) * tri_mask * ((2.0 / LMAX) ** 0.5)
    spec_w = jax.random.normal(keys[9], (2, LMAX, CHANNELS, CHANNELS)) * ((2.0 * CHANNELS) ** -0.5)
    w_in = jax.random.normal(keys[10], (CHANNELS, 2 * CHANNELS)) * (CHANNELS ** -0.5)
    w_out = jax.random.normal(keys[11], (2 * CHANNELS, CHANNELS)) * ((2.0 * CHANNELS) ** -0.5)
    return {"field": field.astype(jnp.float32), "target": target.astype(jnp.float32), "lat_weight": lat_weight.astype(jnp.float32), "leg_fwd": leg_fwd.astype(jnp.float32), "leg_inv": leg_inv.astype(jnp.float32), "spec_w": spec_w.astype(jnp.float32), "w_in": w_in.astype(jnp.bfloat16), "w_out": w_out.astype(jnp.bfloat16)}


def as_bf16_value(values):
    return values + lax.stop_gradient(values.astype(jnp.bfloat16).astype(jnp.float32) - values)


def sample_energy(sample, lat_weight, leg_fwd, leg_inv, spec_w, w_in, w_out):
    field, target = sample
    chan_mean = jnp.mean(field, axis=(1, 2), keepdims=True)
    centred = field - chan_mean
    variance = jnp.mean(centred * centred, axis=(1, 2), keepdims=True)
    normed = centred * lax.rsqrt(variance + NORM_EPS)
    lon_spec = jnp.fft.rfft(normed, axis=2, norm="ortho")[:, :, :LMAX]
    coef_re = jnp.einsum("mlt,ctm->clm", leg_fwd, lon_spec.real)
    coef_im = jnp.einsum("mlt,ctm->clm", leg_fwd, lon_spec.imag)
    mix_re = jnp.einsum("ilm,lio->olm", coef_re, spec_w[0]) - jnp.einsum("ilm,lio->olm", coef_im, spec_w[1])
    mix_im = jnp.einsum("ilm,lio->olm", coef_re, spec_w[1]) + jnp.einsum("ilm,lio->olm", coef_im, spec_w[0])
    back_re = jnp.einsum("mlt,clm->ctm", leg_inv, mix_re)
    back_im = jnp.einsum("mlt,clm->ctm", leg_inv, mix_im)
    back_spec = jnp.pad(lax.complex(back_re, back_im), ((0, 0), (0, 0), (0, NLON // 2 + 1 - LMAX)))
    y_grid = jnp.fft.irfft(back_spec, n=NLON, axis=2, norm="ortho")
    hidden = jnp.einsum("ctp,cf->ftp", as_bf16_value(y_grid), w_in)
    activation = as_bf16_value(jax.nn.gelu(hidden))
    mlp_out = jnp.einsum("ftp,fc->ctp", activation, w_out)
    residual = field + y_grid + mlp_out - target
    return 0.5 * jnp.sum(lat_weight[:, None] * residual * residual)


def total_energy(field, spec_w, w_in, w_out, target, lat_weight, leg_fwd, leg_inv):
    body = jax.checkpoint(functools.partial(sample_energy, lat_weight=lat_weight, leg_fwd=leg_fwd, leg_inv=leg_inv, spec_w=spec_w, w_in=w_in, w_out=w_out))
    return jnp.sum(lax.map(body, (field, target)))


def reference(field, target, lat_weight, leg_fwd, leg_inv, spec_w, w_in, w_out):
    energy_fn = functools.partial(total_energy, target=target, lat_weight=lat_weight, leg_fwd=leg_fwd, leg_inv=leg_inv)
    energy, pullback = jax.vjp(energy_fn, field, spec_w, w_in.astype(jnp.float32), w_out.astype(jnp.float32))
    grad_field, grad_spec, grad_w_in, grad_w_out = pullback(jnp.ones_like(energy))
    loss = 2.0 * energy / TOTAL
    return (loss, grad_field, grad_spec, grad_w_in, grad_w_out)
```

```python
import math
import numpy as np
import jax
import jax.numpy as jnp
from jax import lax
from jax.experimental import pallas as pl
from jax.experimental.pallas import tpu as pltpu
from jax.sharding import PartitionSpec as P

NORM_EPS = 1e-5
HI = lax.Precision.HIGHEST
F32 = jnp.float32
BF16 = jnp.bfloat16
MESH = pl.DeviceIdType.MESH
GELU_A = math.sqrt(2.0 / math.pi)
GELU_B = 0.044715

NB, CH, NT, NN = 3, 64, 64, 256
NM, NL = 128, 128
LON, LAT, BATCH = 512, 256, 12
POINTS = LON * LAT
TOTAL = POINTS * BATCH * CH
LANES = NB * 2 * CH
SUB, LN = 8, 128
T8 = NT // SUB
GROUPS = NM // SUB
PLANE = 8
H_OF_PAIR = (0, 0, 3, 3, 1, 1, 2, 2)
BLOCK = SUB * SUB
PLACES = GROUPS + 1
DATA = PLACES * BLOCK
STAT = DATA
GRAD = DATA + SUB
ROWS = GRAD + SUB
SPARE = BLOCK
STEP = 3 * BLOCK
COUNT = 6
NN_DIMS, NT_DIMS, TN_DIMS = ((1,), (0,)), ((1,), (1,)), ((0,), (0,))
SUM_STEPS = ((0, 2), (2, 5), (5, 8), (8, 11), (11, 14), (14, 16))
GATHER_STEPS = ((13, 16), (10, 13), (7, 10), (4, 7), (1, 4), (0, 1))

SMEM = pl.BlockSpec(memory_space=pltpu.SMEM)
VMEM = pl.BlockSpec(memory_space=pltpu.VMEM)
ANY = pl.BlockSpec(memory_space=pl.ANY)


def dot(a, b, dims=NN_DIMS):
    return lax.dot_general(a, b, (dims, ((), ())), precision=HI, preferred_element_type=F32)


def mxu(a, b, dims=NN_DIMS):
    return lax.dot_general(a, b, (dims, ((), ())), preferred_element_type=F32)


def call(kernel, outs, scratch=(), cid=None, **kw):
    extra = {} if cid is None else {"collective_id": cid, "has_side_effects": True}
    return pl.pallas_call(
        kernel,
        out_shape=tuple(jax.ShapeDtypeStruct(s, F32) for s in outs),
        scratch_shapes=list(scratch),
        compiler_params=pltpu.CompilerParams(vmem_limit_bytes=62 << 20, **extra),
        **kw,
    )


def vmem(*shape, dtype=F32):
    return pltpu.VMEM(shape, dtype)


def dma_sems(*shape):
    return pltpu.SemaphoreType.DMA(shape)


def rows(lo, hi):
    return pl.ds(lo, hi - lo)


def dft_matrix():
    theta = 2.0 * np.pi * ((np.arange(NN)[:, None] * np.arange(NM)[None, :]) % LON) / LON
    return (np.concatenate([np.cos(theta), -np.sin(theta)], axis=1) / math.sqrt(LON)).astype(np.float32)


def signed(base, half, weight):
    m = lax.broadcasted_iota(jnp.int32, base.shape, 1) % NM
    out = jnp.where((m % 2) * half == 1, -base, base)
    return jnp.where(m == 0, out, weight * out) if weight > 1 else out


def to_orders(lines, ft):
    z = dot(lines, ft).reshape(SUB, CH, NN)
    z = jnp.concatenate([z[:, :, :NM], z[:, :, NM:]], axis=1)
    return jnp.swapaxes(jnp.swapaxes(z, 1, 2), 0, 1)


def to_grid(orders, ft):
    u = jnp.swapaxes(jnp.swapaxes(orders, 0, 1), 1, 2)
    u = jnp.concatenate([u[:, :CH, :], u[:, CH:, :]], axis=2).reshape(SUB * CH, NN)
    return dot(u, ft)


def place_of_block(j):
    k = min(j, GROUPS - 1 - j)
    return H_OF_PAIR[k] // 2, H_OF_PAIR[k] % 2, k % 2


def sum_position(j, g):
    k = min(j, GROUPS - 1 - j)
    return 2 * g + 1 if j < SUB else jnp.where(g <= k, 2 * g, k + 1 + g)


def chunk(i, share):
    lo = i * STEP
    hi = lo + STEP if i < COUNT - 1 else ROWS
    return lo, lo + (hi - lo) * share // BLOCK * SUB, hi


class Place:
    def __init__(self):
        self.h, self.y, self.z = lax.axis_index("h"), lax.axis_index("w"), lax.axis_index("dp")
        self.x, self.c = self.h // 2, self.h % 2
        self.slot = 2 * self.h + self.y
        self.low = self.h < 2
        self.pair = jnp.where(self.low, 4 * self.h, 14 - 4 * self.h) + self.y
        self.sibling = {"h": 2 * self.x + 1 - self.c}
        self.xn = {"h": 2 * (1 - self.x) + self.c}
        self.yn = {"w": 1 - self.y}

    def plane(self, r):
        s = (self.slot + r) % PLANE
        return {"h": s // 2, "w": s % 2}

    def greet(self, others):
        barrier = pltpu.get_barrier_semaphore()
        for other in others:
            pl.semaphore_signal(barrier, inc=1, device_id=other, device_id_type=MESH)
        pl.semaphore_wait(barrier, len(others))


def send(src, dst, sems, i, to):
    return pltpu.make_async_remote_copy(
        src_ref=src, dst_ref=dst, send_sem=sems.at[0, i], recv_sem=sems.at[1, i], device_id=to, device_id_type=MESH
    )


CB = 16
PIECES = CH // CB
HALF_TABLE = (SUB, SUB, NT, NL)


def near_far(k):
    return pl.ds(pl.multiple_of(SUB * k, SUB), SUB), pl.ds(pl.multiple_of(SUB * (GROUPS - 1 - k), SUB), SUB)


def front_kernel(x_hbm, p_hbm, w_hbm, base_ref, z_hbm, p_peer, mu_ref, inv_ref, c0_ref, kern_ref,
                 xbuf, wbuf, p0, cols, pay, sbuf, zbuf, ftbuf, turned, own, s_x, s_w, s_z, s_p, s_st):
    place = Place()
    near, far = near_far(place.pair)

    def load_x(n):
        b, part = n // PIECES, pl.ds(n % PIECES * CB, CB)
        return pltpu.make_async_copy(x_hbm.at[b, part], xbuf.at[b, part], s_x.at[n])

    def load_w(i):
        return pltpu.make_async_copy(w_hbm.at[i], wbuf.at[i], s_w.at[i])

    def load_p0():
        return pltpu.make_async_copy(p_hbm.at[0, 0], p0, s_w.at[2])

    def give_p(g):
        return send(p_hbm.at[g], p_peer.at[g], s_p, g, place.yn)

    load_p0().start()
    for n in range(NB * PIECES):
        load_x(n).start()
    for i in range(2):
        load_w(i).start()
    others = range(1, PLANE)
    place.greet([place.plane(r) for r in others])

    @pl.loop(0, SUB)
    def _(g):
        give_p(g).start()

    cols[...] = jnp.zeros_like(cols)
    for n in range(NB * PIECES):
        load_x(n).wait()
        v = xbuf[n // PIECES, n % PIECES * CB:(n % PIECES + 1) * CB]
        mean = jnp.sum(jnp.sum(v, axis=1, keepdims=True), axis=2, keepdims=True) / (NT * NN)
        diff = v - mean
        m2 = jnp.sum(jnp.sum(diff * diff, axis=1, keepdims=True), axis=2, keepdims=True)
        lane = lax.broadcasted_iota(jnp.int32, (CB, 1, LN), 2)
        cols[pl.ds(n * CB, CB)] = jnp.where(lane < CH, mean, m2).reshape(CB, LN)
    wide = cols[...].T
    load_p0().wait()
    p1 = jnp.where(place.y == 0, jnp.sum(p0[...], axis=0, keepdims=True), 0.0)
    pay[...] = jnp.concatenate([
        wide[:1], wide[CH:CH + 1], jnp.concatenate([p1, p1], axis=1), jnp.zeros((SUB - 3, NN), F32)
    ], axis=0)

    def give_stats(r):
        return send(pay, sbuf.at[place.slot], s_st, r, place.plane(r))

    for r in others:
        give_stats(r).start()
    sbuf[place.slot] = pay[...]
    ftbuf[...] = signed(base_ref[...], place.y, 1)

    for i in range(2):
        load_w(i).wait()

    @pl.loop(0, CH)
    def _(i):
        turned[...] = jnp.concatenate([wbuf[0, i], wbuf[1, i]], axis=0).T
        own[i, :SUB] = turned[near]
        own[i, SUB:] = turned[far]

    top = jnp.swapaxes(own[...], 0, 1)
    kern_ref[:, :CH] = top
    kern_ref[:, CH:] = jnp.concatenate([-top[:, :, CH:], top[:, :, :CH]], axis=2)

    for r in others:
        give_stats(r).wait_recv()
    means, m2s, p1s = (jnp.concatenate([sbuf[s, n:n + 1] for s in range(PLANE)], axis=0) for n in range(3))
    mu = jnp.sum(means, axis=0, keepdims=True) / PLANE
    dev = means - mu
    var = (jnp.sum(m2s, axis=0, keepdims=True) + (NT * NN) * jnp.sum(dev * dev, axis=0, keepdims=True)) / POINTS
    c0 = math.sqrt(LON) * jnp.sum(p1s, axis=0, keepdims=True)
    mu_ref[...], inv_ref[...], turned[...] = (
        jnp.broadcast_to(v, (LN, NN)).T[:n] for v, n in ((mu, NB * CH), (lax.rsqrt(var + NORM_EPS), NB * CH), (c0, NL))
    )
    c0_ref[:SUB] = turned[near]
    c0_ref[SUB:] = turned[far]

    def store_z(n):
        t = pl.multiple_of(n % T8 * SUB, SUB)
        lanes = pl.multiple_of(n // T8 * LN, LN)
        return pltpu.make_async_copy(zbuf.at[n % 2], z_hbm.at[:, pl.ds(t, SUB), pl.ds(lanes, LN)], s_z.at[n % 2])

    @pl.loop(0, NB * T8)
    def _(n):
        @pl.when(n >= 2)
        def _():
            store_z(n - 2).wait()

        b = n // T8
        xt = jnp.swapaxes(xbuf[b, :, pl.ds(pl.multiple_of(n % T8 * SUB, SUB), SUB), :], 0, 1)
        chans = pl.ds(pl.multiple_of(b * CH, CH), CH)
        xn = (xt - mu_ref[chans, :1]) * inv_ref[chans, :1]
        zbuf[n % 2] = to_orders(xn.reshape(SUB * CH, NN), ftbuf[...])
        store_z(n).start()

    for n in range(2):
        store_z(NB * T8 - 2 + n).wait()
    for r in others:
        give_stats(r).wait_send()

    @pl.loop(0, SUB)
    def _(g):
        give_p(g).wait()


def front(x, p_own, spec_w, base, cid):
    return call(
        front_kernel,
        [(NM, NT, LANES), HALF_TABLE, (NB * CH, LN), (NB * CH, LN), (2 * SUB, LN), (2 * SUB, LN, LN)],
        [
            vmem(NB, CH, NT, NN), vmem(2, CH, CH, NL), vmem(NT, NL), vmem(NN, LN), vmem(SUB, NN), vmem(PLANE, SUB, NN),
            vmem(2, NM, SUB, LN), vmem(NN, NN), vmem(NL, LN), vmem(CH, 2 * SUB, LN),
            dma_sems(NB * PIECES), dma_sems(3), dma_sems(2), dma_sems(2, SUB), dma_sems(2, PLANE),
        ],
        cid=cid,
        in_specs=[ANY, ANY, ANY, VMEM],
        out_specs=(ANY, ANY, VMEM, VMEM, VMEM, VMEM),
        name="front",
    )(x, p_own, spec_w, base)


def table_loader(own, peer, tbuf, sems, y):
    def copy(src, g):
        return pltpu.make_async_copy(src.at[g % SUB], tbuf.at[g], sems.at[g])

    def start(g):
        @pl.when(g // SUB == y)
        def _():
            copy(own, g).start()

        @pl.when(g // SUB != y)
        def _():
            copy(peer, g).start()

    def wait(g):
        copy(own, g).wait()

    return start, wait


def quarters(lo, hi):
    return [(max(lo, 4 * k), min(hi, 4 * k + 4), k) for k in range(4) if max(lo, 4 * k) < min(hi, 4 * k + 4)]


def analyze_kernel(share, with_q, *refs):
    if with_q:
        t_own, t_peer, z_hbm, ext_ref, q_own, out_ref, q_peer, *rest = refs
    else:
        t_own, t_peer, z_hbm, ext_ref, out_ref, *rest = refs
    tbuf, zbuf, part, sib, rx, ry, fx, fy, s_t, s_z, s_q, s_sib, s_x, s_y, s_fx, s_fy = rest
    p = Place()
    x, c, y = p.x, p.c, p.y
    start_t, wait_t = table_loader(t_own, t_peer, tbuf, s_t, y)

    def load_z(g):
        return pltpu.make_async_copy(z_hbm.at[g], zbuf.at[g], s_z.at[g])

    @pl.loop(0, GROUPS)
    def _(g):
        start_t(g)
        load_z(g).start()

    p.greet([p.sibling, p.xn, p.yn])
    for d in range(PLANE):
        part[d // 4, d // 2 % 2, d % 2, STAT:GRAD] = ext_ref[SUB * d:SUB * (d + 1)]
        part[d // 4, d // 2 % 2, d % 2, GRAD:ROWS] = jnp.zeros((SUB, LANES), F32)

    def give_q(g):
        return send(q_own.at[g], q_peer.at[g], s_q, g, p.yn)

    def compute(lo, hi, k):
        @pl.loop(lo, hi)
        def _(g):
            wait_t(g)
            load_z(g).wait()
            for m in range(SUB):
                r = dot(tbuf[g, m].T[4 * SUB * k:], zbuf[g, m])
                for n in range(GROUPS - 4 * k):
                    j = 4 * k + n
                    row = sum_position(j, g) * BLOCK + SUB * m
                    if n < 4:
                        row = jnp.where(j >= g, row, ROWS)
                    xj, cj, yj = place_of_block(j)
                    part[xj, cj, yj, pl.ds(pl.multiple_of(row, SUB), SUB), :] = r[SUB * n:SUB * (n + 1)]

    def to_sibling(i):
        lo, _, hi = chunk(i, share)
        return send(part.at[:, 1 - c, :, rows(lo, hi)], sib.at[:, :, rows(lo, hi)], s_sib, i, p.sibling)

    def to_x(i):
        lo, mid, _ = chunk(i, share)
        return send(part.at[1 - x, c, :, rows(lo, mid)], rx.at[:, rows(lo, mid)], s_x, i, p.xn)

    def to_y(i):
        _, mid, hi = chunk(i, share)
        return send(part.at[:, c, 1 - y, rows(mid, hi)], ry.at[:, rows(mid, hi)], s_y, i, p.yn)

    def forward_y(i):
        lo, mid, _ = chunk(i, share)
        return send(part.at[x, c, 1 - y, rows(lo, mid)], fy.at[rows(lo, mid)], s_fy, i, p.yn)

    def forward_x(i):
        _, mid, hi = chunk(i, share)
        return send(part.at[1 - x, c, y, rows(mid, hi)], fx.at[rows(mid, hi)], s_fx, i, p.xn)

    def chip_sum(i):
        lo, _, hi = chunk(i, share)
        to_sibling(i).wait_recv()
        for a in range(2):
            for b in range(2):
                part[a, c, b, rows(lo, hi)] += sib[a, b, rows(lo, hi)]
        to_x(i).start()
        to_y(i).start()
        if with_q:
            give_q(i).start()

    def half_sum(i):
        lo, mid, hi = chunk(i, share)
        to_x(i).wait_recv()
        part[x, c, 1 - y, rows(lo, mid)] += rx[1 - y, rows(lo, mid)]
        forward_y(i).start()
        to_y(i).wait_recv()
        part[1 - x, c, y, rows(mid, hi)] += ry[1 - x, rows(mid, hi)]
        forward_x(i).start()
        out_ref[rows(lo, mid)] = part[x, c, y, rows(lo, mid)] + rx[y, rows(lo, mid)]
        out_ref[rows(mid, hi)] = part[x, c, y, rows(mid, hi)] + ry[x, rows(mid, hi)]

    def last_sum(i):
        lo, mid, hi = chunk(i, share)
        forward_y(i).wait_recv()
        out_ref[rows(lo, mid)] += fy[rows(lo, mid)]
        forward_x(i).wait_recv()
        out_ref[rows(mid, hi)] += fx[rows(mid, hi)]

    if with_q:
        for g in (COUNT, COUNT + 1):
            give_q(g).start()
    for i in range(COUNT):
        for step in quarters(*SUM_STEPS[i]):
            compute(*step)
        to_sibling(i).start()
        if i > 0:
            chip_sum(i - 1)
    chip_sum(COUNT - 1)
    for i in range(COUNT + 2):
        if i < COUNT:
            half_sum(i)
        if i > 1:
            last_sum(i - 2)
    for i in range(COUNT):
        for copy in (to_sibling, to_x, to_y, forward_x, forward_y):
            copy(i).wait_send()
    if with_q:
        for g in range(SUB):
            give_q(g).wait()


def analyze(table, z, ext, cid, q_own=None):
    with_q = q_own is not None
    share = 7 if with_q else 4
    half = vmem(ROWS, LANES)
    pair = vmem(2, ROWS, LANES)
    outs = call(
        lambda *refs: analyze_kernel(share, with_q, *refs),
        [(ROWS, LANES)] + [HALF_TABLE] * with_q,
        [
            vmem(GROUPS, SUB, NT, NL), vmem(GROUPS, SUB, NT, LANES), vmem(2, 2, 2, ROWS + SPARE, LANES), vmem(2, 2, ROWS, LANES),
            pair, pair, half, half,
            dma_sems(GROUPS), dma_sems(GROUPS), dma_sems(2, SUB),
        ] + [dma_sems(2, COUNT)] * 5,
        cid=cid,
        in_specs=[ANY, ANY, ANY, VMEM] + [ANY] * with_q,
        out_specs=(VMEM,) + (ANY,) * with_q,
        name=f"analyze_{cid}",
    )(*table, z.reshape(GROUPS, SUB, NT, LANES), ext, *([q_own] * with_q))
    return outs if with_q else outs[0]


def synth_kernel(with_grads, *refs):
    if with_grads:
        t_own, t_peer, own_ref, dk_ref, u_hbm, ext_ref, spec_ref, *rest = refs
        *rest, zin, kin, zg, s_zk, s_zg, s_kin, s_kz = rest
    else:
        t_own, t_peer, own_ref, u_hbm, ext_ref, *rest = refs
    tbuf, ubuf, ball, s_t, s_u, s_sib, s_x, s_y, s_dx, s_dy, s_sx, s_sy, s_sd = rest
    p = Place()
    x, c, y = p.x, p.c, p.y
    start_t, wait_t = table_loader(t_own, t_peer, tbuf, s_t, y)

    def store_u(g):
        return pltpu.make_async_copy(ubuf.at[g], u_hbm.at[g], s_u.at[g])

    @pl.loop(0, GROUPS)
    def _(g):
        start_t(g)

    friends = [p.sibling, p.xn, p.yn]
    if with_grads:
        above = [{"dp": (p.z + r) % 4} for r in range(1, 4)]
        partner = [{"h": 3 - p.h}, {"h": 3 - p.h, "w": 1 - y}]
        friends = friends + above + partner
    p.greet(friends)

    def own_to(i, sems, to):
        lo, _, hi = chunk(i, 4)
        src = own_ref if i < COUNT - 1 else ball.at[x, c, y]
        return send(src.at[rows(lo, hi)], ball.at[x, c, y, rows(lo, hi)], sems, i, to)

    def own_x(i):
        return own_to(i, s_x, p.xn)

    def own_y(i):
        return own_to(i, s_y, p.yn)

    def own_s(i):
        return own_to(i, s_sib, p.sibling)

    def relay(i, a, b, sems, to, lo, hi):
        return send(ball.at[a, c, b, rows(lo, hi)], ball.at[a, c, b, rows(lo, hi)], sems, i, to)

    def diagonal_y(i):
        lo, mid, _ = chunk(i, 4)
        return relay(i, 1 - x, y, s_dy, p.yn, lo, mid)

    def diagonal_x(i):
        _, mid, hi = chunk(i, 4)
        return relay(i, x, 1 - y, s_dx, p.xn, mid, hi)

    def sibling_x(i):
        lo, _, hi = chunk(i, 4)
        return relay(i, 1 - x, y, s_sx, p.sibling, lo, hi)

    def sibling_y(i):
        lo, _, hi = chunk(i, 4)
        return relay(i, x, 1 - y, s_sy, p.sibling, lo, hi)

    def sibling_d(i):
        lo, _, hi = chunk(i, 4)
        return relay(i, 1 - x, 1 - y, s_sd, p.sibling, lo, hi)

    def give(i):
        for copy in (own_x, own_y, own_s):
            copy(i).start()

    def pass_on(i):
        own_x(i).wait_recv()
        diagonal_y(i).start()
        own_y(i).wait_recv()
        diagonal_x(i).start()
        sibling_x(i).start()
        sibling_y(i).start()

    def collect(i):
        diagonal_y(i).wait_recv()
        diagonal_x(i).wait_recv()
        sibling_d(i).start()

    def complete(i):
        for copy in (own_s, sibling_x, sibling_y, sibling_d):
            copy(i).wait_recv()

    def compute(lo, hi, k):
        @pl.loop(0, hi - lo)
        def _(n):
            g = hi - 1 - n
            wait_t(g)
            for m in range(SUB):
                tiles = []
                for n in range(GROUPS - 4 * k):
                    j = 4 * k + n
                    row = (GROUPS - sum_position(j, g)) * BLOCK + SUB * m
                    if n < 4:
                        row = jnp.where(j >= g, row, ROWS)
                    xj, cj, yj = place_of_block(j)
                    tiles.append(ball[xj, cj, yj, pl.ds(pl.multiple_of(row, SUB), SUB), :])
                ubuf[g, m] = dot(tbuf[g, m][:, 4 * SUB * k:], jnp.concatenate(tiles, axis=0))
            store_u(g).start()

    if with_grads:
        quarter = pl.ds(2 * p.z, 2)

        def grads_z(r):
            return send(own_ref.at[GRAD:ROWS], zg.at[r], s_zg, r, above[r])

        def dk_z(r):
            return send(dk_ref.at[:, pl.ds(2 * ((p.z + 1 + r) % 4), 2)], zin.at[r], s_zk, r, above[r])

        stay = jnp.where(p.low, 0, 1)
        kept = jnp.where(p.low, p.pair, GROUPS - 1 - p.pair) % 4
        given = jnp.where(p.low, GROUPS - 1 - p.pair, p.pair) % 4

        def dk_plane(r):
            to = (p.yn, *partner)[r]
            src = kin.at[stay] if r == 0 else kin.at[1 - stay]
            return send(src, spec_ref.at[kept if r == 0 else given, quarter], s_kin, r, to)

        def dk_up(r):
            return send(spec_ref.at[:, quarter], spec_ref.at[:, quarter], s_kz, r, above[r])

        for r in range(3):
            grads_z(r).start()
            dk_z(r).start()

    give(0)
    give(1)
    ball[x, c, y, 0:ROWS] = own_ref[...]
    for d in range(PLANE):
        ball[d // 4, d // 2 % 2, d % 2, ROWS:] = jnp.zeros((SPARE, LANES), F32)
    for i in range(COUNT + 2):
        if i < COUNT:
            pass_on(i)
        if with_grads and i == 1:
            for r in range(3):
                grads_z(r).wait_recv()
                ball[x, c, y, GRAD:ROWS] += zg[r]
        if with_grads and i == 2:
            for r in range(3):
                dk_z(r).wait_recv()
            kin[...] = dk_ref[:, quarter] + zin[0] + zin[1] + zin[2]
            for r in range(3):
                dk_plane(r).start()
            spec_ref[kept, quarter] = kin[stay]
        if with_grads and i == 3:
            for r in range(3):
                dk_plane(r).wait_recv()
            for r in range(3):
                dk_up(r).start()
        if i < COUNT - 2:
            give(i + 2)
        if 0 < i < COUNT + 1:
            collect(i - 1)
        if i > 1:
            complete(i - 2)
            for step in reversed(quarters(*GATHER_STEPS[i - 2])):
                compute(*step)
    for d in range(PLANE):
        ext_ref[d] = ball[d // 4, d // 2 % 2, d % 2, STAT:ROWS]
    for i in range(COUNT):
        for copy in (own_x, own_y, own_s, diagonal_x, diagonal_y, sibling_x, sibling_y, sibling_d):
            copy(i).wait_send()
    if with_grads:
        for r in range(3):
            grads_z(r).wait_send()
            dk_z(r).wait_send()
            dk_plane(r).wait_send()
            dk_up(r).wait()

    @pl.loop(0, GROUPS)
    def _(g):
        store_u(g).wait()


def synth(table, own, cid, dk=None):
    with_grads = dk is not None
    quarter = vmem(2, 2, CH, LN)
    outs = call(
        lambda *refs: synth_kernel(with_grads, *refs),
        [(GROUPS, SUB, NT, LANES), (PLANE, 2 * SUB, LANES)] + [(4, SUB, CH, LN)] * with_grads,
        [
            vmem(GROUPS, SUB, NT, NL), vmem(GROUPS, SUB, NT, LANES), vmem(2, 2, 2, ROWS + SPARE, LANES),
            dma_sems(GROUPS), dma_sems(GROUPS),
        ] + [dma_sems(2, COUNT)] * 8
        + [vmem(3, 2, 2, CH, LN), quarter, vmem(3, SUB, LANES)] * with_grads
        + [dma_sems(2, 3)] * 4 * with_grads,
        cid=cid,
        in_specs=[ANY, ANY, VMEM] + [VMEM] * with_grads,
        out_specs=(ANY, VMEM) + (VMEM,) * with_grads,
        name=f"synth_{cid}",
    )(*table, own, *([dk] * with_grads))
    return (outs[0].reshape(NM, NT, LANES), *outs[1:])


MIX = PLACES * SUB


def by_degree(v):
    t = jnp.swapaxes(v.reshape(MIX, SUB, LANES), 0, 1)
    return jnp.concatenate([t[:, :, LN * b:LN * (b + 1)] for b in range(NB)], axis=1)


def samples(v):
    return [v[MIX * b:MIX * (b + 1)] for b in range(NB)]


def put_degrees(ref, parts):
    t = jnp.stack([jnp.concatenate(samples(r), axis=1) for r in parts])
    t = jnp.swapaxes(t, 0, 1).reshape(DATA, LANES)
    for n in range(PLACES):
        ref[BLOCK * (GROUPS - n):BLOCK * (PLACES - n)] = t[BLOCK * n:BLOCK * (n + 1)]


def near_mask():
    place = lax.broadcasted_iota(jnp.int32, (NB * MIX, LN), 0) % MIX // SUB
    return (place % 2 == 1) & (place < 2 * (Place().pair + 1))


def mix_kernel(a_ref, kern_ref, b_ref):
    a = by_degree(a_ref[:DATA])
    near = near_mask()
    put_degrees(b_ref, [jnp.where(near, dot(a[l], kern_ref[l]), dot(a[l], kern_ref[SUB + l])) for l in range(SUB)])
    b_ref[DATA:] = jnp.zeros((ROWS - DATA, LANES), F32)


def mix(a, kern):
    return call(mix_kernel, [(ROWS, LANES)], in_specs=[VMEM, VMEM], out_specs=(VMEM,), name="mix")(a, kern)[0]


def mixb_kernel(a_ref, db_ref, kern_ref, c0_ref, da_ref, dk_ref):
    a = by_degree(a_ref[:DATA])
    db = by_degree(db_ref[:DATA])
    near = near_mask()
    parts = []
    total = jnp.zeros((NB * MIX, LN), F32)
    s0 = jnp.zeros((1, LANES), F32)
    for l in range(SUB):
        da = jnp.where(near, dot(db[l], kern_ref[l], NT_DIMS), dot(db[l], kern_ref[SUB + l], NT_DIMS))
        parts.append(da)
        total = total + da * a[l]
        near_row, far_row = (jnp.concatenate([v[n:n + 1] for v in samples(da)], axis=1) for n in (SUB, 0))
        s0 = s0 + near_row * c0_ref[l:l + 1, :1] + far_row * c0_ref[SUB + l:SUB + l + 1, :1]
        for i, part in enumerate((jnp.where(near, a[l], 0.0), jnp.where(near, 0.0, a[l]))):
            g = dot(part, db[l], TN_DIMS)
            low = g[CH:]
            dk_ref[i, l] = g[:CH] + jnp.concatenate([low[:, CH:], -low[:, :CH]], axis=1)
    put_degrees(da_ref, parts)
    s1 = jnp.concatenate([jnp.sum(v, axis=0, keepdims=True) for v in samples(total)], axis=1)
    da_ref[STAT:GRAD] = jnp.concatenate([s0, s1, jnp.zeros((SUB - 2, LANES), F32)], axis=0)
    da_ref[GRAD:] = db_ref[STAT:GRAD]


def mixb(a, db, kern, c0):
    outs = [(ROWS, LANES), (2, SUB, CH, LN)]
    return call(mixb_kernel, outs, in_specs=[VMEM] * len("adkc"), out_specs=(VMEM, VMEM), name="mixb")(a, db, kern, c0)


GRID_SPEC = pl.BlockSpec((1, CH, SUB, NN), lambda b, t: (b, 0, t, 0))
LINES_SPEC = pl.BlockSpec((1, SUB, CH, NN), lambda b, t: (b, t, 0, 0))
CHAN_SPEC = pl.BlockSpec((CH, LN), lambda b, t: (b, 0))
ORDER_SPEC = pl.BlockSpec((NM, SUB, LN), lambda b, t: (0, t, b))
WIDE = SUB * NN


def whole(*shape):
    return pl.BlockSpec(shape, lambda b, t: (0,) * len(shape))


def first_step():
    return (pl.program_id(0) == 0) & (pl.program_id(1) == 0)


def mlp_kernel(u_ref, x_ref, tgt_ref, q_ref, base_ref, w1_ref, w2t_ref, dout_ref, dz_ref, grads_ref,
               gt_ref, g_ref, line_ref, yb_ref, h_ref, act_ref, db_ref, dh_ref):
    @pl.when(first_step())
    def _():
        grads_ref[...] = jnp.zeros_like(grads_ref)
        gt_ref[...] = signed(base_ref[...], Place().y, 2)
        g_ref[...] = gt_ref[...].T

    y = to_grid(u_ref[...], g_ref[...]).reshape(SUB, CH, NN)
    r0 = jnp.swapaxes(x_ref[0] - tgt_ref[0], 0, 1)

    def wide(v):
        return jnp.concatenate([v[t] for t in range(SUB)], axis=1)

    line_ref[...] = wide(r0 + y)
    yb_ref[...] = wide(y).astype(BF16)
    h_ref[...] = mxu(w1_ref[...], yb_ref[...], TN_DIMS)
    for t in range(SUB):
        cols = slice(NN * t, NN * (t + 1))
        h = h_ref[:, cols]
        h2 = h * h
        th = jnp.tanh(h * (GELU_A + (GELU_A * GELU_B) * h2))
        cdf = 0.5 + 0.5 * th
        act_ref[:, cols] = (h * cdf).astype(BF16)
        h_ref[:, cols] = cdf + (0.5 * h) * (1.0 - th * th) * (GELU_A + (3.0 * GELU_A * GELU_B) * h2)
    res = line_ref[...] + mxu(w2t_ref[...], act_ref[...])
    first = pl.program_id(1) * SUB
    qw = jnp.concatenate([jnp.full((1, NN), q_ref[first + t], F32) for t in range(SUB)], axis=1)
    d = qw * res
    line_ref[...] = d
    db_ref[...] = d.astype(BF16)
    loss = jnp.sum((d * res).reshape(SUB, SUB, WIDE), axis=0)
    grads_ref[0:SUB, 2 * LN:] += sum(loss[:, LN * i:LN * (i + 1)] for i in range(WIDE // LN))
    for t in range(SUB):
        dout_ref[0, t] = line_ref[:, NN * t:NN * (t + 1)]
    dh_ref[...] = (mxu(w2t_ref[...], db_ref[...], TN_DIMS) * h_ref[...]).astype(BF16)
    grads_ref[:, :LN] += mxu(yb_ref[...], dh_ref[...], NT_DIMS)
    grads_ref[:, LN:2 * LN] += mxu(db_ref[...], act_ref[...], NT_DIMS)
    dy = line_ref[...] + mxu(w1_ref[...], dh_ref[...])
    dys = jnp.concatenate([dy[:, NN * t:NN * (t + 1)] for t in range(SUB)], axis=0)
    dz_ref[...] = to_orders(dys, gt_ref[...])


def mlp(u, x, target, q, base, w1, w2t):
    hid = 2 * CH
    return call(
        mlp_kernel,
        [(NB, NT, CH, NN), (NM, NT, LANES), (CH, LANES)],
        [
            vmem(NN, NN), vmem(NN, NN), vmem(CH, WIDE), vmem(CH, WIDE, dtype=BF16), vmem(hid, WIDE),
            vmem(hid, WIDE, dtype=BF16), vmem(CH, WIDE, dtype=BF16), vmem(hid, WIDE, dtype=BF16),
        ],
        grid=(NB, T8),
        in_specs=[
            ORDER_SPEC, GRID_SPEC, GRID_SPEC, SMEM, whole(NN, NN), whole(CH, hid), whole(CH, hid),
        ],
        out_specs=(LINES_SPEC, ORDER_SPEC, whole(CH, LANES)),
        name="mlp",
    )(u, x, target, q, base, w1, w2t)


def final_kernel(u_ref, x_ref, dout_ref, mu_ref, inv_ref, ext_ref, spec_ref, base_ref, out_ref, gspec_ref, gw1_ref, gw2t_ref, loss_ref,
                 g_ref, s0_ref, s1_ref):
    @pl.when(first_step())
    def _():
        g_ref[...] = signed(base_ref[...], Place().y, 1).T
        gspec_ref[0] = spec_ref[:, :, :CH]
        gspec_ref[1] = spec_ref[:, :, CH:]
        grads = ext_ref[:, SUB:].reshape(CH, LANES)
        gw1_ref[...] = grads[:, :LN]
        gw2t_ref[...] = grads[:, LN:2 * LN]
        loss = jnp.sum(jnp.sum(grads[:SUB, 2 * LN:], axis=0, keepdims=True), axis=1, keepdims=True) / TOTAL
        loss_ref[...] = jnp.broadcast_to(loss, (SUB, LN))
        sums = sum(ext_ref[n, :SUB] for n in range(PLANE)) / POINTS
        for b in range(NB):
            chans, lanes = slice(CH * b, CH * (b + 1)), slice(LN * b, LN * (b + 1))
            s0, s1 = (jnp.broadcast_to(sums[n:n + 1, lanes], (LN, LN)).T for n in range(2))
            s0_ref[chans] = s0[:CH]
            s1_ref[chans] = s1[:CH] + s1[CH:]

    dn = to_grid(u_ref[...], g_ref[...]).reshape(SUB, CH, NN)
    xt = jnp.swapaxes(x_ref[0], 0, 1)
    chans = pl.ds(pl.multiple_of(pl.program_id(0) * CH, CH), CH)
    inv = inv_ref[:, :1]
    normed = (xt - mu_ref[:, :1]) * inv
    r = dout_ref[0] + inv * (dn - s0_ref[chans, :1] - normed * s1_ref[chans, :1])
    out_ref[0] = jnp.swapaxes(r, 0, 1)


def final(u, x, dout, mu, inv, ext, spec, base):
    hid = 2 * CH
    degrees = NL // 4
    return call(
        final_kernel,
        [(NB, CH, NT, NN), (2, degrees, CH, CH), (CH, hid), (CH, hid), (SUB, LN)],
        [vmem(NN, NN), vmem(NB * CH, LN), vmem(NB * CH, LN)],
        grid=(NB, T8),
        in_specs=[
            ORDER_SPEC, GRID_SPEC, LINES_SPEC, CHAN_SPEC, CHAN_SPEC,
            whole(PLANE, 2 * SUB, LANES), whole(degrees, CH, LN), whole(NN, NN),
        ],
        out_specs=(GRID_SPEC, whole(2, degrees, CH, CH), whole(CH, hid), whole(CH, hid), whole(SUB, LN)),
        name="final",
    )(u, x, dout, mu, inv, ext, spec.reshape(degrees, CH, LN), base)


def solution(mesh):
    def local_step(x, target, q, leg_fwd, leg_inv, spec_w, w1, w2):
        base = jnp.asarray(dft_matrix())
        p_own, q_own = (jnp.swapaxes(v, 1, 2).reshape(HALF_TABLE) for v in (leg_fwd, leg_inv))
        z, p_peer, mu, inv, c0, kern = front(x, p_own, jnp.moveaxis(spec_w, 1, 3), base, 0)
        a, q_peer = analyze((p_own, p_peer), z, jnp.zeros((CH, LANES), F32), 1, q_own)
        b = mix(a, kern)
        u, _ = synth((q_own, q_peer), b, 2)
        dout, dz, grads = mlp(u, x, target, q, base, w1, w2.T)
        db = analyze((q_own, q_peer), dz, grads, 3)
        da, dk = mixb(a, db, kern, c0)
        du, ext, spec = synth((p_own, p_peer), da, 4, dk)
        d_field, grad_spec, gw1, gw2t, loss = final(du, x, dout, mu, inv, ext, spec, base)
        return loss[0, 0], d_field, grad_spec, gw1, gw2t.T

    grid_spec = P("dp", None, "h", "w")
    table_spec = P("w", None, "h")
    return jax.shard_map(
        local_step,
        mesh=mesh,
        in_specs=(grid_spec, grid_spec, P("h"), table_spec, table_spec, P(), P(), P()),
        out_specs=(P(), grid_spec, P(None, "h", None, None), P(), P()),
        check_vma=False,
    )
```

```python
import math
import numpy as np
import jax
import jax.numpy as jnp
from jax import lax
from jax.experimental import pallas as pl
from jax.experimental.pallas import tpu as pltpu
from jax.sharding import PartitionSpec as P

NORM_EPS = 1e-5
HI = lax.Precision.HIGHEST
F32 = jnp.float32
BF16 = jnp.bfloat16
MESH = pl.DeviceIdType.MESH
GELU_A = math.sqrt(2.0 / math.pi)
GELU_B = 0.044715

NB, CH, NT, NN = 3, 64, 64, 256
NM, NL = 128, 128
LON, LAT, BATCH = 512, 256, 12
POINTS = LON * LAT
TOTAL = POINTS * BATCH * CH
LANES = NB * 2 * CH
SUB, LN = 8, 128
T8 = NT // SUB
GROUPS = NM // SUB
PLANE = 8
H_OF_PAIR = (0, 0, 3, 3, 1, 1, 2, 2)
BLOCK = SUB * SUB
PLACES = GROUPS + 1
DATA = PLACES * BLOCK
STAT = DATA
GRAD = DATA + SUB
ROWS = GRAD + SUB
SPARE = BLOCK
SLOTS = (2, 2, 2)
COUNT = 6
AT_ONCE = 4
UNROLL = 2
LATE = SUB // 2
NN_DIMS, NT_DIMS, TN_DIMS = ((1,), (0,)), ((1,), (1,)), ((0,), (0,))
SUM_ENDS = (2, 5, 8, 11, 14, 16, 17)
GATHER_ENDS = (3, 6, 9, 12, 15, 17)
MIX_AFTER = (2, 3, 4, 6)

SMEM = pl.BlockSpec(memory_space=pltpu.SMEM)
VMEM = pl.BlockSpec(memory_space=pltpu.VMEM)
ANY = pl.BlockSpec(memory_space=pl.ANY)


def dot(a, b, dims=NN_DIMS):
    return lax.dot_general(a, b, (dims, ((), ())), precision=HI, preferred_element_type=F32)


def mxu(a, b, dims=NN_DIMS):
    return lax.dot_general(a, b, (dims, ((), ())), preferred_element_type=F32)


def call(kernel, outs, scratch=(), cid=None, **kw):
    extra = {} if cid is None else {"collective_id": cid, "has_side_effects": True}
    return pl.pallas_call(
        kernel,
        out_shape=tuple(jax.ShapeDtypeStruct(s, F32) for s in outs),
        scratch_shapes=list(scratch),
        compiler_params=pltpu.CompilerParams(vmem_limit_bytes=62 << 20, **extra),
        **kw,
    )


def vmem(*shape, dtype=F32):
    return pltpu.VMEM(shape, dtype)


def dma_sems(*shape):
    return pltpu.SemaphoreType.DMA(shape)


def rows(lo, hi):
    return pl.ds(lo, hi - lo)


def dft_matrix():
    theta = 2.0 * np.pi * ((np.arange(NN)[:, None] * np.arange(NM)[None, :]) % LON) / LON
    return (np.concatenate([np.cos(theta), -np.sin(theta)], axis=1) / math.sqrt(LON)).astype(np.float32)


def signed(base, half, weight):
    m = lax.broadcasted_iota(jnp.int32, base.shape, 1) % NM
    out = jnp.where((m % 2) * half == 1, -base, base)
    return jnp.where(m == 0, out, weight * out) if weight > 1 else out


def to_orders(lines, ft):
    z = dot(lines, ft).reshape(SUB, CH, NN)
    z = jnp.concatenate([z[:, :, :NM], z[:, :, NM:]], axis=1)
    return jnp.swapaxes(z, 1, 2)


def to_grid(orders, ft):
    u = jnp.swapaxes(orders, 1, 2)
    u = jnp.concatenate([u[:, :CH, :], u[:, CH:, :]], axis=2).reshape(SUB * CH, NN)
    return dot(u, ft)


def place_of_block(j):
    k = min(j, GROUPS - 1 - j)
    return H_OF_PAIR[k] // 2, H_OF_PAIR[k] % 2, k % 2


def slot_index(d):
    return d // 4, d // 2 % 2, d % 2


def sum_position(j, g):
    k = min(j, GROUPS - 1 - j)
    return 2 * g + 1 if j < SUB else jnp.where(g <= k, 2 * g, k + 1 + g)


def start_of(i, ends):
    return ends[i - 1] if i > 0 else 0


def chunk(i, share, ends):
    lo = start_of(i, ends) * BLOCK
    hi = ends[i] * BLOCK if ends[i] < PLACES else ROWS
    return lo, lo + (hi - lo) * share // BLOCK * SUB, hi


class Place:
    def __init__(self):
        self.h, self.y, self.z = lax.axis_index("h"), lax.axis_index("w"), lax.axis_index("dp")
        self.x, self.c = self.h // 2, self.h % 2
        self.slot = 2 * self.h + self.y
        self.low = self.h < 2
        self.pair = jnp.where(self.low, 4 * self.h, 14 - 4 * self.h) + self.y
        self.sibling = {"h": 2 * self.x + 1 - self.c}
        self.xn = {"h": 2 * (1 - self.x) + self.c}
        self.yn = {"w": 1 - self.y}

    def plane(self, r):
        s = (self.slot + r) % PLANE
        return {"h": s // 2, "w": s % 2}

    def greet(self, others):
        barrier = pltpu.get_barrier_semaphore()
        for other in others:
            pl.semaphore_signal(barrier, inc=1, device_id=other, device_id_type=MESH)
        pl.semaphore_wait(barrier, len(others))


def send(src, dst, sems, i, to):
    return pltpu.make_async_remote_copy(
        src_ref=src, dst_ref=dst, send_sem=sems.at[0, i], recv_sem=sems.at[1, i], device_id=to, device_id_type=MESH
    )


CB = 16
PIECES = CH // CB
HALF_TABLE = (SUB, SUB, NT, NL)


def near_far(k):
    return pl.ds(pl.multiple_of(SUB * k, SUB), SUB), pl.ds(pl.multiple_of(SUB * (GROUPS - 1 - k), SUB), SUB)


def front_kernel(x_hbm, p_hbm, w_hbm, base_ref, z_hbm, p_peer, mu_ref, inv_ref, c0_ref, kern_ref,
                 xbuf, wbuf, pbuf, cols, pay, sbuf, zbuf, ftbuf, turned, own, s_x, s_w, s_z, s_p, s_st):
    place = Place()
    near, far = near_far(place.pair)

    def load_x(n):
        b, part = n // PIECES, pl.ds(n % PIECES * CB, CB)
        return pltpu.make_async_copy(x_hbm.at[b, part], xbuf.at[b, part], s_x.at[n])

    def load_w(i):
        return pltpu.make_async_copy(w_hbm.at[i], wbuf.at[i], s_w.at[i])

    def load_p(g):
        return pltpu.make_async_copy(p_hbm.at[g], pbuf.at[g], s_p.at[2, g])

    def give_p(g):
        return send(pbuf.at[g], p_peer.at[g], s_p, g, place.yn)

    @pl.loop(0, SUB)
    def _(g):
        load_p(g).start()

    @pl.loop(0, NB * PIECES)
    def _(n):
        load_x(n).start()

    for i in range(2):
        load_w(i).start()
    others = range(1, PLANE)
    place.greet([place.plane(r) for r in others])

    def offer(lo, hi):
        @pl.loop(lo, hi)
        def _(g):
            load_p(g).wait()
            give_p(g).start()

    offer(0, 1)
    cols[...] = jnp.zeros_like(cols)

    @pl.loop(0, NB * PIECES)
    def _(n):
        load_x(n).wait()
        v = xbuf[n // PIECES, pl.ds(n % PIECES * CB, CB)]
        mean = jnp.sum(jnp.sum(v, axis=1, keepdims=True), axis=2, keepdims=True) / (NT * NN)
        diff = v - mean
        m2 = jnp.sum(jnp.sum(diff * diff, axis=1, keepdims=True), axis=2, keepdims=True)
        lane = lax.broadcasted_iota(jnp.int32, (CB, 1, LN), 2)
        cols[pl.ds(pl.multiple_of(n * CB, CB), CB)] = jnp.where(lane < CH, mean, m2).reshape(CB, LN)
    wide = cols[...].T
    p1 = jnp.where(place.y == 0, jnp.sum(pbuf[0, 0], axis=0, keepdims=True), 0.0)
    pay[...] = jnp.concatenate([
        *(wide[n:n + 1] for n in (0, CH)), jnp.concatenate([p1, p1], axis=1), jnp.zeros((SUB - 3, NN), F32)
    ], axis=0)

    def give_stats(r):
        return send(pay, sbuf.at[place.slot], s_st, r, place.plane(r))

    for r in others:
        give_stats(r).start()
    offer(1, SUB)
    sbuf[place.slot] = pay[...]
    ftbuf[...] = signed(base_ref[...], place.y, 1)

    for i in range(2):
        load_w(i).wait()

    @pl.loop(0, CH)
    def _(i):
        turned[...] = jnp.concatenate([wbuf[n, i] for n in range(2)], axis=0).T
        own[i, :SUB] = turned[near]
        own[i, SUB:] = turned[far]

    top = jnp.swapaxes(own[...], 0, 1)
    kern_ref[:, :CH] = top
    kern_ref[:, CH:] = jnp.concatenate([-top[:, :, CH:], top[:, :, :CH]], axis=2)

    for r in others:
        give_stats(r).wait_recv()
    means, m2s, p1s = (jnp.concatenate([sbuf[s, n:n + 1] for s in range(PLANE)], axis=0) for n in range(3))
    mu = jnp.sum(means, axis=0, keepdims=True) / PLANE
    dev = means - mu
    var = (jnp.sum(m2s, axis=0, keepdims=True) + (NT * NN) * jnp.sum(dev * dev, axis=0, keepdims=True)) / POINTS
    c0 = math.sqrt(LON) * jnp.sum(p1s, axis=0, keepdims=True)
    mu_ref[...], inv_ref[...], turned[...] = (
        jnp.broadcast_to(v, (LN, NN)).T[:n] for v, n in ((mu, NB * CH), (lax.rsqrt(var + NORM_EPS), NB * CH), (c0, NL))
    )
    c0_ref[:SUB] = turned[near]
    c0_ref[SUB:] = turned[far]

    def store_z(n):
        t = pl.multiple_of(n % T8 * SUB, SUB)
        lanes = pl.multiple_of(n // T8 * LN, LN)
        return pltpu.make_async_copy(zbuf.at[n % 2], z_hbm.at[pl.ds(t, SUB), :, pl.ds(lanes, LN)], s_z.at[n % 2])

    @pl.loop(0, NB * T8)
    def _(n):
        @pl.when(n >= 2)
        def _():
            store_z(n - 2).wait()

        b = n // T8
        xt = jnp.swapaxes(xbuf[b, :, pl.ds(pl.multiple_of(n % T8 * SUB, SUB), SUB), :], 0, 1)
        chans = pl.ds(pl.multiple_of(b * CH, CH), CH)
        xn = (xt - mu_ref[chans, :1]) * inv_ref[chans, :1]
        zbuf[n % 2] = to_orders(xn.reshape(SUB * CH, NN), ftbuf[...])
        store_z(n).start()

    for n in range(2):
        store_z(NB * T8 - 2 + n).wait()
    for r in others:
        give_stats(r).wait_send()

    @pl.loop(0, SUB)
    def _(g):
        give_p(g).wait()


def front(x, p_own, spec_w, base, cid):
    return call(
        front_kernel,
        [(NT, NM, LANES), HALF_TABLE, (NB * CH, LN), (NB * CH, LN), (2 * SUB, LN), (2 * SUB, LN, LN)],
        [
            vmem(NB, CH, NT, NN), vmem(2, CH, CH, NL), vmem(*HALF_TABLE), vmem(NN, LN), vmem(SUB, NN), vmem(PLANE, SUB, NN),
            vmem(2, SUB, NM, LN), vmem(NN, NN), vmem(NL, LN), vmem(CH, 2 * SUB, LN),
            dma_sems(NB * PIECES), dma_sems(2), dma_sems(2), dma_sems(3, SUB), dma_sems(2, PLANE),
        ],
        cid=cid,
        in_specs=[ANY, ANY, ANY, VMEM],
        out_specs=(ANY, ANY, VMEM, VMEM, VMEM, VMEM),
        name="front",
    )(x, p_own, spec_w, base)


def table_loader(own, peers, tbuf, sems, y):
    def copy(src, at, g):
        return pltpu.make_async_copy(src.at[at], tbuf.at[g], sems.at[g])

    def start(g):
        at = g % SUB
        away = g // SUB != y

        @pl.when(g // SUB == y)
        def _():
            copy(own, at, g).start()

        first = 0
        for src, count in peers:
            if src is not None:
                @pl.when(away & (at >= first) & (at < first + count))
                def _(src=src, first=first):
                    copy(src, at - first, g).start()
            first += count

    def wait(g):
        copy(own, 0, g).wait()

    return start, wait


def quarters(lo, hi):
    return [(max(lo, 4 * k), min(hi, 4 * k + 4), k) for k in range(4) if max(lo, 4 * k) < min(hi, 4 * k + 4)]


def by_degree(ref, v):
    n = v.shape[0] // SUB
    t = jnp.swapaxes(v.reshape(n, SUB, LANES), 0, 1)
    for b in range(NB):
        ref[:, n * b:n * (b + 1)] = t[:, :, LN * b:LN * (b + 1)]


def put_degrees(ref, parts, first, count):
    n = count * SUB
    t = jnp.concatenate([parts[:, n * b:n * (b + 1)] for b in range(NB)], axis=2)
    t = jnp.swapaxes(t, 0, 1)
    for i in range(count):
        to = BLOCK * (GROUPS - first - i)
        ref[to:to + BLOCK] = t[SUB * i:SUB * (i + 1)].reshape(BLOCK, LANES)


def near_mask(first, count, pair):
    place = first + lax.broadcasted_iota(jnp.int32, (NB * count * SUB, LN), 0) % (count * SUB) // SUB
    return (place % 2 == 1) & (place < 2 * (pair + 1))


def mix_places(first, count, pair, a_ref, kern_ref, b_ref, a, b):
    rows_in = a_ref[BLOCK * first:BLOCK * (first + count)]
    n = NB * count * SUB
    by_degree(a, rows_in)
    near = near_mask(first, count, pair)

    @pl.loop(0, SUB, unroll=UNROLL)
    def _(l):
        al = a[l, :n]
        b[l, :n] = jnp.where(near, dot(al, kern_ref[l]), dot(al, kern_ref[SUB + l]))

    put_degrees(b_ref, b, first, count)


def mix_back_places(first, count, pair, a_ref, db_ref, kern_ref, c0_ref, da_ref, dk_ref, s_ref, a, db, da):
    at = slice(BLOCK * first, BLOCK * (first + count))
    n = count * SUB
    by_degree(a, a_ref[at])
    by_degree(db, db_ref[at])
    near = near_mask(first, count, pair)

    @pl.loop(0, SUB, unroll=UNROLL)
    def _(l):
        al, dl = a[l, :NB * n], db[l, :NB * n]
        v = jnp.where(near, dot(dl, kern_ref[l], NT_DIMS), dot(dl, kern_ref[SUB + l], NT_DIMS))
        da[l, :NB * n] = v
        product = v * al
        s_ref[1:2] += jnp.concatenate([jnp.sum(product[n * i:n * (i + 1)], axis=0, keepdims=True) for i in range(NB)], axis=1)
        if first == 0:
            for row, c0 in ((SUB, l), (0, SUB + l)):
                c0 = jnp.concatenate([c0_ref[pl.ds(c0, 1)]] * NB, axis=1)
                s_ref[0:1] += c0 * jnp.concatenate([v[n * i + row:n * i + row + 1] for i in range(NB)], axis=1)
        for i, part in enumerate((jnp.where(near, al, 0.0), jnp.where(near, 0.0, al))):
            g = dot(part, dl, TN_DIMS)
            low = g[CH:]
            dk_ref[i, l] += g[:CH] + jnp.concatenate([low[:, CH:], -low[:, :CH]], axis=1)

    put_degrees(da_ref, da, first, count)


def analyze_kernel(share, with_q, *refs):
    if with_q:
        t_own, t_peer, z_hbm, q_own, kern_ref, out_ref, mix_ref, q_peer, a_deg, b_deg, qbuf, *rest = refs
        peers = [(t_peer, SUB)]
    else:
        t_own, t_low, t_high, z_hbm, ext_ref, kern_ref, a_ref, c0_ref, mix_ref, dk_ref, a_deg, b_deg, out_ref, s_ref, da_deg, *rest = refs
        peers = [(t_low, LATE), (t_high, SUB - LATE)]
        dk_ref[...] = jnp.zeros_like(dk_ref)
        s_ref[...] = jnp.zeros_like(s_ref)
    tbuf, zbuf, turned, part, sib, rx, ry, fx, fy, s_t, s_z, s_q, s_sib, s_x, s_y, s_fx, s_fy = rest
    count = len(SUM_ENDS)
    p = Place()
    x, c, y = p.x, p.c, p.y
    start_t, wait_t = table_loader(t_own, peers, tbuf, s_t, y)

    def load_z(g):
        return pltpu.make_async_copy(z_hbm.at[:, pl.ds(pl.multiple_of(SUB * g, SUB), SUB)], zbuf.at[g], s_z.at[g])

    @pl.loop(0, GROUPS)
    def _(g):
        start_t(g)
        load_z(g).start()

    p.greet([p.sibling, p.xn, p.yn])
    for d in range(PLANE):
        spare = part.at[slot_index(d)]
        spare[STAT:ROWS] = jnp.zeros((ROWS - STAT, LANES), F32)
        if not with_q:
            spare[STAT:GRAD] = ext_ref[SUB * d:SUB * (d + 1)]

    def load_q(g):
        return pltpu.make_async_copy(q_own.at[LATE + g], qbuf.at[g], s_q.at[2, g])

    def give_q(g):
        return send(qbuf.at[g], q_peer.at[g], s_q, g, p.yn)

    def compute(lo, hi, k):
        @pl.loop(lo, hi)
        def _(g):
            wait_t(g)
            load_z(g).wait()
            turned[...] = jnp.swapaxes(zbuf[g], 0, 1)

            at_once = AT_ONCE if k < 2 else 2

            @pl.loop(0, SUB, step=at_once)
            def _(some):
                for m in range(at_once):
                    m = some + m
                    r = dot(tbuf[g, m].T[4 * SUB * k:], turned[m])
                    for n in range(GROUPS - 4 * k):
                        j = 4 * k + n
                        row = sum_position(j, g) * BLOCK + SUB * m
                        if n < 4:
                            row = jnp.where(j >= g, row, ROWS)
                        xj, cj, yj = place_of_block(j)
                        part[xj, cj, yj, pl.ds(pl.multiple_of(row, SUB), SUB), :] = r[SUB * n:SUB * (n + 1)]

    def to_sibling(i):
        lo, _, hi = chunk(i, share, SUM_ENDS)
        return send(part.at[:, 1 - c, :, rows(lo, hi)], sib.at[:, :, rows(lo, hi)], s_sib, i, p.sibling)

    def to_x(i):
        lo, mid, _ = chunk(i, share, SUM_ENDS)
        return send(part.at[1 - x, c, :, rows(lo, mid)], rx.at[:, rows(lo, mid)], s_x, i, p.xn)

    def to_y(i):
        _, mid, hi = chunk(i, share, SUM_ENDS)
        return send(part.at[:, c, 1 - y, rows(mid, hi)], ry.at[:, rows(mid, hi)], s_y, i, p.yn)

    def forward_y(i):
        lo, mid, _ = chunk(i, share, SUM_ENDS)
        return send(part.at[x, c, 1 - y, rows(lo, mid)], fy.at[rows(lo, mid)], s_fy, i, p.yn)

    def forward_x(i):
        _, mid, hi = chunk(i, share, SUM_ENDS)
        return send(part.at[1 - x, c, y, rows(mid, hi)], fx.at[rows(mid, hi)], s_fx, i, p.xn)

    def chip_sum(i):
        lo, _, hi = chunk(i, share, SUM_ENDS)
        to_sibling(i).wait_recv()

        @pl.loop(lo, hi, step=2 * SUB)
        def _(row):
            some = pl.ds(pl.multiple_of(row, SUB), 2 * SUB)
            for a in range(2):
                for b in range(2):
                    part[a, c, b, some] += sib[a, b, some]

        to_x(i).start()
        to_y(i).start()
        if with_q and i < LATE:
            give_q(i).start()

    def half_sum(i):
        lo, mid, hi = chunk(i, share, SUM_ENDS)
        to_x(i).wait_recv()
        part[x, c, 1 - y, rows(lo, mid)] += rx[1 - y, rows(lo, mid)]
        forward_y(i).start()
        to_y(i).wait_recv()
        part[1 - x, c, y, rows(mid, hi)] += ry[1 - x, rows(mid, hi)]
        forward_x(i).start()
        out_ref[rows(lo, mid)] = part[x, c, y, rows(lo, mid)] + rx[y, rows(lo, mid)]
        out_ref[rows(mid, hi)] = part[x, c, y, rows(mid, hi)] + ry[x, rows(mid, hi)]

    def last_sum(i):
        lo, mid, hi = chunk(i, share, SUM_ENDS)
        forward_y(i).wait_recv()
        out_ref[rows(lo, mid)] += fy[rows(lo, mid)]
        forward_x(i).wait_recv()
        out_ref[rows(mid, hi)] += fx[rows(mid, hi)]

    def mixed(first, end):
        places = end - first
        if with_q:
            mix_places(first, places, p.pair, out_ref, kern_ref, mix_ref, a_deg, b_deg)
        else:
            mix_back_places(first, places, p.pair, a_ref, out_ref, kern_ref, c0_ref, mix_ref, dk_ref, s_ref, a_deg, b_deg, da_deg)

    if with_q:
        for g in range(LATE):
            load_q(g).start()
        for g in range(LATE):
            load_q(g).wait()
    for i in range(count + LAST_LAG):
        if i < count:
            for step in quarters(max(start_of(i, SUM_ENDS) - 1, 0), SUM_ENDS[i] - 1):
                compute(*step)
            to_sibling(i).start()
        if 0 < i <= count:
            chip_sum(i - 1)
        if HALF_LAG <= i < count + HALF_LAG:
            half_sum(i - HALF_LAG)
        if i >= LAST_LAG:
            last_sum(i - LAST_LAG)
            if i - LAST_LAG in MIX_AFTER:
                n = MIX_AFTER.index(i - LAST_LAG)
                mixed(SUM_ENDS[MIX_AFTER[n - 1]] if n > 0 else 0, SUM_ENDS[MIX_AFTER[n]])
    if with_q:
        mix_ref[STAT:] = jnp.zeros((ROWS - STAT, LANES), F32)
    else:
        mix_ref[STAT:GRAD] = s_ref[...]
        mix_ref[GRAD:] = out_ref[STAT:GRAD]
    for i in range(count):
        for copy in (to_sibling, to_x, to_y, forward_x, forward_y):
            copy(i).wait_send()
    if with_q:
        for g in range(LATE):
            give_q(g).wait()


HALF_LAG, LAST_LAG = 2, 4
MOST = 8


def analyze(table, z, cid, kern, q_own=None, back=()):
    with_q = q_own is not None
    share = 6 if with_q else 4
    piece = (LATE, *HALF_TABLE[1:])
    half = vmem(ROWS, LANES)
    pair = vmem(2, ROWS, LANES)
    degrees = vmem(SUB, NB * MOST * SUB, LN)
    if with_q:
        ins, places, outs = (q_own, kern), [ANY, VMEM], [(ROWS, LANES), (ROWS, LANES), piece]
        out_places, more = (VMEM, VMEM, ANY), [vmem(*piece)]
    else:
        ext, a, c0 = back
        ins, places, outs = (ext, kern, a, c0), [VMEM] * 4, [(ROWS, LANES), (2, SUB, CH, LN)]
        out_places, more = (VMEM, VMEM), [half, vmem(SUB, LANES), degrees]
    return call(
        lambda *refs: analyze_kernel(share, with_q, *refs),
        outs,
        [degrees, degrees] + more + [
            vmem(GROUPS, SUB, NT, NL), vmem(GROUPS, NT, SUB, LANES), vmem(SUB, NT, LANES), vmem(*SLOTS, ROWS + SPARE, LANES),
            vmem(*SLOTS[1:], ROWS, LANES), pair, pair, half, half,
            dma_sems(GROUPS), dma_sems(GROUPS), dma_sems(3, LATE),
        ] + [dma_sems(2, len(SUM_ENDS))] * 5,
        cid=cid,
        in_specs=[ANY] * len(table) + [ANY] + places,
        out_specs=out_places,
        name=f"analyze_{cid}",
    )(*table, z, *ins)


def synth_kernel(with_grads, *refs):
    if with_grads:
        t_own, t_peer, own_ref, dk_ref, u_hbm, ext_ref, spec_ref, *rest = refs
        *rest, zin, kin, zg, s_zk, s_zg, s_kin, s_kz = rest
        peers, share = [(t_peer, SUB)], 4
    else:
        t_own, t_peer, own_ref, u_hbm, q_low, *rest = refs
        *rest, s_q, s_low = rest
        peers, share = [(None, LATE), (t_peer, SUB - LATE)], 2
    tbuf, ubuf, turned, ball, s_t, s_u, s_sib, s_x, s_y, s_dx, s_dy, s_sx, s_sy, s_sd = rest
    p = Place()
    x, c, y = p.x, p.c, p.y
    start_t, wait_local = table_loader(t_own, peers, tbuf, s_t, y)

    def store_u(g):
        return pltpu.make_async_copy(ubuf.at[g], u_hbm.at[:, pl.ds(pl.multiple_of(SUB * g, SUB), SUB)], s_u.at[g])

    @pl.loop(0, GROUPS)
    def _(g):
        start_t(g)

    friends = [p.sibling, p.xn, p.yn]
    if with_grads:
        above = [{"dp": (p.z + r) % 4} for r in range(1, 4)]
        partner = [{"h": 3 - p.h}, {"h": 3 - p.h, "w": 1 - y}]
        friends = friends + above + partner
    p.greet(friends)

    def own_to(i, sems, to):
        lo, _, hi = chunk(i, share, GATHER_ENDS)
        src = own_ref if i < COUNT - 1 else ball.at[x, c, y]
        return send(src.at[rows(lo, hi)], ball.at[x, c, y, rows(lo, hi)], sems, i, to)

    def own_x(i):
        return own_to(i, s_x, p.xn)

    def own_y(i):
        return own_to(i, s_y, p.yn)

    def own_s(i):
        return own_to(i, s_sib, p.sibling)

    def relay(i, a, b, sems, to, lo, hi):
        return send(ball.at[a, c, b, rows(lo, hi)], ball.at[a, c, b, rows(lo, hi)], sems, i, to)

    def diagonal_y(i):
        lo, mid, _ = chunk(i, share, GATHER_ENDS)
        return relay(i, 1 - x, y, s_dy, p.yn, lo, mid)

    def diagonal_x(i):
        _, mid, hi = chunk(i, share, GATHER_ENDS)
        return relay(i, x, 1 - y, s_dx, p.xn, mid, hi)

    def sibling_x(i):
        lo, _, hi = chunk(i, share, GATHER_ENDS)
        return relay(i, 1 - x, y, s_sx, p.sibling, lo, hi)

    def sibling_y(i):
        lo, _, hi = chunk(i, share, GATHER_ENDS)
        return relay(i, x, 1 - y, s_sy, p.sibling, lo, hi)

    def sibling_d(i):
        lo, _, hi = chunk(i, share, GATHER_ENDS)
        return relay(i, 1 - x, 1 - y, s_sd, p.sibling, lo, hi)

    def give_q(g):
        return send(tbuf.at[SUB * y + g], tbuf.at[SUB * y + g], s_q, g, p.yn)

    def store_low(g):
        return pltpu.make_async_copy(tbuf.at[SUB * (1 - y) + g], q_low.at[g], s_low.at[g])

    def wait_t(g):
        if with_grads:
            wait_local(g)
        else:
            at = g % SUB

            @pl.when(at >= LATE)
            def _():
                wait_local(g)

            @pl.when((at < LATE) & (g // SUB != y))
            def _():
                give_q(at).wait_recv()
                store_low(at).start()

    def give(i):
        for copy in (own_x, own_y, own_s):
            copy(i).start()

    def pass_on(i):
        own_x(i).wait_recv()
        diagonal_y(i).start()
        own_y(i).wait_recv()
        diagonal_x(i).start()
        sibling_x(i).start()
        sibling_y(i).start()

    def collect(i):
        diagonal_y(i).wait_recv()
        diagonal_x(i).wait_recv()
        sibling_d(i).start()

    def complete(i):
        for copy in (own_s, sibling_x, sibling_y, sibling_d):
            copy(i).wait_recv()

    def compute(lo, hi, k):
        @pl.loop(0, hi - lo)
        def _(n):
            g = hi - 1 - n
            wait_t(g)

            at_once = AT_ONCE if k < 2 else 2

            @pl.loop(0, SUB, step=at_once)
            def _(some):
                for m in range(at_once):
                    m = some + m
                    tiles = []
                    for n in range(GROUPS - 4 * k):
                        j = 4 * k + n
                        row = (GROUPS - sum_position(j, g)) * BLOCK + SUB * m
                        if n < 4:
                            row = jnp.where(j >= g, row, ROWS)
                        xj, cj, yj = place_of_block(j)
                        tiles.append(ball[xj, cj, yj, pl.ds(pl.multiple_of(row, SUB), SUB), :])
                    turned[m] = dot(tbuf[g, m][:, 4 * SUB * k:], jnp.concatenate(tiles, axis=0))

            ubuf[g] = jnp.swapaxes(turned[...], 0, 1)
            store_u(g).start()

    if with_grads:
        quarter = pl.ds(2 * p.z, 2)

        def grads_z(r):
            return send(own_ref.at[GRAD:ROWS], zg.at[r], s_zg, r, above[r])

        def dk_z(r):
            return send(dk_ref.at[:, pl.ds(2 * ((p.z + 1 + r) % 4), 2)], zin.at[r], s_zk, r, above[r])

        stay = jnp.where(p.low, 0, 1)
        kept = jnp.where(p.low, p.pair, GROUPS - 1 - p.pair) % 4
        given = jnp.where(p.low, GROUPS - 1 - p.pair, p.pair) % 4

        def dk_plane(r):
            to = (p.yn, *partner)[r]
            src = kin.at[stay] if r == 0 else kin.at[1 - stay]
            return send(src, spec_ref.at[kept if r == 0 else given, quarter], s_kin, r, to)

        def dk_up(r):
            return send(spec_ref.at[:, quarter], spec_ref.at[:, quarter], s_kz, r, above[r])

        for r in range(3):
            grads_z(r).start()
            dk_z(r).start()

    give(0)
    if not with_grads:
        for g in range(LATE):
            wait_local(SUB * y + LATE - 1 - g)
        give_q(LATE - 1).start()
    give(1)
    ball[x, c, y, 0:ROWS] = own_ref[...]
    for d in range(PLANE):
        ball[*slot_index(d), ROWS:] = jnp.zeros((SPARE, LANES), F32)
    for i in range(COUNT + 2):
        if i < COUNT:
            pass_on(i)
        if not with_grads and i < LATE - 1:
            give_q(LATE - 2 - i).start()
        if with_grads and i == 1:
            for r in range(3):
                grads_z(r).wait_recv()
                ball[x, c, y, GRAD:ROWS] += zg[r]
        if with_grads and i == 2:
            for r in range(3):
                dk_z(r).wait_recv()
            kin[...] = dk_ref[:, quarter] + zin[0] + zin[1] + zin[2]
            for r in range(3):
                dk_plane(r).start()
            spec_ref[kept, quarter] = kin[stay]
        if with_grads and i == 3:
            for r in range(3):
                dk_plane(r).wait_recv()
            for r in range(3):
                dk_up(r).start()
        if i < COUNT - 2:
            give(i + 2)
        if 0 < i < COUNT:
            collect(i - 1)
        if i > 1:
            complete(i - 2)
            for step in reversed(quarters(max(GROUPS - GATHER_ENDS[i - 2], 0), GROUPS - start_of(i - 2, GATHER_ENDS))):
                compute(*step)
        if i == COUNT:
            collect(i - 1)
    if with_grads:
        for d in range(PLANE):
            ext_ref[d] = ball[*slot_index(d), STAT:ROWS]
    else:
        for g in range(LATE):
            give_q(g).wait_send()
            store_low(g).wait()
    for i in range(COUNT):
        for copy in (own_x, own_y, own_s, diagonal_x, diagonal_y, sibling_x, sibling_y, sibling_d):
            copy(i).wait_send()
    if with_grads:
        for r in range(3):
            grads_z(r).wait_send()
            dk_z(r).wait_send()
            dk_plane(r).wait_send()
            dk_up(r).wait()

    @pl.loop(0, GROUPS)
    def _(g):
        store_u(g).wait()


def synth(table, own, cid, dk=None):
    with_grads = dk is not None
    quarter = vmem(*SLOTS[1:], CH, LN)
    if with_grads:
        more = [(PLANE, 2 * SUB, LANES), (4, SUB, CH, LN)]
        scratch = [vmem(NB, *SLOTS[1:], CH, LN), quarter, vmem(NB, SUB, LANES)] + [dma_sems(2, NB)] * 4
    else:
        more = [(LATE, *HALF_TABLE[1:])]
        scratch = [dma_sems(2, LATE), dma_sems(LATE)]
    return call(
        lambda *refs: synth_kernel(with_grads, *refs),
        [(NT, NM, LANES)] + more,
        [
            vmem(GROUPS, SUB, NT, NL), vmem(GROUPS, NT, SUB, LANES), vmem(SUB, NT, LANES), vmem(*SLOTS, ROWS + SPARE, LANES),
            dma_sems(GROUPS), dma_sems(GROUPS),
        ] + [dma_sems(2, COUNT)] * 8 + scratch,
        cid=cid,
        in_specs=[ANY, ANY, VMEM] + [VMEM] * with_grads,
        out_specs=(ANY, VMEM, VMEM) if with_grads else (ANY, ANY),
        name=f"synth_{cid}",
    )(*table, own, *([dk] * with_grads))


def blocks(nt):
    return (
        pl.BlockSpec((1, CH, nt, NN), lambda b, t: (b, 0, t, 0)),
        pl.BlockSpec((1, nt, CH, NN), lambda b, t: (b, t, 0, 0)),
        pl.BlockSpec((nt, NM, LN), lambda b, t: (t, 0, b)),
    )


CHAN_SPEC = pl.BlockSpec((CH, LN), lambda b, t: (b, 0))
FINAL_T = 4 * SUB
WIDE = SUB * NN


def whole(*shape):
    return pl.BlockSpec(shape, lambda b, t: (0,) * len(shape))


def first_step():
    return (pl.program_id(0) == 0) & (pl.program_id(1) == 0)


def mlp_kernel(u_ref, x_ref, tgt_ref, q_ref, base_ref, w1_ref, w2t_ref, dout_ref, dz_ref, grads_ref,
               gt_ref, g_ref, line_ref, yb_ref, h_ref, act_ref, db_ref, dh_ref):
    @pl.when(first_step())
    def _():
        grads_ref[...] = jnp.zeros_like(grads_ref)
        gt_ref[...] = signed(base_ref[...], Place().y, 2)
        g_ref[...] = gt_ref[...].T

    y = to_grid(u_ref[...], g_ref[...]).reshape(SUB, CH, NN)
    r0 = jnp.swapaxes(x_ref[0] - tgt_ref[0], 0, 1)

    def wide(v):
        return jnp.concatenate([v[t] for t in range(SUB)], axis=1)

    line_ref[...] = wide(r0 + y)
    yb_ref[...] = wide(y).astype(BF16)
    h_ref[...] = mxu(w1_ref[...], yb_ref[...], TN_DIMS)
    for t in range(SUB):
        cols = slice(NN * t, NN * (t + 1))
        h = h_ref[:, cols]
        h2 = h * h
        th = jnp.tanh(h * (GELU_A + (GELU_A * GELU_B) * h2))
        cdf = 0.5 + 0.5 * th
        act_ref[:, cols] = (h * cdf).astype(BF16)
        h_ref[:, cols] = cdf + (0.5 * h) * (1.0 - th * th) * (GELU_A + (3.0 * GELU_A * GELU_B) * h2)
    res = line_ref[...] + mxu(w2t_ref[...], act_ref[...])
    first = pl.program_id(1) * SUB
    qw = jnp.concatenate([jnp.full((1, NN), q_ref[first + t], F32) for t in range(SUB)], axis=1)
    d = qw * res
    line_ref[...] = d
    db_ref[...] = d.astype(BF16)
    loss = jnp.sum((d * res).reshape(SUB, SUB, WIDE), axis=0)
    grads_ref[0:SUB, 2 * LN:] += sum(loss[:, LN * i:LN * (i + 1)] for i in range(WIDE // LN))
    for t in range(SUB):
        dout_ref[0, t] = line_ref[:, NN * t:NN * (t + 1)]
    dh_ref[...] = (mxu(w2t_ref[...], db_ref[...], TN_DIMS) * h_ref[...]).astype(BF16)
    grads_ref[:, :LN] += mxu(yb_ref[...], dh_ref[...], NT_DIMS)
    grads_ref[:, LN:2 * LN] += mxu(db_ref[...], act_ref[...], NT_DIMS)
    dy = line_ref[...] + mxu(w1_ref[...], dh_ref[...])
    dys = jnp.concatenate([dy[:, NN * t:NN * (t + 1)] for t in range(SUB)], axis=0)
    dz_ref[...] = to_orders(dys, gt_ref[...])


def mlp(u, x, target, q, base, w1, w2t):
    hid = 2 * CH
    grid, lines, orders = blocks(SUB)
    return call(
        mlp_kernel,
        [(NB, NT, CH, NN), (NT, NM, LANES), (CH, LANES)],
        [
            vmem(NN, NN), vmem(NN, NN), vmem(CH, WIDE), vmem(CH, WIDE, dtype=BF16), vmem(hid, WIDE),
            vmem(hid, WIDE, dtype=BF16), vmem(CH, WIDE, dtype=BF16), vmem(hid, WIDE, dtype=BF16),
        ],
        grid=(NB, T8),
        in_specs=[
            orders, grid, grid, SMEM, whole(NN, NN), whole(CH, hid), whole(CH, hid),
        ],
        out_specs=(lines, orders, whole(CH, LANES)),
        name="mlp",
    )(u, x, target, q, base, w1, w2t)


def final_kernel(u_ref, x_ref, dout_ref, mu_ref, inv_ref, ext_ref, spec_ref, base_ref, out_ref, gspec_ref, gw1_ref, gw2t_ref, loss_ref,
                 g_ref, s0_ref, s1_ref):
    @pl.when(first_step())
    def _():
        g_ref[...] = signed(base_ref[...], Place().y, 1).T
        gspec_ref[0] = spec_ref[:, :, :CH]
        gspec_ref[1] = spec_ref[:, :, CH:]
        grads = ext_ref[:, SUB:].reshape(CH, LANES)
        gw1_ref[...] = grads[:, :LN]
        gw2t_ref[...] = grads[:, LN:2 * LN]
        loss = jnp.sum(jnp.sum(grads[:SUB, 2 * LN:], axis=0, keepdims=True), axis=1, keepdims=True) / TOTAL
        loss_ref[...] = loss
        sums = sum(ext_ref[n, :SUB] for n in range(PLANE)) / POINTS
        for b in range(NB):
            chans, lanes = slice(CH * b, CH * (b + 1)), slice(LN * b, LN * (b + 1))
            s0, s1 = (jnp.broadcast_to(sums[n:n + 1, lanes], (LN, LN)).T for n in range(2))
            s0_ref[chans] = s0[:CH]
            s1_ref[chans] = s1[:CH] + s1[CH:]

    chans = pl.ds(pl.multiple_of(pl.program_id(0) * CH, CH), CH)
    inv = inv_ref[:, :1]
    slope = inv_ref[...] * inv_ref[...] * s1_ref[chans]

    @pl.loop(0, FINAL_T // SUB)
    def _(k):
        ts = pl.ds(pl.multiple_of(SUB * k, SUB), SUB)
        dn = to_grid(u_ref[ts], g_ref[...]).reshape(SUB, CH, NN)
        r = jnp.swapaxes(dout_ref[0, ts] + inv * (dn - s0_ref[chans, :1]), 0, 1)
        for c in range(CH):
            for n in range(NN // LN):
                lanes = slice(LN * n, LN * (n + 1))
                out_ref[0, c, ts, lanes] = r[c, :, lanes] - (x_ref[0, c, ts, lanes] - mu_ref[c:c + 1]) * slope[c:c + 1]


def final(u, x, dout, mu, inv, ext, spec, base):
    hid = 2 * CH
    degrees = NL // 4
    grid, lines, orders = blocks(FINAL_T)
    return call(
        final_kernel,
        [(NB, CH, NT, NN), (2, degrees, CH, CH), (CH, hid), (CH, hid), (1, 1)],
        [vmem(NN, NN), vmem(NB * CH, LN), vmem(NB * CH, LN)],
        grid=(NB, NT // FINAL_T),
        in_specs=[
            orders, grid, lines, CHAN_SPEC, CHAN_SPEC,
            whole(PLANE, 2 * SUB, LANES), whole(degrees, CH, LN), whole(NN, NN),
        ],
        out_specs=(grid, whole(2, degrees, CH, CH), whole(CH, hid), whole(CH, hid), whole(1, 1)),
        name="final",
    )(u, x, dout, mu, inv, ext, spec.reshape(degrees, CH, LN), base)


def solution(mesh):
    def local_step(x, target, q, leg_fwd, leg_inv, spec_w, w1, w2):
        base = jnp.asarray(dft_matrix())
        p_own, q_own = (jnp.swapaxes(v, 1, 2).reshape(HALF_TABLE) for v in (leg_fwd, leg_inv))
        z, p_peer, mu, inv, c0, kern = front(x, p_own, jnp.moveaxis(spec_w, 1, 3), base, 0)
        a, b, q_high = analyze((p_own, p_peer), z, 1, kern, q_own=q_own)
        u, q_low = synth((q_own, q_high), b, 2)
        dout, dz, grads = mlp(u, x, target, q, base, w1, w2.T)
        da, dk = analyze((q_own, q_low, q_high), dz, 3, kern, back=(grads, a, c0))
        du, ext, spec = synth((p_own, p_peer), da, 4, dk)
        d_field, grad_spec, gw1, gw2t, loss = final(du, x, dout, mu, inv, ext, spec, base)
        return loss.reshape(()), d_field, grad_spec, gw1, gw2t.T

    grid_spec = P("dp", None, "h", "w")
    table_spec = P("w", None, "h")
    return jax.shard_map(
        local_step,
        mesh=mesh,
        in_specs=(grid_spec, grid_spec, P("h"), table_spec, table_spec, P(), P(), P()),
        out_specs=(P(), grid_spec, P(None, "h", None, None), P(), P()),
        check_vma=False,
    )
```

```python
import math
import numpy as np
import jax
import jax.numpy as jnp
from jax import lax
from jax.experimental import pallas as pl
from jax.experimental.pallas import tpu as pltpu
from jax.sharding import PartitionSpec as P

NORM_EPS = 1e-5
HI = lax.Precision.HIGHEST
F32 = jnp.float32
BF16 = jnp.bfloat16
MESH = pl.DeviceIdType.MESH
GELU_A = math.sqrt(2.0 / math.pi)
GELU_B = 0.044715

ROW, COL = 0, 1
NB, CH, NT, NN = 3, 64, 64, 256
NM, NL = 128, 128
LON, LAT, BATCH = 512, 256, 12
POINTS = LON * LAT
TOTAL = POINTS * BATCH * CH
LANES = NB * 2 * CH
SUB, LN = 8, 128
T8 = NT // SUB
GROUPS = NM // SUB
PLANE = 8
H_OF_PAIR = (0, 0, 3, 3, 1, 1, 2, 2)
BLOCK = SUB * SUB
PLACES = GROUPS + 1
DATA = PLACES * BLOCK
STAT = DATA
GRAD = DATA + SUB
ROWS = GRAD + SUB
SPARE = BLOCK
SLOTS = (2, 2, 2)
AT_ONCE = 4
UNROLL = 2
LATE = 2
EARLY = SUB - LATE
NN_DIMS, NT_DIMS, TN_DIMS = ((1,), (0,)), ((1,), (1,)), ((0,), (0,))
SUM_ENDS = (2, 5, 8, 11, 14, 16, 17)
GATHER_ENDS = (3, 6, 9, 12, 15, 17)
MIX_AFTER = (2, 3, 4, 6)

SMEM = pl.BlockSpec(memory_space=pltpu.SMEM)
VMEM = pl.BlockSpec(memory_space=pltpu.VMEM)
ANY = pl.BlockSpec(memory_space=pl.ANY)


def dot(a, b, dims=NN_DIMS):
    return lax.dot_general(a, b, (dims, ((), ())), precision=HI, preferred_element_type=F32)


def mxu(a, b, dims=NN_DIMS):
    return lax.dot_general(a, b, (dims, ((), ())), preferred_element_type=F32)


def call(kernel, outs, scratch=(), cid=None, **kw):
    extra = {} if cid is None else {"collective_id": cid, "has_side_effects": True}
    return pl.pallas_call(
        kernel,
        out_shape=tuple(jax.ShapeDtypeStruct(s, F32) for s in outs),
        scratch_shapes=list(scratch),
        compiler_params=pltpu.CompilerParams(vmem_limit_bytes=62 << 20, **extra),
        **kw,
    )


def vmem(*shape, dtype=F32):
    return pltpu.VMEM(shape, dtype)


def dma_sems(*shape):
    return pltpu.SemaphoreType.DMA(shape)


def row_sum(v):
    return jnp.sum(v, axis=ROW, keepdims=True)


def block_sum(v):
    return jnp.sum(jnp.sum(v, axis=COL, keepdims=True), axis=COL + 1, keepdims=True)


def turn(v):
    return jnp.swapaxes(v, ROW, COL)


def rows(lo, hi):
    return pl.ds(lo, hi - lo)


def dft_matrix():
    theta = 2.0 * np.pi * ((np.arange(NN)[:, None] * np.arange(NM)[None, :]) % LON) / LON
    return (np.concatenate([np.cos(theta), -np.sin(theta)], axis=COL) / math.sqrt(LON)).astype(np.float32)


def signed(base, half, weight):
    m = lax.broadcasted_iota(jnp.int32, base.shape, 1) % NM
    out = jnp.where((m % 2) * half == 1, -base, base)
    return jnp.where(m == 0, out, weight * out) if weight > 1 else out


def to_orders(lines, ft):
    z = dot(lines, ft).reshape(SUB, CH, NN)
    z = jnp.concatenate([z[:, :, :NM], z[:, :, NM:]], axis=COL)
    return jnp.swapaxes(z, 1, 2)


def to_grid(orders, ft):
    u = jnp.swapaxes(orders, 1, 2)
    u = jnp.concatenate([u[:, :CH, :], u[:, CH:, :]], axis=2).reshape(SUB * CH, NN)
    return dot(u, ft)


def place_of_block(j):
    k = min(j, GROUPS - 1 - j)
    return H_OF_PAIR[k] // 2, H_OF_PAIR[k] % 2, k % 2


def slot_index(d):
    return d // 4, d // 2 % 2, d % 2


def sum_position(j, g):
    k = min(j, GROUPS - 1 - j)
    return 2 * g + 1 if j < SUB else jnp.where(g <= k, 2 * g, k + 1 + g)


def start_of(i, ends):
    return ends[i - 1] if i > 0 else 0


def chunk(i, share, ends):
    lo = start_of(i, ends) * BLOCK
    hi = ends[i] * BLOCK if ends[i] < PLACES else ROWS
    return lo, lo + (hi - lo) * share // BLOCK * SUB, hi


class Place:
    def __init__(self):
        self.h, self.y, self.z = lax.axis_index("h"), lax.axis_index("w"), lax.axis_index("dp")
        self.x, self.c = self.h // 2, self.h % 2
        self.slot = 2 * self.h + self.y
        self.low = self.h < 2
        self.pair = jnp.where(self.low, 4 * self.h, 14 - 4 * self.h) + self.y
        self.ox, self.oy = 1 - self.x, 1 - self.y
        self.sibling = {"h": 2 * self.x + 1 - self.c}
        self.xn = {"h": 2 * self.ox + self.c}
        self.yn = {"w": self.oy}

    def plane(self, r):
        s = (self.slot + r) % PLANE
        return {"h": s // 2, "w": s % 2}

    def greet(self, others):
        barrier = pltpu.get_barrier_semaphore()
        for other in others:
            pl.semaphore_signal(barrier, inc=1, device_id=other, device_id_type=MESH)
        pl.semaphore_wait(barrier, len(others))


def send(src, dst, sems, i, to):
    return pltpu.make_async_remote_copy(
        src_ref=src, dst_ref=dst, send_sem=sems.at[0, i], recv_sem=sems.at[1, i], device_id=to, device_id_type=MESH
    )


CB = 16
PIECES = CH // CB
HALF_TABLE = (SUB, SUB, NT, NL)


def near_far(k):
    return pl.ds(pl.multiple_of(SUB * k, SUB), SUB), pl.ds(pl.multiple_of(SUB * (GROUPS - 1 - k), SUB), SUB)


def front_kernel(x_hbm, p_hbm, w_hbm, base_ref, z_hbm, p_peer, mu_ref, inv_ref, c0_ref, kern_ref,
                 xbuf, wbuf, pbuf, cols, pay, sbuf, zbuf, ftbuf, turned, own, s_x, s_w, s_z, s_p, s_st):
    place = Place()
    near, far = near_far(place.pair)

    def load_x(n):
        b, part = n // PIECES, pl.ds(n % PIECES * CB, CB)
        return pltpu.make_async_copy(x_hbm.at[b, part], xbuf.at[b, part], s_x.at[n])

    def load_w(i):
        return pltpu.make_async_copy(w_hbm.at[i], wbuf.at[i], s_w.at[i])

    def load_p(g):
        return pltpu.make_async_copy(p_hbm.at[g], pbuf.at[g], s_p.at[2, g])

    def give_p(g):
        return send(pbuf.at[g], p_peer.at[g], s_p, g, place.yn)

    @pl.loop(0, SUB)
    def _(g):
        load_p(g).start()

    @pl.loop(0, NB * PIECES)
    def _(n):
        load_x(n).start()

    for i in range(2):
        load_w(i).start()
    others = range(1, PLANE)
    place.greet([place.plane(r) for r in others])

    def offer(lo, hi):
        @pl.loop(lo, hi)
        def _(g):
            load_p(g).wait()
            give_p(g).start()

    offer(0, 1)
    cols[...] = jnp.zeros_like(cols)

    @pl.loop(0, NB * PIECES)
    def _(n):
        load_x(n).wait()
        v = xbuf[n // PIECES, pl.ds(n % PIECES * CB, CB)]
        mean = block_sum(v) / (NT * NN)
        diff = v - mean
        m2 = block_sum(diff * diff)
        lane = lax.broadcasted_iota(jnp.int32, (CB, 1, LN), 2)
        cols[pl.ds(pl.multiple_of(n * CB, CB), CB)] = jnp.where(lane < CH, mean, m2).reshape(CB, LN)
    wide = cols[...].T
    p1 = jnp.where(place.y == 0, row_sum(pbuf[0, 0]), 0.0)
    pay[...] = jnp.concatenate([
        *(wide[n:n + 1] for n in (0, CH)), jnp.concatenate([p1, p1], axis=COL), jnp.zeros((SUB - 3, NN), F32)
    ], axis=ROW)

    def give_stats(r):
        return send(pay, sbuf.at[place.slot], s_st, r, place.plane(r))

    for r in others:
        give_stats(r).start()
    offer(1, SUB)
    sbuf[place.slot] = pay[...]
    ftbuf[...] = signed(base_ref[...], place.y, 1)

    for i in range(2):
        load_w(i).wait()

    @pl.loop(0, CH)
    def _(i):
        turned[...] = jnp.concatenate([wbuf[n, i] for n in range(2)], axis=ROW).T
        own[i, :SUB] = turned[near]
        own[i, SUB:] = turned[far]

    top = turn(own[...])
    kern_ref[:, :CH] = top
    kern_ref[:, CH:] = jnp.concatenate([-top[:, :, CH:], top[:, :, :CH]], axis=2)

    for r in others:
        give_stats(r).wait_recv()
    means, m2s, p1s = (jnp.concatenate([sbuf[s, n:n + 1] for s in range(PLANE)], axis=ROW) for n in range(3))
    mu = row_sum(means) / PLANE
    dev = means - mu
    var = (row_sum(m2s) + (NT * NN) * row_sum(dev * dev)) / POINTS
    c0 = math.sqrt(LON) * row_sum(p1s)
    mu_ref[...], inv_ref[...], turned[...] = (
        jnp.broadcast_to(v, (LN, NN)).T[:n] for v, n in ((mu, NB * CH), (lax.rsqrt(var + NORM_EPS), NB * CH), (c0, NL))
    )
    c0_ref[:SUB] = turned[near]
    c0_ref[SUB:] = turned[far]

    def store_z(n):
        t = pl.multiple_of(n % T8 * SUB, SUB)
        lanes = pl.multiple_of(n // T8 * LN, LN)
        return pltpu.make_async_copy(zbuf.at[n % 2], z_hbm.at[pl.ds(t, SUB), :, pl.ds(lanes, LN)], s_z.at[n % 2])

    @pl.loop(0, NB * T8)
    def _(n):
        @pl.when(n >= 2)
        def _():
            store_z(n - 2).wait()

        b = n // T8
        xt = turn(xbuf[b, :, pl.ds(pl.multiple_of(n % T8 * SUB, SUB), SUB), :])
        chans = pl.ds(pl.multiple_of(b * CH, CH), CH)
        xn = (xt - mu_ref[chans, :1]) * inv_ref[chans, :1]
        zbuf[n % 2] = to_orders(xn.reshape(SUB * CH, NN), ftbuf[...])
        store_z(n).start()

    for n in range(2):
        store_z(NB * T8 - 2 + n).wait()
    for r in others:
        give_stats(r).wait_send()

    @pl.loop(0, SUB)
    def _(g):
        give_p(g).wait()


def front(x, p_own, spec_w, base, cid):
    return call(
        front_kernel,
        [(NT, NM, LANES), HALF_TABLE, (NB * CH, LN), (NB * CH, LN), (2 * SUB, LN), (2 * SUB, LN, LN)],
        [
            vmem(NB, CH, NT, NN), vmem(2, CH, CH, NL), vmem(*HALF_TABLE), vmem(NN, LN), vmem(SUB, NN), vmem(PLANE, SUB, NN),
            vmem(2, SUB, NM, LN), vmem(NN, NN), vmem(NL, LN), vmem(CH, 2 * SUB, LN),
            dma_sems(NB * PIECES), dma_sems(2), dma_sems(2), dma_sems(3, SUB), dma_sems(2, PLANE),
        ],
        cid=cid,
        in_specs=[ANY, ANY, ANY, VMEM],
        out_specs=(ANY, ANY, VMEM, VMEM, VMEM, VMEM),
        name="front",
    )(x, p_own, spec_w, base)


def table_loader(own, peers, tbuf, sems, y):
    def copy(src, at, g):
        return pltpu.make_async_copy(src.at[at], tbuf.at[g], sems.at[g])

    def start(g):
        at = g % SUB
        away = g // SUB != y

        @pl.when(g // SUB == y)
        def _():
            copy(own, at, g).start()

        first = 0
        for src, count in peers:
            if src is not None:
                @pl.when(away & (at >= first) & (at < first + count))
                def _(src=src, first=first):
                    copy(src, at - first, g).start()
            first += count

    def wait(g):
        copy(own, 0, g).wait()

    return start, wait


def quarters(lo, hi):
    return [(max(lo, 4 * k), min(hi, 4 * k + 4), k) for k in range(4) if max(lo, 4 * k) < min(hi, 4 * k + 4)]


def by_degree(ref, v):
    n = v.shape[0] // SUB
    t = turn(v.reshape(n, SUB, LANES))
    for b in range(NB):
        ref[:, n * b:n * (b + 1)] = t[:, :, LN * b:LN * (b + 1)]


def put_degrees(ref, parts, first, count):
    n = count * SUB
    t = jnp.concatenate([parts[:, n * b:n * (b + 1)] for b in range(NB)], axis=2)
    t = turn(t)
    for i in range(count):
        to = BLOCK * (GROUPS - first - i)
        ref[to:to + BLOCK] = t[SUB * i:SUB * (i + 1)].reshape(BLOCK, LANES)


def near_mask(first, count, pair):
    place = first + lax.broadcasted_iota(jnp.int32, (NB * count * SUB, LN), 0) % (count * SUB) // SUB
    return (place % 2 == 1) & (place < 2 * (pair + 1))


def mix_places(first, count, pair, a_ref, kern_ref, b_ref, a, b):
    rows_in = a_ref[BLOCK * first:BLOCK * (first + count)]
    n = NB * count * SUB
    by_degree(a, rows_in)
    near = near_mask(first, count, pair)

    @pl.loop(0, SUB, unroll=UNROLL)
    def _(l):
        al = a[l, :n]
        b[l, :n] = jnp.where(near, dot(al, kern_ref[l]), dot(al, kern_ref[SUB + l]))

    put_degrees(b_ref, b, first, count)


def mix_back_places(first, count, pair, a_ref, db_ref, kern_ref, c0_ref, da_ref, dk_ref, s_ref, a, db, da):
    at = slice(BLOCK * first, BLOCK * (first + count))
    n = count * SUB
    by_degree(a, a_ref[at])
    by_degree(db, db_ref[at])
    near = near_mask(first, count, pair)

    @pl.loop(0, SUB, unroll=UNROLL)
    def _(l):
        al, dl = a[l, :NB * n], db[l, :NB * n]
        v = jnp.where(near, dot(dl, kern_ref[l], NT_DIMS), dot(dl, kern_ref[SUB + l], NT_DIMS))
        da[l, :NB * n] = v
        product = v * al
        s_ref[1:2] += jnp.concatenate([row_sum(product[n * i:n * (i + 1)]) for i in range(NB)], axis=COL)
        if first == 0:
            for row, c0 in ((SUB, l), (0, SUB + l)):
                c0 = jnp.concatenate([c0_ref[pl.ds(c0, 1)]] * NB, axis=COL)
                s_ref[0:1] += c0 * jnp.concatenate([v[n * i + row:n * i + row + 1] for i in range(NB)], axis=COL)
        for i, part in enumerate((jnp.where(near, al, 0.0), jnp.where(near, 0.0, al))):
            g = dot(part, dl, TN_DIMS)
            low = g[CH:]
            dk_ref[i, l] += g[:CH] + jnp.concatenate([low[:, CH:], -low[:, :CH]], axis=COL)

    put_degrees(da_ref, da, first, count)


def analyze_kernel(share, with_q, *refs):
    if with_q:
        t_own, t_peer, z_hbm, q_own, kern_ref, out_ref, mix_ref, q_peer, a_deg, b_deg, qbuf, *rest = refs
        peers = [(t_peer, SUB)]
    else:
        t_own, t_low, t_high, z_hbm, ext_ref, kern_ref, a_ref, c0_ref, mix_ref, dk_ref, a_deg, b_deg, out_ref, s_ref, da_deg, *rest = refs
        peers = [(t_low, LATE), (t_high, EARLY)]
        dk_ref[...] = jnp.zeros_like(dk_ref)
        s_ref[...] = jnp.zeros_like(s_ref)
    tbuf, zbuf, turned, part, sib, rx, ry, fx, fy, s_t, s_z, s_q, s_sib, s_x, s_y, s_fx, s_fy = rest
    count = len(SUM_ENDS)
    p = Place()
    x, c, y = p.x, p.c, p.y
    start_t, wait_t = table_loader(t_own, peers, tbuf, s_t, y)

    def load_z(g):
        return pltpu.make_async_copy(z_hbm.at[:, pl.ds(pl.multiple_of(SUB * g, SUB), SUB)], zbuf.at[g], s_z.at[g])

    @pl.loop(0, GROUPS)
    def _(g):
        start_t(g)
        load_z(g).start()

    p.greet([p.sibling, p.xn, p.yn])
    for d in range(PLANE):
        spare = part.at[slot_index(d)]
        spare[STAT:ROWS] = jnp.zeros((ROWS - STAT, LANES), F32)
        if not with_q:
            spare[STAT:GRAD] = ext_ref[SUB * d:SUB * (d + 1)]

    def load_q(g):
        return pltpu.make_async_copy(q_own.at[LATE + g], qbuf.at[g], s_q.at[2, g])

    def give_q(g):
        return send(qbuf.at[g], q_peer.at[g], s_q, g, p.yn)

    def compute(lo, hi, k):
        @pl.loop(lo, hi)
        def _(g):
            wait_t(g)
            load_z(g).wait()
            turned[...] = turn(zbuf[g])

            at_once = AT_ONCE if k < 2 else 2

            @pl.loop(0, SUB, step=at_once)
            def _(some):
                for m in range(at_once):
                    m = some + m
                    r = dot(tbuf[g, m].T[4 * SUB * k:], turned[m])
                    for n in range(GROUPS - 4 * k):
                        j = 4 * k + n
                        row = sum_position(j, g) * BLOCK + SUB * m
                        if n < 4:
                            row = jnp.where(j >= g, row, ROWS)
                        xj, cj, yj = place_of_block(j)
                        part[xj, cj, yj, pl.ds(pl.multiple_of(row, SUB), SUB), :] = r[SUB * n:SUB * (n + 1)]

    def to_sibling(i):
        lo, _, hi = chunk(i, share, SUM_ENDS)
        return send(part.at[:, 1 - c, :, rows(lo, hi)], sib.at[:, :, rows(lo, hi)], s_sib, i, p.sibling)

    def to_x(i):
        lo, mid, _ = chunk(i, share, SUM_ENDS)
        return send(part.at[p.ox, c, :, rows(lo, mid)], rx.at[:, rows(lo, mid)], s_x, i, p.xn)

    def to_y(i):
        _, mid, hi = chunk(i, share, SUM_ENDS)
        return send(part.at[:, c, p.oy, rows(mid, hi)], ry.at[:, rows(mid, hi)], s_y, i, p.yn)

    def forward_y(i):
        lo, mid, _ = chunk(i, share, SUM_ENDS)
        return send(part.at[x, c, p.oy, rows(lo, mid)], fy.at[rows(lo, mid)], s_fy, i, p.yn)

    def forward_x(i):
        _, mid, hi = chunk(i, share, SUM_ENDS)
        return send(part.at[p.ox, c, y, rows(mid, hi)], fx.at[rows(mid, hi)], s_fx, i, p.xn)

    def chip_sum(i):
        lo, _, hi = chunk(i, share, SUM_ENDS)
        to_sibling(i).wait_recv()

        @pl.loop(lo, hi, step=2 * SUB)
        def _(row):
            some = pl.ds(pl.multiple_of(row, SUB), 2 * SUB)
            for a in range(2):
                for b in range(2):
                    part[a, c, b, some] += sib[a, b, some]

        to_x(i).start()
        to_y(i).start()
        if with_q and i < EARLY:
            give_q(i).start()

    def half_sum(i):
        lo, mid, hi = chunk(i, share, SUM_ENDS)
        to_x(i).wait_recv()
        part[x, c, p.oy, rows(lo, mid)] += rx[p.oy, rows(lo, mid)]
        forward_y(i).start()
        to_y(i).wait_recv()
        part[p.ox, c, y, rows(mid, hi)] += ry[p.ox, rows(mid, hi)]
        forward_x(i).start()
        out_ref[rows(lo, mid)] = part[x, c, y, rows(lo, mid)] + rx[y, rows(lo, mid)]
        out_ref[rows(mid, hi)] = part[x, c, y, rows(mid, hi)] + ry[x, rows(mid, hi)]

    def last_sum(i):
        lo, mid, hi = chunk(i, share, SUM_ENDS)
        forward_y(i).wait_recv()
        out_ref[rows(lo, mid)] += fy[rows(lo, mid)]
        forward_x(i).wait_recv()
        out_ref[rows(mid, hi)] += fx[rows(mid, hi)]

    def mixed(first, end):
        places = end - first
        if with_q:
            mix_places(first, places, p.pair, out_ref, kern_ref, mix_ref, a_deg, b_deg)
        else:
            mix_back_places(first, places, p.pair, a_ref, out_ref, kern_ref, c0_ref, mix_ref, dk_ref, s_ref, a_deg, b_deg, da_deg)

    if with_q:
        for g in range(EARLY):
            load_q(g).start()
        for g in range(EARLY):
            load_q(g).wait()
    for i in range(count + LAST_LAG):
        if i < count:
            for step in quarters(max(start_of(i, SUM_ENDS) - 1, 0), SUM_ENDS[i] - 1):
                compute(*step)
            to_sibling(i).start()
        if 0 < i <= count:
            chip_sum(i - 1)
        if HALF_LAG <= i < count + HALF_LAG:
            half_sum(i - HALF_LAG)
        if i >= LAST_LAG:
            last_sum(i - LAST_LAG)
            if i - LAST_LAG in MIX_AFTER:
                n = MIX_AFTER.index(i - LAST_LAG)
                mixed(SUM_ENDS[MIX_AFTER[n - 1]] if n > 0 else 0, SUM_ENDS[MIX_AFTER[n]])
    if with_q:
        mix_ref[STAT:] = jnp.zeros((ROWS - STAT, LANES), F32)
    else:
        mix_ref[STAT:GRAD] = s_ref[...]
        mix_ref[GRAD:] = out_ref[STAT:GRAD]
    for i in range(count):
        for copy in (to_sibling, to_x, to_y, forward_x, forward_y):
            copy(i).wait_send()
    if with_q:
        for g in range(EARLY):
            give_q(g).wait()


HALF_LAG, LAST_LAG = 2, 4
MOST = 8


def analyze(table, z, cid, kern, q_own=None, back=()):
    with_q = q_own is not None
    share = 7 if with_q else 4
    piece = (EARLY, *HALF_TABLE[1:])
    half = vmem(ROWS, LANES)
    pair = vmem(2, ROWS, LANES)
    degrees = vmem(SUB, NB * MOST * SUB, LN)
    if with_q:
        ins, places, outs = (q_own, kern), [ANY, VMEM], [(ROWS, LANES), (ROWS, LANES), piece]
        out_places, more = (VMEM, VMEM, ANY), [vmem(*piece)]
    else:
        ext, a, c0 = back
        ins, places, outs = (ext, kern, a, c0), [VMEM] * 4, [(ROWS, LANES), (2, SUB, CH, LN)]
        out_places, more = (VMEM, VMEM), [half, vmem(SUB, LANES), degrees]
    return call(
        lambda *refs: analyze_kernel(share, with_q, *refs),
        outs,
        [degrees, degrees] + more + [
            vmem(GROUPS, SUB, NT, NL), vmem(GROUPS, NT, SUB, LANES), vmem(SUB, NT, LANES), vmem(*SLOTS, ROWS + SPARE, LANES),
            vmem(*SLOTS[1:], ROWS, LANES), pair, pair, half, half,
            dma_sems(GROUPS), dma_sems(GROUPS), dma_sems(3, EARLY),
        ] + [dma_sems(2, len(SUM_ENDS))] * 5,
        cid=cid,
        in_specs=[ANY] * len(table) + [ANY] + places,
        out_specs=out_places,
        name=f"analyze_{cid}",
    )(*table, z, *ins)


class Gather:
    def __init__(self, p, own_ref, ball, sems):
        self.p, self.own_ref, self.ball, self.sems = p, own_ref, ball, sems

    def relay(self, piece, n, to, a, b, part, src=None):
        i, lo, mid, hi, lanes = piece
        at = (rows(lo, hi), rows(lo, mid), rows(mid, hi))[part]
        here = self.ball.at[a, self.p.c, b, at, lanes]
        return send(here if src is None else src.at[at, lanes], here, self.sems[n], i, to)

    def own(self, piece, n, to):
        return self.relay(piece, n, to, self.p.x, self.p.y, 0, self.own_ref)

    def own_x(self, piece):
        return self.own(piece, 0, self.p.xn)

    def own_y(self, piece):
        return self.own(piece, 1, self.p.yn)

    def own_s(self, piece):
        return self.own(piece, 2, self.p.sibling)

    def diagonal_y(self, piece):
        return self.relay(piece, 3, self.p.yn, self.p.ox, self.p.y, 1)

    def diagonal_x(self, piece):
        return self.relay(piece, 4, self.p.xn, self.p.x, self.p.oy, 2)

    def sibling_x(self, piece):
        return self.relay(piece, 5, self.p.sibling, self.p.ox, self.p.y, 0)

    def sibling_y(self, piece):
        return self.relay(piece, 6, self.p.sibling, self.p.x, self.p.oy, 0)

    def sibling_d(self, piece):
        return self.relay(piece, 7, self.p.sibling, self.p.ox, self.p.oy, 0)

    def give(self, piece):
        for copy in (self.own_x, self.own_y, self.own_s):
            copy(piece).start()

    def pass_on(self, piece):
        self.own_x(piece).wait_recv()
        self.diagonal_y(piece).start()
        self.own_y(piece).wait_recv()
        self.diagonal_x(piece).start()
        self.sibling_x(piece).start()
        self.sibling_y(piece).start()

    def collect(self, piece):
        self.diagonal_y(piece).wait_recv()
        self.diagonal_x(piece).wait_recv()
        self.sibling_d(piece).start()

    def complete(self, piece):
        for copy in (self.own_s, self.sibling_x, self.sibling_y, self.sibling_d):
            copy(piece).wait_recv()

    def finish(self, piece):
        for copy in (
            self.own_x, self.own_y, self.own_s, self.diagonal_y, self.diagonal_x,
            self.sibling_x, self.sibling_y, self.sibling_d,
        ):
            copy(piece).wait_send()


def inverse_sums(tbuf, ball, turned, g, k, lanes, at_once):
    @pl.loop(0, SUB, step=at_once)
    def _(some):
        for m in range(at_once):
            m = some + m
            tiles = []
            for n in range(GROUPS - 4 * k):
                j = 4 * k + n
                row = (GROUPS - sum_position(j, g)) * BLOCK + SUB * m
                if n < 4:
                    row = jnp.where(j >= g, row, ROWS)
                xj, cj, yj = place_of_block(j)
                tiles.append(ball[xj, cj, yj, pl.ds(pl.multiple_of(row, SUB), SUB), lanes])
            turned[m] = dot(tbuf[g, m][:, 4 * SUB * k:], jnp.concatenate(tiles, axis=ROW))


ALL = pl.ds(0, LANES)


def synth_kernel(t_own, t_peer, own_ref, dk_ref, u_hbm, ext_ref, spec_ref, tbuf, ubuf, turned, ball, zin, kin, zg,
                 s_t, s_u, s_zk, s_zg, s_kin, s_kz, *sems):
    p = Place()
    x, c, y = p.x, p.c, p.y
    start_t, wait_t = table_loader(t_own, [(t_peer, SUB)], tbuf, s_t, y)
    count = len(GATHER_ENDS)

    def store_u(g):
        return pltpu.make_async_copy(ubuf.at[g], u_hbm.at[:, pl.ds(pl.multiple_of(SUB * g, SUB), SUB)], s_u.at[g])

    @pl.loop(0, GROUPS)
    def _(g):
        start_t(g)

    above = [{"dp": (p.z + r) % 4} for r in range(1, 4)]
    partner = [{"h": 3 - p.h}, {"h": 3 - p.h, "w": p.oy}]
    p.greet([p.sibling, p.xn, p.yn, *above, *partner])

    early = Gather(p, own_ref, ball, sems)
    late = Gather(p, ball.at[x, c, y], ball, sems)

    def piece(i):
        return i, *chunk(i, 4, GATHER_ENDS), ALL

    def gather(i):
        return late if i == count - 1 else early

    quarter = pl.ds(2 * p.z, 2)

    def grads_z(r):
        return send(own_ref.at[GRAD:ROWS], zg.at[r], s_zg, r, above[r])

    def dk_z(r):
        return send(dk_ref.at[:, pl.ds(2 * ((p.z + 1 + r) % 4), 2)], zin.at[r], s_zk, r, above[r])

    stay = jnp.where(p.low, 0, 1)
    kept = jnp.where(p.low, p.pair, GROUPS - 1 - p.pair) % 4
    given = jnp.where(p.low, GROUPS - 1 - p.pair, p.pair) % 4

    def dk_plane(r):
        to = (p.yn, *partner)[r]
        src = kin.at[stay] if r == 0 else kin.at[1 - stay]
        return send(src, spec_ref.at[kept if r == 0 else given, quarter], s_kin, r, to)

    def dk_up(r):
        return send(spec_ref.at[:, quarter], spec_ref.at[:, quarter], s_kz, r, above[r])

    def compute(lo, hi, k):
        @pl.loop(0, hi - lo)
        def _(n):
            g = hi - 1 - n
            wait_t(g)
            inverse_sums(tbuf, ball, turned, g, k, ALL, AT_ONCE)
            ubuf[g] = turn(turned[...])
            store_u(g).start()

    for r in range(3):
        grads_z(r).start()
        dk_z(r).start()
    for i in range(2):
        gather(i).give(piece(i))
    ball[x, c, y, 0:ROWS] = own_ref[...]
    for d in range(PLANE):
        ball[*slot_index(d), ROWS:] = jnp.zeros((SPARE, LANES), F32)
    for i in range(count + 2):
        if i < count:
            gather(i).pass_on(piece(i))
        if i == 1:
            for r in range(3):
                grads_z(r).wait_recv()
                ball[x, c, y, GRAD:ROWS] += zg[r]
        if i == 2:
            for r in range(3):
                dk_z(r).wait_recv()
            kin[...] = dk_ref[:, quarter] + zin[0] + zin[1] + zin[2]
            for r in range(3):
                dk_plane(r).start()
            spec_ref[kept, quarter] = kin[stay]
        if i == 3:
            for r in range(3):
                dk_plane(r).wait_recv()
            for r in range(3):
                dk_up(r).start()
        if i < count - 2:
            gather(i + 2).give(piece(i + 2))
        if 0 < i < count:
            gather(i - 1).collect(piece(i - 1))
        if i > 1:
            gather(i - 2).complete(piece(i - 2))
            for step in reversed(quarters(max(GROUPS - GATHER_ENDS[i - 2], 0), GROUPS - start_of(i - 2, GATHER_ENDS))):
                compute(*step)
        if i == count:
            gather(i - 1).collect(piece(i - 1))
    for d in range(PLANE):
        ext_ref[d] = ball[*slot_index(d), STAT:ROWS]
    for i in range(count):
        gather(i).finish(piece(i))
    for r in range(3):
        grads_z(r).wait_send()
        dk_z(r).wait_send()
        dk_plane(r).wait_send()
        dk_up(r).wait()

    @pl.loop(0, GROUPS)
    def _(g):
        store_u(g).wait()


def synth(table, own, cid, dk):
    quarter = (*SLOTS[1:], CH, LN)
    return call(
        synth_kernel,
        [(NT, NM, LANES), (PLANE, 2 * SUB, LANES), (4, SUB, CH, LN)],
        [
            vmem(GROUPS, SUB, NT, NL), vmem(GROUPS, NT, SUB, LANES), vmem(SUB, NT, LANES), vmem(*SLOTS, ROWS + SPARE, LANES),
            vmem(NB, *quarter), vmem(*quarter), vmem(NB, SUB, LANES), dma_sems(GROUPS), dma_sems(GROUPS),
        ] + [dma_sems(2, NB)] * 4 + [dma_sems(2, len(GATHER_ENDS))] * 8,
        cid=cid,
        in_specs=[ANY, ANY, VMEM, VMEM],
        out_specs=(ANY, VMEM, VMEM),
        name=f"synth_{cid}",
    )(*table, own, dk)


WIDE = SUB * NN
BT = 2 * SUB
PER = NT // BT
FIRST = 9 * BLOCK


def grid_stage(n, orders, x, tgt, q_ref, weights, dout, dz, grads_ref, scratch):
    g_ref, gt_ref, w1_ref, w2t_ref = weights
    some = range(BT // SUB)
    ts = [slice(SUB * k, SUB * (k + 1)) for k in some]

    def columns(t):
        return slice(NN * t, NN * (t + 1))

    def wide(v):
        return jnp.concatenate([v[t] for t in range(SUB)], axis=COL)

    line, yb, hid, act, db, dh = ([ref.at[k] for k in some] for ref in scratch)
    for k in some:
        y = to_grid(orders[k][...], g_ref[...]).reshape(SUB, CH, NN)
        r0 = turn(x[:, ts[k]] - tgt[:, ts[k]])
        line[k][...] = wide(r0 + y)
        yb[k][...] = wide(y).astype(BF16)
    for k in some:
        hid[k][...] = mxu(w1_ref[...], yb[k][...], TN_DIMS)
        for t in range(SUB):
            h = hid[k][:, columns(t)]
            h2 = h * h
            th = jnp.tanh(h * (GELU_A + (GELU_A * GELU_B) * h2))
            cdf = 0.5 + 0.5 * th
            act[k][:, columns(t)] = (h * cdf).astype(BF16)
            hid[k][:, columns(t)] = cdf + (0.5 * h) * (1.0 - th * th) * (GELU_A + (3.0 * GELU_A * GELU_B) * h2)
    for k in some:
        res = line[k][...] + mxu(w2t_ref[...], act[k][...])
        first = n % PER * BT + SUB * k
        d = jnp.concatenate([jnp.full((1, NN), q_ref[first + t], F32) for t in range(SUB)], axis=COL) * res
        line[k][...] = d
        db[k][...] = d.astype(BF16)
        loss = jnp.sum((d * res).reshape(SUB, SUB, WIDE), axis=ROW)
        grads_ref[:SUB, 2 * LN:] += sum(loss[:, LN * i:LN * (i + 1)] for i in range(WIDE // LN))
        for t in range(SUB):
            dout[SUB * k + t] = line[k][:, columns(t)]
    for k in some:
        dh[k][...] = (mxu(w2t_ref[...], db[k][...], TN_DIMS) * hid[k][...]).astype(BF16)
        grads_ref[:, :LN] += mxu(yb[k][...], dh[k][...], NT_DIMS)
        grads_ref[:, LN:2 * LN] += mxu(db[k][...], act[k][...], NT_DIMS)
    for k in some:
        dy = line[k][...] + mxu(w1_ref[...], dh[k][...])
        dys = jnp.concatenate([dy[:, columns(t)] for t in range(SUB)], axis=ROW)
        dz[ts[k]] = to_orders(dys, gt_ref[...])


def forward_kernel(t_own, t_high, own_ref, x_hbm, tgt_hbm, q_ref, base_ref, w1_ref, w2t_ref, dout_hbm, dz_hbm, q_low, grads_ref,
                   tbuf, ubuf, turned, ball, xbuf, tgtbuf, dbuf, zbuf, g_ref, gt_ref, line, yb, hid, act, db, dh,
                   s_t, s_in, s_out, s_q, s_low, *sems):
    p = Place()
    y = p.y
    start_t, wait_local = table_loader(t_own, [(None, LATE), (t_high, EARLY)], tbuf, s_t, y)
    gather = Gather(p, own_ref, ball, sems)
    share = 2

    def lanes(s):
        return pl.ds(pl.multiple_of(LN * s, LN), LN)

    def piece(s, half):
        lo, hi = ((0, FIRST), (FIRST, ROWS))[half]
        return 2 * s + half, lo, lo + (hi - lo) * share // BLOCK * SUB, hi, lanes(s)

    def each(step, s):
        for half in range(2):
            step(piece(s, half))

    def block(n):
        return n // PER, pl.ds(pl.multiple_of(n % PER * BT, BT), BT)

    def loads(n):
        b, t = block(n)
        return [
            pltpu.make_async_copy(src.at[b, :, t], dst.at[n % 2], s_in.at[i, n % 2])
            for i, (src, dst) in enumerate(((x_hbm, xbuf), (tgt_hbm, tgtbuf)))
        ]

    def stores(n):
        b, t = block(n)
        return [
            pltpu.make_async_copy(dbuf.at[n % 2], dout_hbm.at[b, t], s_out.at[0, n % 2]),
            pltpu.make_async_copy(zbuf.at[n % 2], dz_hbm.at[t, :, lanes(b)], s_out.at[1, n % 2]),
        ]

    def give_q(g):
        return send(tbuf.at[SUB * y + g], tbuf.at[SUB * y + g], s_q, g, p.yn)

    def store_low(g):
        return pltpu.make_async_copy(tbuf.at[SUB * p.oy + g], q_low.at[g], s_low.at[g])

    @pl.loop(0, GROUPS)
    def _(g):
        start_t(g)

    p.greet([p.sibling, p.xn, p.yn])
    gather.give(piece(0, 0))
    for g in reversed(range(LATE)):
        wait_local(SUB * y + g)
        give_q(g).start()
        if g == LATE - 1:
            gather.give(piece(0, 1))
    for copy in loads(0):
        copy.start()
    ball[p.x, p.c, y, :ROWS] = own_ref[...]
    for d in range(PLANE):
        ball[*slot_index(d), ROWS:] = jnp.zeros((SPARE, LANES), F32)
    grads_ref[...] = jnp.zeros_like(grads_ref)
    gt_ref[...] = signed(base_ref[...], y, 2)
    g_ref[...] = gt_ref[...].T
    each(gather.pass_on, 0)
    each(gather.give, 1)
    each(gather.collect, 0)

    @pl.loop(0, NB)
    def _(s):
        each(gather.complete, s)
        for k in reversed(range(4)):
            @pl.loop(0, 4)
            def _(n):
                g = 4 * k + 3 - n
                at = g % SUB

                @pl.when((s == 0) & (at >= LATE))
                def _():
                    wait_local(g)

                @pl.when((s == 0) & (at < LATE) & (g // SUB != y))
                def _():
                    give_q(at).wait_recv()
                    store_low(at).start()

                inverse_sums(tbuf, ball, turned, g, k, lanes(s), SUB)
                ubuf[:, pl.ds(pl.multiple_of(SUB * g, SUB), SUB)] = turn(turned[...])

        @pl.when(s + 1 < NB)
        def _():
            each(gather.pass_on, s + 1)

        @pl.when(s + 2 < NB)
        def _():
            each(gather.give, s + 2)

        @pl.loop(0, PER)
        def _(i):
            n = s * PER + i
            for copy in loads(n):
                copy.wait()

            @pl.when(n + 1 < NB * PER)
            def _():
                for copy in loads(n + 1):
                    copy.start()

            @pl.when(n > 1)
            def _():
                for copy in stores(n - 2):
                    copy.wait()

            orders = [ubuf.at[pl.ds(pl.multiple_of(i * BT + SUB * k, SUB), SUB)] for k in range(BT // SUB)]
            grid_stage(
                n, orders, xbuf.at[n % 2], tgtbuf.at[n % 2], q_ref, (g_ref, gt_ref, w1_ref, w2t_ref),
                dbuf.at[n % 2], zbuf.at[n % 2], grads_ref, (line, yb, hid, act, db, dh),
            )
            for copy in stores(n):
                copy.start()

            @pl.when((i == 1) & (s + 1 < NB))
            def _():
                each(gather.collect, s + 1)

    for n in range(2):
        for copy in stores(NB * PER - 2 + n):
            copy.wait()

    @pl.loop(0, NB)
    def _(s):
        each(gather.finish, s)

    for g in range(LATE):
        give_q(g).wait_send()
        store_low(g).wait()


def forward(table, own, x, target, q, base, w1, w2t, cid):
    hid = 2 * CH
    grid, two = (2, CH, BT, NN), BT // SUB
    return call(
        forward_kernel,
        [(NB, NT, CH, NN), (NT, NM, LANES), (LATE, *HALF_TABLE[1:]), (CH, LANES)],
        [
            vmem(GROUPS, SUB, NT, NL), vmem(NT, NM, LN), vmem(SUB, NT, LN), vmem(*SLOTS, ROWS + SPARE, LANES),
            vmem(*grid), vmem(*grid), vmem(2, BT, CH, NN), vmem(2, BT, NM, LN), vmem(NN, NN), vmem(NN, NN),
            vmem(two, CH, WIDE), vmem(two, CH, WIDE, dtype=BF16), vmem(two, hid, WIDE), vmem(two, hid, WIDE, dtype=BF16),
            vmem(two, CH, WIDE, dtype=BF16), vmem(two, hid, WIDE, dtype=BF16),
            dma_sems(GROUPS), dma_sems(2, 2), dma_sems(2, 2), dma_sems(2, LATE), dma_sems(LATE),
        ] + [dma_sems(2, 2 * NB)] * 8,
        cid=cid,
        in_specs=[ANY, ANY, VMEM, ANY, ANY, SMEM, VMEM, VMEM, VMEM],
        out_specs=(ANY, ANY, ANY, VMEM),
        name="forward",
    )(*table, own, x, target, q, base, w1, w2t)


def blocks(nt):
    return (
        pl.BlockSpec((1, CH, nt, NN), lambda b, t: (b, 0, t, 0)),
        pl.BlockSpec((1, nt, CH, NN), lambda b, t: (b, t, 0, 0)),
        pl.BlockSpec((nt, NM, LN), lambda b, t: (t, 0, b)),
    )


CHAN_SPEC = pl.BlockSpec((CH, LN), lambda b, t: (b, 0))
FINAL_T = 4 * SUB

def whole(*shape):
    return pl.BlockSpec(shape, lambda b, t: (0,) * len(shape))


def first_step():
    return (pl.program_id(0) == 0) & (pl.program_id(1) == 0)


def final_kernel(u_ref, x_ref, dout_ref, mu_ref, inv_ref, ext_ref, spec_ref, base_ref, out_ref, gspec_ref, gw1_ref, gw2t_ref, loss_ref,
                 g_ref, s0_ref, s1_ref):
    @pl.when(first_step())
    def _():
        g_ref[...] = signed(base_ref[...], Place().y, 1).T
        gspec_ref[0] = spec_ref[:, :, :CH]
        gspec_ref[1] = spec_ref[:, :, CH:]
        grads = ext_ref[:, SUB:].reshape(CH, LANES)
        gw1_ref[...] = grads[:, :LN]
        gw2t_ref[...] = grads[:, LN:2 * LN]
        loss = block_sum(grads[None, :SUB, 2 * LN:])[0] / TOTAL
        loss_ref[...] = loss
        sums = sum(ext_ref[n, :SUB] for n in range(PLANE)) / POINTS
        for b in range(NB):
            chans, lanes = slice(CH * b, CH * (b + 1)), slice(LN * b, LN * (b + 1))
            s0, s1 = (jnp.broadcast_to(sums[n:n + 1, lanes], (LN, LN)).T for n in range(2))
            s0_ref[chans] = s0[:CH]
            s1_ref[chans] = s1[:CH] + s1[CH:]

    chans = pl.ds(pl.multiple_of(pl.program_id(0) * CH, CH), CH)
    inv = inv_ref[:, :1]
    slope = inv_ref[...] * inv_ref[...] * s1_ref[chans]

    @pl.loop(0, FINAL_T // SUB)
    def _(k):
        ts = pl.ds(pl.multiple_of(SUB * k, SUB), SUB)
        dn = to_grid(u_ref[ts], g_ref[...]).reshape(SUB, CH, NN)
        r = turn(dout_ref[0, ts] + inv * (dn - s0_ref[chans, :1]))
        for c in range(CH):
            for n in range(NN // LN):
                lanes = slice(LN * n, LN * (n + 1))
                out_ref[0, c, ts, lanes] = r[c, :, lanes] - (x_ref[0, c, ts, lanes] - mu_ref[c:c + 1]) * slope[c:c + 1]


def final(u, x, dout, mu, inv, ext, spec, base):
    hid = 2 * CH
    degrees = NL // 4
    grid, lines, orders = blocks(FINAL_T)
    return call(
        final_kernel,
        [(NB, CH, NT, NN), (2, degrees, CH, CH), (CH, hid), (CH, hid), (1, 1)],
        [vmem(NN, NN), vmem(NB * CH, LN), vmem(NB * CH, LN)],
        grid=(NB, NT // FINAL_T),
        in_specs=[
            orders, grid, lines, CHAN_SPEC, CHAN_SPEC,
            whole(PLANE, 2 * SUB, LANES), whole(degrees, CH, LN), whole(NN, NN),
        ],
        out_specs=(grid, whole(2, degrees, CH, CH), whole(CH, hid), whole(CH, hid), whole(1, 1)),
        name="final",
    )(u, x, dout, mu, inv, ext, spec.reshape(degrees, CH, LN), base)


def solution(mesh):
    def local_step(x, target, q, leg_fwd, leg_inv, spec_w, w1, w2):
        base = jnp.asarray(dft_matrix())
        p_own, q_own = (jnp.swapaxes(v, 1, 2).reshape(HALF_TABLE) for v in (leg_fwd, leg_inv))
        z, p_peer, mu, inv, c0, kern = front(x, p_own, jnp.moveaxis(spec_w, 1, 3), base, 0)
        a, b, q_high = analyze((p_own, p_peer), z, 1, kern, q_own=q_own)
        dout, dz, q_low, grads = forward((q_own, q_high), b, x, target, q, base, w1, w2.T, 2)
        da, dk = analyze((q_own, q_low, q_high), dz, 3, kern, back=(grads, a, c0))
        du, ext, spec = synth((p_own, p_peer), da, 4, dk)
        d_field, grad_spec, gw1, gw2t, loss = final(du, x, dout, mu, inv, ext, spec, base)
        return loss.reshape(()), d_field, grad_spec, gw1, gw2t.T

    grid_spec = P("dp", None, "h", "w")
    table_spec = P("w", None, "h")
    return jax.shard_map(
        local_step,
        mesh=mesh,
        in_specs=(grid_spec, grid_spec, P("h"), table_spec, table_spec, P(), P(), P()),
        out_specs=(P(), grid_spec, P(None, "h", None, None), P(), P()),
        check_vma=False,
    )
```

```python
import math
import numpy as np
import jax
import jax.numpy as jnp
from jax import lax
from jax.experimental import pallas as pl
from jax.experimental.pallas import tpu as pltpu
from jax.sharding import PartitionSpec as P

NORM_EPS = 1e-5
HI = lax.Precision.HIGHEST
F32 = jnp.float32
BF16 = jnp.bfloat16
MESH = pl.DeviceIdType.MESH
GELU_A = math.sqrt(2.0 / math.pi)
GELU_B = 0.044715

ROW, COL = 0, 1
NB, CH, NT, NN = 3, 64, 64, 256
NM, NL = 128, 128
DFT_STEP = 16
BUFFERS = 2
HALF = 0.5
LON, LAT, BATCH = 512, 256, 12
POINTS = LON * LAT
TOTAL = POINTS * BATCH * CH
LANES = NB * 2 * CH
SUB, LN = 8, 128
T8 = NT // SUB
GROUPS = NM // SUB
PLANE, Z = 8, 4
PAIRS = SUB // 2
H_OF_PAIR = (0, 0, 3, 3, 1, 1, 2, 2)
BLOCK = SUB * SUB
PLACES = GROUPS + 1
DATA = PLACES * BLOCK
STAT = DATA
GRAD = DATA + SUB
ROWS = GRAD + SUB
SPARE = BLOCK
SLOTS = (2, 2, 2)
AT_ONCE = 4
UNROLL = 2
LATE = 2
EARLY = SUB - LATE
NN_DIMS, NT_DIMS, TN_DIMS = ((1,), (0,)), ((1,), (1,)), ((0,), (0,))
SUM_ENDS = (2, 5, 8, 11, 14, 16, 17)
GATHER_ENDS = (3, 6, 9, 12, 15, 17)
MIX_AFTER = (1, 3, 4, 5, 6), (2, 4, 6)

SMEM = pl.BlockSpec(memory_space=pltpu.SMEM)
VMEM = pl.BlockSpec(memory_space=pltpu.VMEM)
ANY = pl.BlockSpec(memory_space=pl.ANY)


def dot(a, b, dims=NN_DIMS):
    return lax.dot_general(a, b, (dims, ((), ())), precision=HI, preferred_element_type=F32)


def mxu(a, b, dims=NN_DIMS):
    return lax.dot_general(a, b, (dims, ((), ())), preferred_element_type=F32)


def call(kernel, outs, scratch=(), cid=None, **kw):
    extra = {} if cid is None else {"collective_id": cid, "has_side_effects": True}
    return pl.pallas_call(
        kernel,
        out_shape=tuple(jax.ShapeDtypeStruct(s, F32) for s in outs),
        scratch_shapes=list(scratch),
        compiler_params=pltpu.CompilerParams(vmem_limit_bytes=62 << 20, **extra),
        **kw,
    )


def vmem(*shape, dtype=F32):
    return pltpu.VMEM(shape, dtype)


def dma_sems(*shape):
    return pltpu.SemaphoreType.DMA(shape)


def row_sum(v):
    return jnp.sum(v, axis=ROW, keepdims=True)


def block_sum(v):
    return jnp.sum(jnp.sum(v, axis=COL, keepdims=True), axis=COL + 1, keepdims=True)


def col(v):
    return v[:, :1]


def turn(v):
    return jnp.swapaxes(v, ROW, COL)


def rows(lo, hi):
    return pl.ds(lo, hi - lo)


def dft_tables():
    small = np.arange(DFT_STEP)[:, None] * np.arange(NM)[None]
    coarse, fine = (np.exp(-2j * np.pi * (v % LON) / LON) for v in (DFT_STEP * small, small))
    coarse = coarse / math.sqrt(LON)
    return np.stack([coarse.real, coarse.imag, fine.real, fine.imag]).astype(np.float32)


def signed(tables, half, weight):
    fine_re, fine_im = tables[2], tables[3]
    lines = []
    for n in range(DFT_STEP):
        re, im = tables[0, n:n + 1], tables[1, n:n + 1]
        lines.append(jnp.concatenate([re * fine_re - im * fine_im, re * fine_im + im * fine_re], axis=COL))
    out = jnp.concatenate(lines, axis=ROW)
    m = lax.broadcasted_iota(jnp.int32, out.shape, 1) % NM
    out = jnp.where((m % 2) * half == 1, -out, out)
    return jnp.where(m == 0, out, weight * out) if weight > 1 else out


def to_orders(lines, ft):
    z = dot(lines, ft).reshape(SUB, CH, NN)
    z = jnp.concatenate([z[:, :, :NM], z[:, :, NM:]], axis=COL)
    return jnp.swapaxes(z, 1, 2)


def to_grid(orders, ft):
    u = jnp.swapaxes(orders, 1, 2)
    u = jnp.concatenate([u[:, :CH, :], u[:, CH:, :]], axis=2).reshape(SUB * CH, NN)
    return dot(u, ft)


def place_of_block(j):
    k = min(j, GROUPS - 1 - j)
    return H_OF_PAIR[k] // 2, H_OF_PAIR[k] % 2, k % 2


def slot_index(d):
    return d // 4, d // 2 % 2, d % 2


def sum_position(j, g):
    k = min(j, GROUPS - 1 - j)
    return 2 * g + 1 if j < SUB else jnp.where(g <= k, 2 * g, k + 1 + g)


def start_of(i, ends):
    return ends[i - 1] if i > 0 else 0


def chunk(i, share, ends):
    lo = start_of(i, ends) * BLOCK
    hi = ends[i] * BLOCK if ends[i] < PLACES else ROWS
    return lo, lo + (hi - lo) * share // (2 * BLOCK) * SUB, hi


class Place:
    def __init__(self):
        self.h, self.y, self.z = lax.axis_index("h"), lax.axis_index("w"), lax.axis_index("dp")
        self.x, self.c = self.h // 2, self.h % 2
        self.slot = 2 * self.h + self.y
        self.low = self.h < 2
        self.pair = jnp.where(self.low, 4 * self.h, 14 - 4 * self.h) + self.y
        self.ox, self.oy = 1 - self.x, 1 - self.y
        self.sibling = {"h": 2 * self.x + 1 - self.c}
        self.xn = {"h": 2 * self.ox + self.c}
        self.yn = {"w": self.oy}

    def plane(self, r):
        s = (self.slot + r) % PLANE
        return {"h": s // 2, "w": s % 2}

    def greet(self, others):
        barrier = pltpu.get_barrier_semaphore()
        for other in others:
            pl.semaphore_signal(barrier, inc=1, device_id=other, device_id_type=MESH)
        pl.semaphore_wait(barrier, len(others))


def send(src, dst, sems, i, to):
    return pltpu.make_async_remote_copy(
        src_ref=src, dst_ref=dst, send_sem=sems.at[0, i], recv_sem=sems.at[1, i], device_id=to, device_id_type=MESH
    )


CB = 16
PIECES = CH // CB
RAW_TABLE = (SUB, SUB, NT, NL)
HALF_TABLE = (SUB, PAIRS, NL, LN)


def near_far(k):
    return pl.ds(pl.multiple_of(SUB * k, SUB), SUB), pl.ds(pl.multiple_of(SUB * (GROUPS - 1 - k), SUB), SUB)


def front_kernel(x_hbm, p_hbm, q_hbm, w_hbm, base_ref, z_hbm, p_own, p_peer, q_own, mu_ref, inv_ref, c0_ref, kern_ref,
                 xbuf, wbuf, pbuf, qbuf, ppack, qpack, zeros, cols, pay, sbuf, zbuf, ftbuf, turned, own, s_x, s_w, s_z, s_p, s_q, s_st):
    place = Place()
    near, far = near_far(place.pair)

    def load_x(n):
        b, part = n // PIECES, pl.ds(n % PIECES * CB, CB)
        return pltpu.make_async_copy(x_hbm.at[b, part], xbuf.at[b, part], s_x.at[n])

    def load_w(i):
        return pltpu.make_async_copy(w_hbm.at[i], wbuf.at[i], s_w.at[i])

    def load_p(g):
        return pltpu.make_async_copy(p_hbm.at[g], pbuf.at[g], s_p.at[2, g])

    def load_q(g):
        return pltpu.make_async_copy(q_hbm.at[g], qbuf.at[g], s_q.at[0, g])

    def store_p(g):
        return pltpu.make_async_copy(ppack.at[g], p_own.at[g], s_q.at[1, g])

    def store_q(g):
        return pltpu.make_async_copy(qpack.at[g], q_own.at[g], s_q.at[2, g])

    def give_p(g):
        return send(ppack.at[g, :, used(g)], p_peer.at[g, :, used(g)], s_p, g, place.yn)

    def clear_p(g):
        return pltpu.make_async_copy(zeros.at[:, unused(g)], p_peer.at[g, :, unused(g)], s_q.at[3, g])

    def pack(src, dst, g):
        for i in range(PAIRS):
            dst[g, i] = jnp.concatenate([src[g, 2 * i + n] for n in range(2)], axis=ROW).T

    @pl.loop(0, SUB)
    def _(g):
        load_p(g).start()

    @pl.loop(0, NB * PIECES)
    def _(n):
        load_x(n).start()

    for i in range(2):
        load_w(i).start()

    @pl.loop(0, SUB)
    def _(g):
        load_q(g).start()

    others = range(1, PLANE)
    place.greet([place.plane(r) for r in others])

    zeros[...] = jnp.zeros_like(zeros)
    for g in range(1, SUB):
        clear_p(g).start()

    def offer(lo, hi):
        @pl.loop(lo, hi)
        def _(g):
            load_p(g).wait()
            pack(pbuf, ppack, g)
            store_p(g).start()

        for g in range(lo, hi):
            give_p(g).start()

    offer(0, 1)
    cols[...] = jnp.zeros_like(cols)

    @pl.loop(0, NB * PIECES)
    def _(n):
        load_x(n).wait()
        v = xbuf[n // PIECES, pl.ds(n % PIECES * CB, CB)]
        mean = block_sum(v) / (NT * NN)
        diff = v - mean
        m2 = block_sum(diff * diff)
        lane = lax.broadcasted_iota(jnp.int32, (CB, 1, LN), 2)
        cols[pl.ds(pl.multiple_of(n * CB, CB), CB)] = jnp.where(lane < CH, mean, m2).reshape(CB, LN)
    wide = cols[...].T
    p1 = jnp.where(place.y == 0, row_sum(pbuf[0, 0]), 0.0)
    pay[...] = jnp.concatenate([
        *(wide[n:n + 1] for n in (0, CH)), jnp.concatenate([p1, p1], axis=COL), jnp.zeros((SUB - 3, NN), F32)
    ], axis=ROW)

    def give_stats(r):
        return send(pay, sbuf.at[place.slot], s_st, r, place.plane(r))

    for r in others:
        give_stats(r).start()
    offer(1, SUB)
    sbuf[place.slot] = pay[...]
    ftbuf[...] = signed(base_ref, place.y, 1)

    @pl.loop(0, SUB)
    def _(g):
        load_q(g).wait()
        pack(qbuf, qpack, g)
        store_q(g).start()

    for i in range(2):
        load_w(i).wait()

    @pl.loop(0, CH)
    def _(i):
        turned[...] = jnp.concatenate([wbuf[n, i] for n in range(2)], axis=ROW).T
        own[i, :SUB] = turned[near]
        own[i, SUB:] = turned[far]

    top = turn(own[...])
    kern_ref[:, :CH] = top
    kern_ref[:, CH:] = jnp.concatenate([-top[:, :, CH:], top[:, :, :CH]], axis=2)

    for r in others:
        give_stats(r).wait_recv()
    means, m2s, p1s = (jnp.concatenate([sbuf[s, n:n + 1] for s in range(PLANE)], axis=ROW) for n in range(3))
    mu = row_sum(means) / PLANE
    dev = means - mu
    var = (row_sum(m2s) + (NT * NN) * row_sum(dev * dev)) / POINTS
    c0 = math.sqrt(LON) * row_sum(p1s)
    mu_ref[...], inv_ref[...], turned[...] = (
        jnp.broadcast_to(v, (LN, NN)).T[:n] for v, n in ((mu, NB * CH), (lax.rsqrt(var + NORM_EPS), NB * CH), (c0, NL))
    )
    c0_ref[:SUB] = turned[near]
    c0_ref[SUB:] = turned[far]

    def store_z(n):
        t = pl.multiple_of(n % T8 * SUB, SUB)
        lanes = pl.multiple_of(n // T8 * LN, LN)
        return pltpu.make_async_copy(zbuf.at[n % BUFFERS], z_hbm.at[pl.ds(t, SUB), :, pl.ds(lanes, LN)], s_z.at[n % BUFFERS])

    @pl.loop(0, NB * T8)
    def _(n):
        @pl.when(n >= BUFFERS)
        def _():
            store_z(n - BUFFERS).wait()

        b = n // T8
        xt = turn(xbuf[b, :, pl.ds(pl.multiple_of(n % T8 * SUB, SUB), SUB), :])
        chans = pl.ds(pl.multiple_of(b * CH, CH), CH)
        xn = (xt - col(mu_ref[chans])) * col(inv_ref[chans])
        zbuf[n % BUFFERS] = to_orders(xn.reshape(SUB * CH, NN), ftbuf[...])
        store_z(n).start()

    for n in range(BUFFERS):
        store_z(NB * T8 - BUFFERS + n).wait()
    for r in others:
        give_stats(r).wait_send()

    @pl.loop(0, SUB)
    def _(g):
        store_p(g).wait()
        store_q(g).wait()

    for g in range(SUB):
        give_p(g).wait()
        if g > 0:
            clear_p(g).wait()


def used(g):
    return rows(SUB * g, NL)


def unused(g):
    return rows(0, SUB * g)


def front(x, p_raw, q_raw, spec_w, base, cid):
    return call(
        front_kernel,
        [(NT, NM, LANES), HALF_TABLE, HALF_TABLE, HALF_TABLE, (NB * CH, LN), (NB * CH, LN), (2 * SUB, LN), (2 * SUB, LN, LN)],
        [
            vmem(NB, CH, NT, NN), vmem(2, CH, CH, NL), vmem(*RAW_TABLE), vmem(*RAW_TABLE), vmem(*HALF_TABLE), vmem(*HALF_TABLE),
            vmem(PAIRS, CH, LN), vmem(NN, LN), vmem(SUB, NN), vmem(PLANE, SUB, NN),
            vmem(BUFFERS, SUB, NM, LN), vmem(NN, NN), vmem(NL, LN), vmem(CH, 2 * SUB, LN),
            dma_sems(NB * PIECES), dma_sems(2), dma_sems(2), dma_sems(3, SUB), dma_sems(4, SUB), dma_sems(2, PLANE),
        ],
        cid=cid,
        in_specs=[ANY, ANY, ANY, ANY, VMEM],
        out_specs=(ANY, ANY, ANY, ANY, VMEM, VMEM, VMEM, VMEM),
        name="front",
    )(x, p_raw, q_raw, spec_w, base)


def table_loader(own, peers, tbuf, sems, y):
    def copy(src, at, g):
        return pltpu.make_async_copy(src.at[at], tbuf.at[g], sems.at[g])

    def start(g):
        at = g % SUB
        away = g // SUB != y

        @pl.when(g // SUB == y)
        def _():
            copy(own, at, g).start()

        first = 0
        for src, count in peers:
            if src is not None:
                @pl.when(away & (at >= first) & (at < first + count))
                def _(src=src, first=first):
                    copy(src, at - first, g).start()
            first += count

    def wait(g):
        copy(own, 0, g).wait()

    return start, wait


def quarters(lo, hi):
    return [(max(lo, 4 * k), min(hi, 4 * k + 4), k) for k in range(4) if max(lo, 4 * k) < min(hi, 4 * k + 4)]


def by_degree(ref, v):
    n = v.shape[0] // SUB
    t = turn(v.reshape(n, SUB, LANES))
    for b in range(NB):
        ref[:, n * b:n * (b + 1)] = t[:, :, LN * b:LN * (b + 1)]


def put_degrees(ref, parts, first, count):
    n = count * SUB
    t = jnp.concatenate([parts[:, n * b:n * (b + 1)] for b in range(NB)], axis=2)
    t = turn(t)
    for i in range(count):
        to = BLOCK * (GROUPS - first - i)
        ref[to:to + BLOCK] = t[SUB * i:SUB * (i + 1)].reshape(BLOCK, LANES)


def near_mask(first, count, pair):
    place = first + lax.broadcasted_iota(jnp.int32, (NB * count * SUB, LN), 0) % (count * SUB) // SUB
    return (place % 2 == 1) & (place < 2 * (pair + 1))


def mix_places(first, count, pair, a_ref, kern_ref, b_ref, a, b):
    rows_in = a_ref[BLOCK * first:BLOCK * (first + count)]
    n = NB * count * SUB
    by_degree(a, rows_in)
    near = near_mask(first, count, pair)

    @pl.loop(0, SUB)
    def _(l):
        al = a[l, :n]
        b[l, :n] = jnp.where(near, dot(al, kern_ref[l]), dot(al, kern_ref[SUB + l]))

    put_degrees(b_ref, b, first, count)


def mix_back_places(first, count, pair, a_ref, db_ref, kern_ref, c0_ref, da_ref, dk_ref, s_ref, a, db, da):
    at = slice(BLOCK * first, BLOCK * (first + count))
    n = count * SUB
    by_degree(a, a_ref[at])
    by_degree(db, db_ref[at])
    near = near_mask(first, count, pair)

    @pl.loop(0, SUB, unroll=UNROLL)
    def _(l):
        al, dl = a[l, :NB * n], db[l, :NB * n]
        v = jnp.where(near, dot(dl, kern_ref[l], NT_DIMS), dot(dl, kern_ref[SUB + l], NT_DIMS))
        da[l, :NB * n] = v
        product = v * al
        s_ref[1:2] += jnp.concatenate([row_sum(product[n * i:n * (i + 1)]) for i in range(NB)], axis=COL)
        if first == 0:
            for row, c0 in ((SUB, l), (0, SUB + l)):
                c0 = jnp.concatenate([c0_ref[pl.ds(c0, 1)]] * NB, axis=COL)
                s_ref[0:1] += c0 * jnp.concatenate([v[n * i + row:n * i + row + 1] for i in range(NB)], axis=COL)
        for i, part in enumerate((jnp.where(near, al, 0.0), jnp.where(near, 0.0, al))):
            g = dot(part, dl, TN_DIMS)
            low = g[CH:]
            dk_ref[i, l] += g[:CH] + jnp.concatenate([low[:, CH:], -low[:, :CH]], axis=COL)

    put_degrees(da_ref, da, first, count)


def analyze_kernel(share, with_q, *refs):
    if with_q:
        t_own, t_peer, z_hbm, q_own, kern_ref, out_ref, mix_ref, q_peer, a_deg, b_deg, qbuf, zeros, s_clear, *rest = refs
        peers = [(t_peer, SUB)]
    else:
        t_own, t_low, t_high, z_hbm, ext_ref, kern_ref, a_ref, c0_ref, mix_ref, dk_ref, a_deg, b_deg, out_ref, s_ref, da_deg, *rest = refs
        peers = [(t_low, LATE), (t_high, EARLY)]
        dk_ref[...] = jnp.zeros_like(dk_ref)
        s_ref[...] = jnp.zeros_like(s_ref)
    tbuf, zbuf, turned, part, sib, rx, ry, fx, fy, s_t, s_z, s_q, s_sib, s_x, s_y, s_fx, s_fy = rest
    count = len(SUM_ENDS)
    mix_after = MIX_AFTER[0 if with_q else 1]
    p = Place()
    x, c, y = p.x, p.c, p.y
    start_t, wait_t = table_loader(t_own, peers, tbuf, s_t, y)

    def load_z(g):
        return pltpu.make_async_copy(z_hbm.at[:, pl.ds(pl.multiple_of(SUB * g, SUB), SUB)], zbuf.at[g], s_z.at[g])

    @pl.loop(0, GROUPS)
    def _(g):
        start_t(g)
        load_z(g).start()

    p.greet([p.sibling, p.xn, p.yn])
    for d in range(PLANE):
        spare = part.at[slot_index(d)]
        spare[STAT:ROWS] = jnp.zeros((ROWS - STAT, LANES), F32)
        if not with_q:
            spare[STAT:GRAD] = ext_ref[SUB * d:SUB * (d + 1)]

    def load_q(g):
        return pltpu.make_async_copy(q_own.at[LATE + g], qbuf.at[g], s_q.at[2, g])

    def give_q(g):
        at = used(LATE + g)
        return send(qbuf.at[g, :, at], q_peer.at[g, :, at], s_q, g, p.yn)

    def clear_q(g):
        at = unused(LATE + g)
        return pltpu.make_async_copy(zeros.at[:, at], q_peer.at[g, :, at], s_clear.at[g])

    def compute(lo, hi, k):
        @pl.loop(lo, hi)
        def _(g):
            wait_t(g)
            load_z(g).wait()
            turned[...] = turn(zbuf[g])

            at_once = AT_ONCE if k < 2 else 2

            @pl.loop(0, SUB, step=at_once)
            def _(some):
                for m in range(at_once):
                    odd, m = m % 2, some + m
                    r = dot(tbuf[g, m // 2][4 * SUB * k:, NT * odd:NT * (odd + 1)], turned[m])
                    for n in range(GROUPS - 4 * k):
                        j = 4 * k + n
                        row = sum_position(j, g) * BLOCK + SUB * m
                        if n < 4:
                            row = jnp.where(j >= g, row, ROWS)
                        xj, cj, yj = place_of_block(j)
                        part[xj, cj, yj, pl.ds(pl.multiple_of(row, SUB), SUB), :] = r[SUB * n:SUB * (n + 1)]

    def to_sibling(i):
        lo, _, hi = chunk(i, share, SUM_ENDS)
        return send(part.at[:, 1 - c, :, rows(lo, hi)], sib.at[:, :, rows(lo, hi)], s_sib, i, p.sibling)

    def to_x(i):
        lo, mid, _ = chunk(i, share, SUM_ENDS)
        return send(part.at[p.ox, c, :, rows(lo, mid)], rx.at[:, rows(lo, mid)], s_x, i, p.xn)

    def to_y(i):
        _, mid, hi = chunk(i, share, SUM_ENDS)
        return send(part.at[:, c, p.oy, rows(mid, hi)], ry.at[:, rows(mid, hi)], s_y, i, p.yn)

    def forward_y(i):
        lo, mid, _ = chunk(i, share, SUM_ENDS)
        return send(part.at[x, c, p.oy, rows(lo, mid)], fy.at[rows(lo, mid)], s_fy, i, p.yn)

    def forward_x(i):
        _, mid, hi = chunk(i, share, SUM_ENDS)
        return send(part.at[p.ox, c, y, rows(mid, hi)], fx.at[rows(mid, hi)], s_fx, i, p.xn)

    def chip_sum(i):
        lo, _, hi = chunk(i, share, SUM_ENDS)
        to_sibling(i).wait_recv()

        @pl.loop(lo, hi, step=2 * SUB)
        def _(row):
            some = pl.ds(pl.multiple_of(row, SUB), 2 * SUB)
            for a in range(2):
                for b in range(2):
                    part[a, c, b, some] += sib[a, b, some]

        to_x(i).start()
        to_y(i).start()
        if with_q and i < EARLY:
            give_q(i).start()

    def add(lo, hi, *sums):
        @pl.loop(lo, hi, step=SUB)
        def _(row):
            some = pl.ds(pl.multiple_of(row, SUB), SUB)
            for to, a, b in sums:
                to[some] = a[some] + b[some]

    def half_sum(i):
        lo, mid, hi = chunk(i, share, SUM_ENDS)
        to_x(i).wait_recv()
        other = part.at[x, c, p.oy]
        add(lo, mid, (other, other, rx.at[p.oy]))
        forward_y(i).start()
        to_y(i).wait_recv()
        other = part.at[p.ox, c, y]
        add(mid, hi, (other, other, ry.at[p.ox]))
        forward_x(i).start()
        mine = part.at[x, c, y]
        add(lo, mid, (out_ref, mine, rx.at[y]))
        add(mid, hi, (out_ref, mine, ry.at[x]))

    def last_sum(i):
        lo, mid, hi = chunk(i, share, SUM_ENDS)
        forward_y(i).wait_recv()
        add(lo, mid, (out_ref, out_ref, fy))
        forward_x(i).wait_recv()
        add(mid, hi, (out_ref, out_ref, fx))

    def mixed(first, end):
        places = end - first
        if with_q:
            mix_places(first, places, p.pair, out_ref, kern_ref, mix_ref, a_deg, b_deg)
        else:
            mix_back_places(first, places, p.pair, a_ref, out_ref, kern_ref, c0_ref, mix_ref, dk_ref, s_ref, a_deg, b_deg, da_deg)

    if with_q:
        zeros[...] = jnp.zeros_like(zeros)
        for g in range(EARLY):
            load_q(g).start()
            clear_q(g).start()
        for g in range(EARLY):
            load_q(g).wait()
    for i in range(count + LAST_LAG):
        if i < count:
            for step in quarters(max(start_of(i, SUM_ENDS) - 1, 0), SUM_ENDS[i] - 1):
                compute(*step)
            to_sibling(i).start()
        if 0 < i <= count:
            chip_sum(i - 1)
        if HALF_LAG <= i < count + HALF_LAG:
            half_sum(i - HALF_LAG)
        if i >= LAST_LAG:
            last_sum(i - LAST_LAG)
            if i - LAST_LAG in mix_after:
                n = mix_after.index(i - LAST_LAG)
                mixed(start_of(n, [SUM_ENDS[m] for m in mix_after]), SUM_ENDS[i - LAST_LAG])
    if with_q:
        mix_ref[STAT:] = jnp.zeros((ROWS - STAT, LANES), F32)
    else:
        mix_ref[STAT:GRAD] = s_ref[...]
        mix_ref[GRAD:] = out_ref[STAT:GRAD]
    for i in range(count):
        for copy in (to_sibling, to_x, to_y, forward_x, forward_y):
            copy(i).wait_send()
    if with_q:
        for g in range(EARLY):
            give_q(g).wait()
            clear_q(g).wait()


HALF_LAG, LAST_LAG = 2, 4
MOST = 8


def analyze(table, z, cid, kern, q_own=None, back=()):
    with_q = q_own is not None
    share = 13 if with_q else 8
    piece = (EARLY, *HALF_TABLE[1:])
    half = vmem(ROWS, LANES)
    pair = vmem(2, ROWS, LANES)
    degrees = vmem(SUB, NB * MOST * SUB, LN)
    if with_q:
        ins, places, outs = (q_own, kern), [ANY, VMEM], [(ROWS, LANES), (ROWS, LANES), piece]
        out_places, more = (VMEM, VMEM, ANY), [vmem(*piece), vmem(PAIRS, CH, LN), dma_sems(EARLY)]
    else:
        ext, a, c0 = back
        ins, places, outs = (ext, kern, a, c0), [VMEM] * 4, [(ROWS, LANES), (2, SUB, CH, LN)]
        out_places, more = (VMEM, VMEM), [half, vmem(SUB, LANES), degrees]
    return call(
        lambda *refs: analyze_kernel(share, with_q, *refs),
        outs,
        [degrees, degrees] + more + [
            vmem(GROUPS, *HALF_TABLE[1:]), vmem(GROUPS, NT, SUB, LANES), vmem(SUB, NT, LANES), vmem(*SLOTS, ROWS + SPARE, LANES),
            vmem(*SLOTS[1:], ROWS, LANES), pair, pair, half, half,
            dma_sems(GROUPS), dma_sems(GROUPS), dma_sems(3, EARLY),
        ] + [dma_sems(2, len(SUM_ENDS))] * 5,
        cid=cid,
        in_specs=[ANY] * len(table) + [ANY] + places,
        out_specs=out_places,
        name=f"analyze_{cid}",
    )(*table, z, *ins)


class Gather:
    def __init__(self, p, own_ref, ball, sems):
        self.p, self.own_ref, self.ball, self.sems = p, own_ref, ball, sems

    def relay(self, piece, n, to, a, b, part, src=None):
        i, lo, mid, hi, lanes = piece
        at = (rows(lo, hi), rows(lo, mid), rows(mid, hi))[part]
        here = self.ball.at[a, self.p.c, b, at, lanes]
        return send(here if src is None else src.at[at, lanes], here, self.sems[n], i, to)

    def own(self, piece, n, to):
        return self.relay(piece, n, to, self.p.x, self.p.y, 0, self.own_ref)

    def own_x(self, piece):
        return self.own(piece, 0, self.p.xn)

    def own_y(self, piece):
        return self.own(piece, 1, self.p.yn)

    def own_s(self, piece):
        return self.own(piece, 2, self.p.sibling)

    def diagonal_y(self, piece):
        return self.relay(piece, 3, self.p.yn, self.p.ox, self.p.y, 1)

    def diagonal_x(self, piece):
        return self.relay(piece, 4, self.p.xn, self.p.x, self.p.oy, 2)

    def sibling_x(self, piece):
        return self.relay(piece, 5, self.p.sibling, self.p.ox, self.p.y, 0)

    def sibling_y(self, piece):
        return self.relay(piece, 6, self.p.sibling, self.p.x, self.p.oy, 0)

    def sibling_d(self, piece):
        return self.relay(piece, 7, self.p.sibling, self.p.ox, self.p.oy, 0)

    def give(self, piece):
        for copy in (self.own_x, self.own_y, self.own_s):
            copy(piece).start()

    def pass_on(self, piece):
        self.own_x(piece).wait_recv()
        self.diagonal_y(piece).start()
        self.own_y(piece).wait_recv()
        self.diagonal_x(piece).start()
        self.sibling_x(piece).start()
        self.sibling_y(piece).start()

    def collect(self, piece):
        self.diagonal_y(piece).wait_recv()
        self.diagonal_x(piece).wait_recv()
        self.sibling_d(piece).start()

    def complete(self, piece):
        for copy in (self.own_s, self.sibling_x, self.sibling_y, self.sibling_d):
            copy(piece).wait_recv()

    def finish(self, piece):
        for copy in (
            self.own_x, self.own_y, self.own_s, self.diagonal_y, self.diagonal_x,
            self.sibling_x, self.sibling_y, self.sibling_d,
        ):
            copy(piece).wait_send()


def inverse_sums(table, ball, turned, g, k, lanes, at_once):
    @pl.loop(0, SUB, step=at_once)
    def _(some):
        for m in range(at_once):
            odd, m = m % 2, some + m
            if not odd:
                both = table(g, m // 2)
            tiles = []
            for n in range(GROUPS - 4 * k):
                j = 4 * k + n
                row = (GROUPS - sum_position(j, g)) * BLOCK + SUB * m
                if n < 4:
                    row = jnp.where(j >= g, row, ROWS)
                xj, cj, yj = place_of_block(j)
                tiles.append(ball[xj, cj, yj, pl.ds(pl.multiple_of(row, SUB), SUB), lanes])
            turned[m] = dot(both[NT * odd:NT * (odd + 1), 4 * SUB * k:], jnp.concatenate(tiles, axis=ROW))


ALL = pl.ds(0, LANES)


def synth_kernel(t_own, t_peer, own_ref, dk_ref, u_hbm, ext_ref, spec_ref, tbuf, ubuf, turned, ball, zin, kin, zg,
                 s_t, s_u, s_zk, s_zg, s_kin, s_kz, *sems):
    p = Place()
    x, c, y = p.x, p.c, p.y
    start_t, wait_t = table_loader(t_own, [(t_peer, SUB)], tbuf, s_t, y)
    count = len(GATHER_ENDS)

    def store_u(g):
        return pltpu.make_async_copy(ubuf.at[g], u_hbm.at[:, pl.ds(pl.multiple_of(SUB * g, SUB), SUB)], s_u.at[g])

    @pl.loop(0, GROUPS)
    def _(g):
        start_t(g)

    above = [{"dp": (p.z + r) % Z} for r in range(1, Z)]
    partner = [{"h": 3 - p.h}, {"h": 3 - p.h, "w": p.oy}]
    p.greet([p.sibling, p.xn, p.yn, *above, *partner])

    others = range(Z - 1)
    early = Gather(p, own_ref, ball, sems)
    late = Gather(p, ball.at[x, c, y], ball, sems)

    def piece(i):
        return i, *chunk(i, SUB, GATHER_ENDS), ALL

    def gather(i):
        return late if i == count - 1 else early

    quarter = pl.ds(2 * p.z, 2)

    def grads_z(r):
        return send(own_ref.at[GRAD:ROWS], zg.at[r], s_zg, r, above[r])

    def dk_z(r):
        return send(dk_ref.at[:, pl.ds(2 * ((p.z + 1 + r) % Z), 2)], zin.at[r], s_zk, r, above[r])

    stay = jnp.where(p.low, 0, 1)
    kept = jnp.where(p.low, p.pair, GROUPS - 1 - p.pair) % 4
    given = jnp.where(p.low, GROUPS - 1 - p.pair, p.pair) % 4

    def dk_plane(r):
        to = (p.yn, *partner)[r]
        src = kin.at[stay] if r == 0 else kin.at[1 - stay]
        return send(src, spec_ref.at[kept if r == 0 else given, quarter], s_kin, r, to)

    def dk_up(r):
        return send(spec_ref.at[:, quarter], spec_ref.at[:, quarter], s_kz, r, above[r])

    def compute(lo, hi, k):
        @pl.loop(0, hi - lo)
        def _(n):
            g = hi - 1 - n
            wait_t(g)
            inverse_sums(lambda g, i: tbuf[g, i].T, ball, turned, g, k, ALL, SUB if k > 0 else AT_ONCE)
            ubuf[g] = turn(turned[...])
            store_u(g).start()

    for r in others:
        grads_z(r).start()
        dk_z(r).start()
    for i in range(2):
        gather(i).give(piece(i))
    ball[x, c, y, 0:ROWS] = own_ref[...]
    for d in range(PLANE):
        ball[*slot_index(d), ROWS:] = jnp.zeros((SPARE, LANES), F32)
    for i in range(count + 2):
        if i < count:
            gather(i).pass_on(piece(i))
        if i == 1:
            for r in others:
                grads_z(r).wait_recv()
                ball[x, c, y, GRAD:ROWS] += zg[r]
        if i == 2:
            for r in others:
                dk_z(r).wait_recv()
            kin[...] = dk_ref[:, quarter] + zin[0] + zin[1] + zin[2]
            for r in others:
                dk_plane(r).start()
            spec_ref[kept, quarter] = kin[stay]
        if i == 3:
            for r in others:
                dk_plane(r).wait_recv()
            for r in others:
                dk_up(r).start()
        if i < count - 2:
            gather(i + 2).give(piece(i + 2))
        if 0 < i < count:
            gather(i - 1).collect(piece(i - 1))
        if i > 1:
            gather(i - 2).complete(piece(i - 2))
            for step in reversed(quarters(max(GROUPS - GATHER_ENDS[i - 2], 0), GROUPS - start_of(i - 2, GATHER_ENDS))):
                compute(*step)
        if i == count:
            gather(i - 1).collect(piece(i - 1))
    for d in range(PLANE):
        ext_ref[d] = ball[*slot_index(d), STAT:ROWS]
    for i in range(count):
        gather(i).finish(piece(i))
    for r in others:
        grads_z(r).wait_send()
        dk_z(r).wait_send()
        dk_plane(r).wait_send()
        dk_up(r).wait()

    @pl.loop(0, GROUPS)
    def _(g):
        store_u(g).wait()


def synth(table, own, cid, dk):
    quarter = (*SLOTS[1:], CH, LN)
    return call(
        synth_kernel,
        [(NT, NM, LANES), (PLANE, 2 * SUB, LANES), (4, SUB, CH, LN)],
        [
            vmem(GROUPS, *HALF_TABLE[1:]), vmem(GROUPS, NT, SUB, LANES), vmem(SUB, NT, LANES), vmem(*SLOTS, ROWS + SPARE, LANES),
            vmem(NB, *quarter), vmem(*quarter), vmem(NB, SUB, LANES), dma_sems(GROUPS), dma_sems(GROUPS),
        ] + [dma_sems(2, NB)] * 4 + [dma_sems(2, len(GATHER_ENDS))] * 8,
        cid=cid,
        in_specs=[ANY, ANY, VMEM, VMEM],
        out_specs=(ANY, VMEM, VMEM),
        name=f"synth_{cid}",
    )(*table, own, dk)


WIDE = SUB * NN
BT = 2 * SUB
PER = NT // BT
FIRST = 9 * BLOCK


def grid_stage(n, orders, x, tgt, q_ref, weights, dout, dz, grads_ref, scratch):
    g_ref, gt_ref, w1_ref, w2t_ref = weights
    some = range(BT // SUB)
    ts = [slice(SUB * k, SUB * (k + 1)) for k in some]

    def columns(t):
        return slice(NN * t, NN * (t + 1))

    def wide(v):
        return jnp.concatenate([v[t] for t in range(SUB)], axis=COL)

    line, yb, hid, act, db, dh = ([ref.at[k] for k in some] for ref in scratch)
    for k in some:
        y = to_grid(orders[k][...], g_ref[...]).reshape(SUB, CH, NN)
        r0 = turn(x[:, ts[k]] - tgt[:, ts[k]])
        line[k][...] = wide(r0 + y)
        yb[k][...] = wide(y).astype(BF16)
    for k in some:
        hid[k][...] = mxu(w1_ref[...], yb[k][...], TN_DIMS)
        for t in range(SUB):
            h = hid[k][:, columns(t)]
            h2 = h * h
            th = jnp.tanh(h * (GELU_A + (GELU_A * GELU_B) * h2))
            cdf = HALF + HALF * th
            act[k][:, columns(t)] = (h * cdf).astype(BF16)
            hid[k][:, columns(t)] = cdf + (HALF * h) * (1.0 - th * th) * (GELU_A + (3.0 * GELU_A * GELU_B) * h2)
    for k in some:
        res = line[k][...] + mxu(w2t_ref[...], act[k][...])
        first = n % PER * BT + SUB * k
        d = jnp.concatenate([jnp.full((1, NN), q_ref[first + t], F32) for t in range(SUB)], axis=COL) * res
        line[k][...] = d
        db[k][...] = d.astype(BF16)
        loss = jnp.sum((d * res).reshape(SUB, SUB, WIDE), axis=ROW)
        grads_ref[:SUB, 2 * LN:] += sum(loss[:, LN * i:LN * (i + 1)] for i in range(WIDE // LN))
        for t in range(SUB):
            dout[SUB * k + t] = line[k][:, columns(t)]
    for k in some:
        dh[k][...] = (mxu(w2t_ref[...], db[k][...], TN_DIMS) * hid[k][...]).astype(BF16)
        grads_ref[:, :LN] += mxu(yb[k][...], dh[k][...], NT_DIMS)
        grads_ref[:, LN:2 * LN] += mxu(db[k][...], act[k][...], NT_DIMS)
    for k in some:
        dy = line[k][...] + mxu(w1_ref[...], dh[k][...])
        dys = jnp.concatenate([dy[:, columns(t)] for t in range(SUB)], axis=ROW)
        dz[ts[k]] = to_orders(dys, gt_ref[...])


def forward_kernel(t_own, t_high, own_ref, x_hbm, tgt_hbm, q_ref, base_ref, w1_ref, w2t_ref, dout_hbm, dz_hbm, q_low, grads_ref,
                   tbuf, across, ubuf, turned, ball, xbuf, tgtbuf, dbuf, zbuf, g_ref, gt_ref, line, yb, hid, act, db, dh,
                   s_t, s_in, s_out, s_q, s_low, *sems):
    p = Place()
    y = p.y
    start_t, wait_local = table_loader(t_own, [(None, LATE), (t_high, EARLY)], tbuf, s_t, y)
    gather = Gather(p, own_ref, ball, sems)
    share = 2

    def lanes(s):
        return pl.ds(pl.multiple_of(LN * s, LN), LN)

    def piece(s, half):
        lo, hi = ((0, FIRST), (FIRST, ROWS))[half]
        return 2 * s + half, lo, lo + (hi - lo) * share // BLOCK * SUB, hi, lanes(s)

    def each(step, s):
        for half in range(2):
            step(piece(s, half))

    def block(n):
        return n // PER, pl.ds(pl.multiple_of(n % PER * BT, BT), BT)

    def loads(n):
        b, t = block(n)
        return [
            pltpu.make_async_copy(src.at[b, :, t], dst.at[n % BUFFERS], s_in.at[i, n % BUFFERS])
            for i, (src, dst) in enumerate(((x_hbm, xbuf), (tgt_hbm, tgtbuf)))
        ]

    def stores(n):
        b, t = block(n)
        return [
            pltpu.make_async_copy(dbuf.at[n % BUFFERS], dout_hbm.at[b, t], s_out.at[0, n % BUFFERS]),
            pltpu.make_async_copy(zbuf.at[n % BUFFERS], dz_hbm.at[t, :, lanes(b)], s_out.at[1, n % BUFFERS]),
        ]

    def give_q(g):
        return send(tbuf.at[SUB * y + g], tbuf.at[SUB * y + g], s_q, g, p.yn)

    def store_low(g):
        return pltpu.make_async_copy(tbuf.at[SUB * p.oy + g], q_low.at[g], s_low.at[g])

    @pl.loop(0, GROUPS)
    def _(g):
        start_t(g)

    p.greet([p.sibling, p.xn, p.yn])
    each(gather.give, 0)
    for copy in loads(0):
        copy.start()
    ball[p.x, p.c, y, :ROWS] = own_ref[...]
    for d in range(PLANE):
        ball[*slot_index(d), ROWS:] = jnp.zeros((SPARE, LANES), F32)
    grads_ref[...] = jnp.zeros_like(grads_ref)
    gt_ref[...] = signed(base_ref, y, 2)
    g_ref[...] = gt_ref[...].T
    def across_table(g):
        for i in range(PAIRS):
            across[g, i] = tbuf[g, i].T

    @pl.loop(0, GROUPS)
    def _(g):
        at = g % SUB

        @pl.when((at >= LATE) | (g // SUB == y))
        def _():
            wait_local(g)
            across_table(g)

    each(gather.pass_on, 0)
    for g in reversed(range(LATE)):
        give_q(g).start()
    each(gather.give, 1)
    each(gather.collect, 0)

    @pl.loop(0, NB)
    def _(s):
        each(gather.complete, s)
        for k in reversed(range(4)):
            @pl.loop(0, 4)
            def _(n):
                g = 4 * k + 3 - n
                at = g % SUB

                @pl.when((s == 0) & (at < LATE) & (g // SUB != y))
                def _():
                    give_q(at).wait_recv()
                    store_low(at).start()
                    across_table(g)

                inverse_sums(lambda g, i: across[g, i], ball, turned, g, k, lanes(s), SUB)
                ubuf[:, pl.ds(pl.multiple_of(SUB * g, SUB), SUB)] = turn(turned[...])

        @pl.loop(0, PER)
        def _(i):
            n = s * PER + i
            for copy in loads(n):
                copy.wait()

            @pl.when(n + 1 < NB * PER)
            def _():
                for copy in loads(n + 1):
                    copy.start()

            @pl.when(n >= BUFFERS)
            def _():
                for copy in stores(n - BUFFERS):
                    copy.wait()

            orders = [ubuf.at[pl.ds(pl.multiple_of(i * BT + SUB * k, SUB), SUB)] for k in range(BT // SUB)]
            grid_stage(
                n, orders, xbuf.at[n % BUFFERS], tgtbuf.at[n % BUFFERS], q_ref, (g_ref, gt_ref, w1_ref, w2t_ref),
                dbuf.at[n % BUFFERS], zbuf.at[n % BUFFERS], grads_ref, (line, yb, hid, act, db, dh),
            )
            for copy in stores(n):
                copy.start()

            @pl.when((i == 0) & (s + 1 < NB))
            def _():
                each(gather.pass_on, s + 1)

            @pl.when((i == 0) & (s + 2 < NB))
            def _():
                each(gather.give, s + 2)

            @pl.when((i == 2) & (s + 1 < NB))
            def _():
                each(gather.collect, s + 1)

    for n in range(BUFFERS):
        for copy in stores(NB * PER - BUFFERS + n):
            copy.wait()

    @pl.loop(0, NB)
    def _(s):
        each(gather.finish, s)

    for g in range(LATE):
        give_q(g).wait_send()
        store_low(g).wait()


def forward(table, own, x, target, q, base, w1, w2t, cid):
    hid = 2 * CH
    grid, two = (BUFFERS, CH, BT, NN), BT // SUB
    return call(
        forward_kernel,
        [(NB, NT, CH, NN), (NT, NM, LANES), (LATE, *HALF_TABLE[1:]), (CH, LANES)],
        [
            vmem(GROUPS, *HALF_TABLE[1:]), vmem(GROUPS, *HALF_TABLE[1:]), vmem(NT, NM, LN), vmem(SUB, NT, LN), vmem(*SLOTS, ROWS + SPARE, LANES),
            vmem(*grid), vmem(*grid), vmem(BUFFERS, BT, CH, NN), vmem(BUFFERS, BT, NM, LN), vmem(NN, NN), vmem(NN, NN),
            vmem(two, CH, WIDE), vmem(two, CH, WIDE, dtype=BF16), vmem(two, hid, WIDE), vmem(two, hid, WIDE, dtype=BF16),
            vmem(two, CH, WIDE, dtype=BF16), vmem(two, hid, WIDE, dtype=BF16),
            dma_sems(GROUPS), dma_sems(2, BUFFERS), dma_sems(2, BUFFERS), dma_sems(2, LATE), dma_sems(LATE),
        ] + [dma_sems(2, 2 * NB)] * 8,
        cid=cid,
        in_specs=[ANY, ANY, VMEM, ANY, ANY, SMEM, VMEM, VMEM, VMEM],
        out_specs=(ANY, ANY, ANY, VMEM),
        name="forward",
    )(*table, own, x, target, q, base, w1, w2t)


def blocks(nt):
    return (
        pl.BlockSpec((1, CH, nt, NN), lambda b, t: (b, 0, t, 0)),
        pl.BlockSpec((1, nt, CH, NN), lambda b, t: (b, t, 0, 0)),
        pl.BlockSpec((nt, NM, LN), lambda b, t: (t, 0, b)),
    )


CHAN_SPEC = pl.BlockSpec((CH, LN), lambda b, t: (b, 0))
FINAL_T = 4 * SUB

def whole(*shape):
    return pl.BlockSpec(shape, lambda b, t: (0,) * len(shape))


def first_step():
    return (pl.program_id(0) == 0) & (pl.program_id(1) == 0)


def final_kernel(u_ref, x_ref, dout_ref, mu_ref, inv_ref, ext_ref, spec_ref, base_ref, out_ref, gspec_ref, gw1_ref, gw2t_ref, loss_ref,
                 g_ref, s0_ref, s1_ref):
    @pl.when(first_step())
    def _():
        g_ref[...] = signed(base_ref, Place().y, 1).T
        gspec_ref[0] = spec_ref[:, :, :CH]
        gspec_ref[1] = spec_ref[:, :, CH:]
        grads = ext_ref[:, SUB:].reshape(CH, LANES)
        gw1_ref[...] = grads[:, :LN]
        gw2t_ref[...] = grads[:, LN:2 * LN]
        loss = block_sum(grads[None, :SUB, 2 * LN:])[0] / TOTAL
        loss_ref[...] = loss
        sums = sum(ext_ref[n, :SUB] for n in range(PLANE)) / POINTS
        for b in range(NB):
            chans, lanes = slice(CH * b, CH * (b + 1)), slice(LN * b, LN * (b + 1))
            s0, s1 = (jnp.broadcast_to(sums[n:n + 1, lanes], (LN, LN)).T for n in range(2))
            s0_ref[chans] = s0[:CH]
            s1_ref[chans] = s1[:CH] + s1[CH:]

    chans = pl.ds(pl.multiple_of(pl.program_id(0) * CH, CH), CH)
    inv = col(inv_ref[...])
    slope = inv_ref[...] * inv_ref[...] * s1_ref[chans]

    @pl.loop(0, FINAL_T // SUB)
    def _(k):
        ts = pl.ds(pl.multiple_of(SUB * k, SUB), SUB)
        dn = to_grid(u_ref[ts], g_ref[...]).reshape(SUB, CH, NN)
        r = turn(dout_ref[0, ts] + inv * (dn - col(s0_ref[chans])))
        for c in range(CH):
            for n in range(NN // LN):
                lanes = slice(LN * n, LN * (n + 1))
                out_ref[0, c, ts, lanes] = r[c, :, lanes] - (x_ref[0, c, ts, lanes] - mu_ref[c:c + 1]) * slope[c:c + 1]


def final(u, x, dout, mu, inv, ext, spec, base):
    hid = 2 * CH
    degrees = NL // 4
    grid, lines, orders = blocks(FINAL_T)
    return call(
        final_kernel,
        [(NB, CH, NT, NN), (2, degrees, CH, CH), (CH, hid), (CH, hid), (1, 1)],
        [vmem(NN, NN), vmem(NB * CH, LN), vmem(NB * CH, LN)],
        grid=(NB, NT // FINAL_T),
        in_specs=[
            orders, grid, lines, CHAN_SPEC, CHAN_SPEC,
            whole(PLANE, 2 * SUB, LANES), whole(degrees, CH, LN), whole(4, DFT_STEP, NM),
        ],
        out_specs=(grid, whole(2, degrees, CH, CH), whole(CH, hid), whole(CH, hid), whole(1, 1)),
        name="final",
    )(u, x, dout, mu, inv, ext, spec.reshape(degrees, CH, LN), base)


def solution(mesh):
    def local_step(x, target, q, leg_fwd, leg_inv, spec_w, w1, w2):
        base = jnp.asarray(dft_tables())
        p_raw, q_raw = (jnp.swapaxes(v, 1, 2).reshape(RAW_TABLE) for v in (leg_fwd, leg_inv))
        z, p_own, p_peer, q_own, mu, inv, c0, kern = front(x, p_raw, q_raw, jnp.moveaxis(spec_w, 1, 3), base, 0)
        a, b, q_high = analyze((p_own, p_peer), z, 1, kern, q_own=q_own)
        dout, dz, q_low, grads = forward((q_own, q_high), b, x, target, q, base, w1, w2.T, 2)
        da, dk = analyze((q_own, q_low, q_high), dz, 3, kern, back=(grads, a, c0))
        du, ext, spec = synth((p_own, p_peer), da, 4, dk)
        d_field, grad_spec, gw1, gw2t, loss = final(du, x, dout, mu, inv, ext, spec, base)
        return loss.reshape(()), d_field, grad_spec, gw1, gw2t.T

    grid_spec = P("dp", None, "h", "w")
    table_spec = P("w", None, "h")
    return jax.shard_map(
        local_step,
        mesh=mesh,
        in_specs=(grid_spec, grid_spec, P("h"), table_spec, table_spec, P(), P(), P()),
        out_specs=(P(), grid_spec, P(None, "h"), P(), P()),
        check_vma=False,
    )
```

```python
import math
import numpy as np
import jax
import jax.numpy as jnp
from jax import lax
from jax.experimental import pallas as pl
from jax.experimental.pallas import tpu as pltpu
from jax.sharding import PartitionSpec as P

NORM_EPS = 1e-5
HI = lax.Precision.HIGHEST
F32 = jnp.float32
BF16 = jnp.bfloat16
MESH = pl.DeviceIdType.MESH
GELU_A = math.sqrt(2.0 / math.pi)
GELU_B = 0.044715

ROW, COL = 0, 1
NB, CH, NT, NN = 3, 64, 64, 256
NM, NL = 128, 128
DFT_STEP = 16
BUFFERS = 2
HALF = 0.5
LON, LAT, BATCH = 512, 256, 12
POINTS = LON * LAT
TOTAL = POINTS * BATCH * CH
LANES = NB * 2 * CH
SUB, LN = 8, 128
T8 = NT // SUB
GROUPS = NM // SUB
PLANE, Z = 8, 4
PAIRS = SUB // 2
FIRST_GROUPS = 3
H_OF_PAIR = (0, 0, 3, 3, 1, 1, 2, 2)
BLOCK = SUB * SUB
PLACES = GROUPS + 1
DATA = PLACES * BLOCK
STAT = DATA
GRAD = DATA + SUB
ROWS = GRAD + SUB
SPARE = BLOCK
SLOTS = (2, 2, 2)
AT_ONCE = 4
UNROLL = 2
LATE = 2
EARLY = SUB - LATE
NN_DIMS, NT_DIMS, TN_DIMS = ((1,), (0,)), ((1,), (1,)), ((0,), (0,))
SUM_ENDS = (2, 5, 8, 11, 14, 16, 17)
GATHER_ENDS = (3, 6, 9, 12, 15, 17)
MIX_AFTER = (2, 3, 4, 6)

SMEM = pl.BlockSpec(memory_space=pltpu.SMEM)
VMEM = pl.BlockSpec(memory_space=pltpu.VMEM)
ANY = pl.BlockSpec(memory_space=pl.ANY)


def dot(a, b, dims=NN_DIMS):
    return lax.dot_general(a, b, (dims, ((), ())), precision=HI, preferred_element_type=F32)


def mxu(a, b, dims=NN_DIMS):
    return lax.dot_general(a, b, (dims, ((), ())), preferred_element_type=F32)


def call(kernel, outs, scratch=(), cid=None, **kw):
    extra = {} if cid is None else {"collective_id": cid, "has_side_effects": True}
    return pl.pallas_call(
        kernel,
        out_shape=tuple(jax.ShapeDtypeStruct(s, F32) for s in outs),
        scratch_shapes=list(scratch),
        compiler_params=pltpu.CompilerParams(vmem_limit_bytes=62 << 20, **extra),
        **kw,
    )


def vmem(*shape, dtype=F32):
    return pltpu.VMEM(shape, dtype)


def dma_sems(*shape):
    return pltpu.SemaphoreType.DMA(shape)


def row_sum(v):
    return jnp.sum(v, axis=ROW, keepdims=True)


def block_sum(v):
    return jnp.sum(jnp.sum(v, axis=COL, keepdims=True), axis=COL + 1, keepdims=True)


def col(v):
    return v[:, :1]


def turn(v):
    return jnp.swapaxes(v, ROW, COL)


def rows(lo, hi):
    return pl.ds(lo, hi - lo)


def dft_tables():
    small = np.arange(DFT_STEP)[:, None] * np.arange(NM)[None]
    coarse, fine = (np.exp(-2j * np.pi * (v % LON) / LON) for v in (DFT_STEP * small, small))
    coarse = coarse / math.sqrt(LON)
    return np.stack([coarse.real, coarse.imag, fine.real, fine.imag]).astype(np.float32)


def signed(tables, half, weight):
    fine_re, fine_im = tables[2], tables[3]
    lines = []
    for n in range(DFT_STEP):
        re, im = tables[0, n:n + 1], tables[1, n:n + 1]
        lines.append(jnp.concatenate([re * fine_re - im * fine_im, re * fine_im + im * fine_re], axis=COL))
    out = jnp.concatenate(lines, axis=ROW)
    m = lax.broadcasted_iota(jnp.int32, out.shape, 1) % NM
    out = jnp.where((m % 2) * half == 1, -out, out)
    return jnp.where(m == 0, out, weight * out) if weight > 1 else out


def to_orders(lines, ft):
    z = dot(lines, ft).reshape(SUB, CH, NN)
    z = jnp.concatenate([z[:, :, :NM], z[:, :, NM:]], axis=COL)
    return jnp.swapaxes(z, 1, 2)


def to_grid(orders, ft):
    u = jnp.swapaxes(orders, 1, 2)
    u = jnp.concatenate([u[:, :CH, :], u[:, CH:, :]], axis=2).reshape(SUB * CH, NN)
    return dot(u, ft)


def place_of_block(j):
    k = min(j, GROUPS - 1 - j)
    return H_OF_PAIR[k] // 2, H_OF_PAIR[k] % 2, k % 2


def slot_index(d):
    return d // 4, d // 2 % 2, d % 2


def sum_position(j, g):
    k = min(j, GROUPS - 1 - j)
    return 2 * g + 1 if j < SUB else jnp.where(g <= k, 2 * g, k + 1 + g)


def start_of(i, ends):
    return ends[i - 1] if i > 0 else 0


def chunk(i, share, ends, last=ROWS):
    lo = start_of(i, ends) * BLOCK
    hi = ends[i] * BLOCK if ends[i] < PLACES else last
    return lo, lo + (hi - lo) * share // (2 * BLOCK) * SUB, hi


class Place:
    def __init__(self):
        self.h, self.y, self.z = lax.axis_index("h"), lax.axis_index("w"), lax.axis_index("dp")
        self.x, self.c = self.h // 2, self.h % 2
        self.slot = 2 * self.h + self.y
        self.low = self.h < 2
        self.pair = jnp.where(self.low, 4 * self.h, 14 - 4 * self.h) + self.y
        self.ox, self.oy = 1 - self.x, 1 - self.y
        self.sibling = {"h": 2 * self.x + 1 - self.c}
        self.xn = {"h": 2 * self.ox + self.c}
        self.yn = {"w": self.oy}

    def plane(self, r):
        s = (self.slot + r) % PLANE
        return {"h": s // 2, "w": s % 2}

    def greet(self, others):
        barrier = pltpu.get_barrier_semaphore()
        for other in others:
            pl.semaphore_signal(barrier, inc=1, device_id=other, device_id_type=MESH)
        pl.semaphore_wait(barrier, len(others))


def send(src, dst, sems, i, to):
    return pltpu.make_async_remote_copy(
        src_ref=src, dst_ref=dst, send_sem=sems.at[0, i], recv_sem=sems.at[1, i], device_id=to, device_id_type=MESH
    )


CB = 16
PIECES = CH // CB
RAW_TABLE = (SUB, SUB, NT, NL)
HALF_TABLE = (SUB, PAIRS, NL, LN)


def near_far(k):
    return pl.ds(pl.multiple_of(SUB * k, SUB), SUB), pl.ds(pl.multiple_of(SUB * (GROUPS - 1 - k), SUB), SUB)


def front_kernel(x_hbm, p_hbm, q_hbm, w_hbm, base_ref, z_hbm, p_own, p_peer, q_own, mu_ref, inv_ref, c0_ref, kern_ref,
                 xbuf, wbuf, pbuf, qbuf, ppack, qpack, zeros, cols, pay, sbuf, zbuf, ftbuf, turned, own, s_x, s_w, s_z, s_p, s_q, s_st):
    place = Place()
    near, far = near_far(place.pair)

    def load_x(n):
        b, part = n // PIECES, pl.ds(n % PIECES * CB, CB)
        return pltpu.make_async_copy(x_hbm.at[b, part], xbuf.at[b, part], s_x.at[n])

    def load_w(i):
        return pltpu.make_async_copy(w_hbm.at[i], wbuf.at[i], s_w.at[i])

    def load_p(g):
        return pltpu.make_async_copy(p_hbm.at[g], pbuf.at[g], s_p.at[2, g])

    def load_q(g):
        return pltpu.make_async_copy(q_hbm.at[g], qbuf.at[g], s_q.at[0, g])

    def store_p(g):
        return pltpu.make_async_copy(ppack.at[g], p_own.at[g], s_q.at[1, g])

    def store_q(g):
        return pltpu.make_async_copy(qpack.at[g], q_own.at[g], s_q.at[2, g])

    def give_p(g):
        return send(ppack.at[g, :, used(g)], p_peer.at[g, :, used(g)], s_p, g, place.yn)

    def clear_p(g):
        return pltpu.make_async_copy(zeros.at[:, unused(g)], p_peer.at[g, :, unused(g)], s_q.at[3, g])

    def pack(src, dst, g):
        for i in range(PAIRS):
            dst[g, i] = jnp.concatenate([src[g, 2 * i + n] for n in range(2)], axis=ROW).T

    @pl.loop(0, SUB)
    def _(g):
        load_p(g).start()

    @pl.loop(0, NB * PIECES)
    def _(n):
        load_x(n).start()

    for i in range(2):
        load_w(i).start()

    @pl.loop(0, SUB)
    def _(g):
        load_q(g).start()

    others = range(1, PLANE)
    place.greet([place.plane(r) for r in others])

    zeros[...] = jnp.zeros_like(zeros)
    for g in range(1, SUB):
        clear_p(g).start()

    def offer(lo, hi):
        @pl.loop(lo, hi)
        def _(g):
            load_p(g).wait()
            pack(pbuf, ppack, g)
            store_p(g).start()

        for g in range(lo, hi):
            give_p(g).start()

    offer(0, 1)
    cols[...] = jnp.zeros_like(cols)

    @pl.loop(0, NB * PIECES)
    def _(n):
        load_x(n).wait()
        v = xbuf[n // PIECES, pl.ds(n % PIECES * CB, CB)]
        mean = block_sum(v) / (NT * NN)
        diff = v - mean
        m2 = block_sum(diff * diff)
        lane = lax.broadcasted_iota(jnp.int32, (CB, 1, LN), 2)
        cols[pl.ds(pl.multiple_of(n * CB, CB), CB)] = jnp.where(lane < CH, mean, m2).reshape(CB, LN)
    wide = cols[...].T
    p1 = jnp.where(place.y == 0, row_sum(pbuf[0, 0]), 0.0)
    pay[...] = jnp.concatenate([
        *(wide[n:n + 1] for n in (0, CH)), jnp.concatenate([p1, p1], axis=COL), jnp.zeros((SUB - 3, NN), F32)
    ], axis=ROW)

    def give_stats(r):
        return send(pay, sbuf.at[place.slot], s_st, r, place.plane(r))

    for r in others:
        give_stats(r).start()
    offer(1, SUB)
    sbuf[place.slot] = pay[...]
    ftbuf[...] = signed(base_ref, place.y, 1)

    @pl.loop(0, SUB)
    def _(g):
        load_q(g).wait()
        pack(qbuf, qpack, g)
        store_q(g).start()

    for i in range(2):
        load_w(i).wait()

    @pl.loop(0, CH)
    def _(i):
        turned[...] = jnp.concatenate([wbuf[n, i] for n in range(2)], axis=ROW).T
        own[i, :SUB] = turned[near]
        own[i, SUB:] = turned[far]

    top = turn(own[...])
    kern_ref[:, :CH] = top
    kern_ref[:, CH:] = jnp.concatenate([-top[:, :, CH:], top[:, :, :CH]], axis=2)

    for r in others:
        give_stats(r).wait_recv()
    means, m2s, p1s = (jnp.concatenate([sbuf[s, n:n + 1] for s in range(PLANE)], axis=ROW) for n in range(3))
    mu = row_sum(means) / PLANE
    dev = means - mu
    var = (row_sum(m2s) + (NT * NN) * row_sum(dev * dev)) / POINTS
    c0 = math.sqrt(LON) * row_sum(p1s)
    mu_ref[...], inv_ref[...], turned[...] = (
        jnp.broadcast_to(v, (LN, NN)).T[:n] for v, n in ((mu, NB * CH), (lax.rsqrt(var + NORM_EPS), NB * CH), (c0, NL))
    )
    c0_ref[:SUB] = turned[near]
    c0_ref[SUB:] = turned[far]

    def store_z(n):
        t = pl.multiple_of(n % T8 * SUB, SUB)
        lanes = pl.multiple_of(n // T8 * LN, LN)
        return pltpu.make_async_copy(zbuf.at[n % BUFFERS], z_hbm.at[pl.ds(t, SUB), :, pl.ds(lanes, LN)], s_z.at[n % BUFFERS])

    @pl.loop(0, NB * T8)
    def _(n):
        @pl.when(n >= BUFFERS)
        def _():
            store_z(n - BUFFERS).wait()

        b = n // T8
        xt = turn(xbuf[b, :, pl.ds(pl.multiple_of(n % T8 * SUB, SUB), SUB), :])
        chans = pl.ds(pl.multiple_of(b * CH, CH), CH)
        xn = (xt - col(mu_ref[chans])) * col(inv_ref[chans])
        zbuf[n % BUFFERS] = to_orders(xn.reshape(SUB * CH, NN), ftbuf[...])
        store_z(n).start()

    for n in range(BUFFERS):
        store_z(NB * T8 - BUFFERS + n).wait()
    for r in others:
        give_stats(r).wait_send()

    @pl.loop(0, SUB)
    def _(g):
        store_p(g).wait()
        store_q(g).wait()

    for g in range(SUB):
        give_p(g).wait()
        if g > 0:
            clear_p(g).wait()


def used(g):
    return rows(SUB * g, NL)


def unused(g):
    return rows(0, SUB * g)


def front(x, p_raw, q_raw, spec_w, base, cid):
    return call(
        front_kernel,
        [(NT, NM, LANES), HALF_TABLE, HALF_TABLE, HALF_TABLE, (NB * CH, LN), (NB * CH, LN), (2 * SUB, LN), (2 * SUB, LN, LN)],
        [
            vmem(NB, CH, NT, NN), vmem(2, CH, CH, NL), vmem(*RAW_TABLE), vmem(*RAW_TABLE), vmem(*HALF_TABLE), vmem(*HALF_TABLE),
            vmem(PAIRS, CH, LN), vmem(NN, LN), vmem(SUB, NN), vmem(PLANE, SUB, NN),
            vmem(BUFFERS, SUB, NM, LN), vmem(NN, NN), vmem(NL, LN), vmem(CH, 2 * SUB, LN),
            dma_sems(NB * PIECES), dma_sems(2), dma_sems(2), dma_sems(3, SUB), dma_sems(4, SUB), dma_sems(2, PLANE),
        ],
        cid=cid,
        in_specs=[ANY, ANY, ANY, ANY, VMEM],
        out_specs=(ANY, ANY, ANY, ANY, VMEM, VMEM, VMEM, VMEM),
        name="front",
    )(x, p_raw, q_raw, spec_w, base)


def table_loader(own, peers, tbuf, sems, y):
    def copy(src, at, g):
        return pltpu.make_async_copy(src.at[at], tbuf.at[g], sems.at[g])

    def start(g):
        at = g % SUB
        away = g // SUB != y

        @pl.when(g // SUB == y)
        def _():
            copy(own, at, g).start()

        first = 0
        for src, count in peers:
            if src is not None:
                @pl.when(away & (at >= first) & (at < first + count))
                def _(src=src, first=first):
                    copy(src, at - first, g).start()
            first += count

    def wait(g):
        copy(own, 0, g).wait()

    return start, wait


def quarters(lo, hi):
    return [(max(lo, 4 * k), min(hi, 4 * k + 4), k) for k in range(4) if max(lo, 4 * k) < min(hi, 4 * k + 4)]


def by_degree(ref, v):
    n = v.shape[0] // SUB
    t = turn(v.reshape(n, SUB, LANES))
    for b in range(NB):
        ref[:, n * b:n * (b + 1)] = t[:, :, LN * b:LN * (b + 1)]


def put_degrees(ref, parts, first, count):
    n = count * SUB
    t = jnp.concatenate([parts[:, n * b:n * (b + 1)] for b in range(NB)], axis=2)
    t = turn(t)
    for i in range(count):
        to = BLOCK * (GROUPS - first - i)
        ref[to:to + BLOCK] = t[SUB * i:SUB * (i + 1)].reshape(BLOCK, LANES)


def near_mask(first, count, pair):
    place = first + lax.broadcasted_iota(jnp.int32, (NB * count * SUB, LN), 0) % (count * SUB) // SUB
    return (place % 2 == 1) & (place < 2 * (pair + 1))


def mix_places(first, count, pair, a_ref, kern_ref, b_ref, a, b):
    rows_in = a_ref[BLOCK * first:BLOCK * (first + count)]
    n = NB * count * SUB
    by_degree(a, rows_in)
    near = near_mask(first, count, pair)

    @pl.loop(0, SUB)
    def _(l):
        al = a[l, :n]
        b[l, :n] = jnp.where(near, dot(al, kern_ref[l]), dot(al, kern_ref[SUB + l]))

    put_degrees(b_ref, b, first, count)


def mix_back_places(first, count, pair, a_ref, db_ref, kern_ref, c0_ref, da_ref, dk_ref, s_ref, a, db, da):
    at = slice(BLOCK * first, BLOCK * (first + count))
    n = count * SUB
    by_degree(a, a_ref[at])
    by_degree(db, db_ref[at])
    near = near_mask(first, count, pair)

    @pl.loop(0, SUB, unroll=UNROLL)
    def _(l):
        al, dl = a[l, :NB * n], db[l, :NB * n]
        v = jnp.where(near, dot(dl, kern_ref[l], NT_DIMS), dot(dl, kern_ref[SUB + l], NT_DIMS))
        da[l, :NB * n] = v
        product = v * al
        s_ref[1:2] += jnp.concatenate([row_sum(product[n * i:n * (i + 1)]) for i in range(NB)], axis=COL)
        if first == 0:
            for row, c0 in ((SUB, l), (0, SUB + l)):
                c0 = jnp.concatenate([c0_ref[pl.ds(c0, 1)]] * NB, axis=COL)
                s_ref[0:1] += c0 * jnp.concatenate([v[n * i + row:n * i + row + 1] for i in range(NB)], axis=COL)
        for i, part in enumerate((jnp.where(near, al, 0.0), jnp.where(near, 0.0, al))):
            g = dot(part, dl, TN_DIMS)
            low = g[CH:]
            dk_ref[i, l] += g[:CH] + jnp.concatenate([low[:, CH:], -low[:, :CH]], axis=COL)

    put_degrees(da_ref, da, first, count)


def analyze_kernel(share, with_q, *refs):
    if with_q:
        t_own, t_peer, z_hbm, q_own, kern_ref, out_ref, mix_ref, q_peer, a_deg, b_deg, qbuf, zeros, s_clear, *rest = refs
        peers = [(t_peer, SUB)]
    else:
        t_own, t_low, t_high, z_hbm, ext_ref, kern_ref, a_ref, c0_ref, mix_ref, dk_ref, a_deg, b_deg, out_ref, s_ref, da_deg, *rest = refs
        peers = [(t_low, LATE), (t_high, EARLY)]
        dk_ref[...] = jnp.zeros_like(dk_ref)
        s_ref[...] = jnp.zeros_like(s_ref)
    tbuf, zbuf, turned, part, sib, rx, ry, fx, fy, s_t, s_z, s_q, s_sib, s_x, s_y, s_fx, s_fy = rest
    count = len(SUM_ENDS)
    end = DATA if with_q else ROWS
    p = Place()
    x, c, y = p.x, p.c, p.y
    start_t, wait_t = table_loader(t_own, peers, tbuf, s_t, y)

    def load_z(g):
        return pltpu.make_async_copy(z_hbm.at[:, pl.ds(pl.multiple_of(SUB * g, SUB), SUB)], zbuf.at[g], s_z.at[g])

    def loads(lo, hi):
        @pl.loop(lo, hi)
        def _(g):
            start_t(g)
            load_z(g).start()

    loads(0, FIRST_GROUPS)
    p.greet([p.sibling, p.xn, p.yn])
    loads(FIRST_GROUPS, GROUPS)
    for d in range(PLANE):
        if not with_q:
            part[*slot_index(d), STAT:GRAD] = ext_ref[SUB * d:SUB * (d + 1)]
            part[*slot_index(d), GRAD:ROWS] = jnp.zeros((SUB, LANES), F32)

    def load_q(g):
        return pltpu.make_async_copy(q_own.at[LATE + g], qbuf.at[g], s_q.at[2, g])

    def give_q(g):
        at = used(LATE + g)
        return send(qbuf.at[g, :, at], q_peer.at[g, :, at], s_q, g, p.yn)

    def clear_q(g):
        at = unused(LATE + g)
        return pltpu.make_async_copy(zeros.at[:, at], q_peer.at[g, :, at], s_clear.at[g])

    def compute(lo, hi, k):
        @pl.loop(lo, hi)
        def _(g):
            wait_t(g)
            load_z(g).wait()
            turned[...] = turn(zbuf[g])

            at_once = AT_ONCE if k < 2 else 2

            @pl.loop(0, SUB, step=at_once)
            def _(some):
                for m in range(at_once):
                    odd, m = m % 2, some + m
                    r = dot(tbuf[g, m // 2][4 * SUB * k:, NT * odd:NT * (odd + 1)], turned[m])
                    for n in range(GROUPS - 4 * k):
                        j = 4 * k + n
                        row = sum_position(j, g) * BLOCK + SUB * m
                        if n < 4:
                            row = jnp.where(j >= g, row, ROWS)
                        xj, cj, yj = place_of_block(j)
                        part[xj, cj, yj, pl.ds(pl.multiple_of(row, SUB), SUB), :] = r[SUB * n:SUB * (n + 1)]

    def to_sibling(i):
        lo, _, hi = chunk(i, share, SUM_ENDS, end)
        return send(part.at[:, 1 - c, :, rows(lo, hi)], sib.at[:, :, rows(lo, hi)], s_sib, i, p.sibling)

    def to_x(i):
        lo, mid, _ = chunk(i, share, SUM_ENDS, end)
        return send(part.at[p.ox, c, :, rows(lo, mid)], rx.at[:, rows(lo, mid)], s_x, i, p.xn)

    def to_y(i):
        _, mid, hi = chunk(i, share, SUM_ENDS, end)
        return send(part.at[:, c, p.oy, rows(mid, hi)], ry.at[:, rows(mid, hi)], s_y, i, p.yn)

    def forward_y(i):
        lo, mid, _ = chunk(i, share, SUM_ENDS, end)
        return send(part.at[x, c, p.oy, rows(lo, mid)], fy.at[rows(lo, mid)], s_fy, i, p.yn)

    def forward_x(i):
        _, mid, hi = chunk(i, share, SUM_ENDS, end)
        return send(part.at[p.ox, c, y, rows(mid, hi)], fx.at[rows(mid, hi)], s_fx, i, p.xn)

    def chip_sum(i):
        lo, _, hi = chunk(i, share, SUM_ENDS, end)
        to_sibling(i).wait_recv()

        @pl.loop(lo, hi, step=2 * SUB)
        def _(row):
            some = pl.ds(pl.multiple_of(row, SUB), 2 * SUB)
            for a in range(2):
                for b in range(2):
                    part[a, c, b, some] += sib[a, b, some]

        to_x(i).start()
        to_y(i).start()
        if with_q and i < EARLY:
            load_q(i).wait()
            give_q(i).start()

    def add(lo, hi, *sums):
        @pl.loop(lo, hi, step=SUB)
        def _(row):
            some = pl.ds(pl.multiple_of(row, SUB), SUB)
            for to, a, b in sums:
                to[some] = a[some] + b[some]

    def half_sum(i):
        lo, mid, hi = chunk(i, share, SUM_ENDS, end)
        to_x(i).wait_recv()
        other = part.at[x, c, p.oy]
        add(lo, mid, (other, other, rx.at[p.oy]))
        forward_y(i).start()
        to_y(i).wait_recv()
        other = part.at[p.ox, c, y]
        add(mid, hi, (other, other, ry.at[p.ox]))
        forward_x(i).start()
        mine = part.at[x, c, y]
        add(lo, mid, (out_ref, mine, rx.at[y]))
        add(mid, hi, (out_ref, mine, ry.at[x]))

    def last_sum(i):
        lo, mid, hi = chunk(i, share, SUM_ENDS, end)
        forward_y(i).wait_recv()
        add(lo, mid, (out_ref, out_ref, fy))
        forward_x(i).wait_recv()
        add(mid, hi, (out_ref, out_ref, fx))

    def mixed(first, end):
        places = end - first
        if with_q:
            mix_places(first, places, p.pair, out_ref, kern_ref, mix_ref, a_deg, b_deg)
        else:
            mix_back_places(first, places, p.pair, a_ref, out_ref, kern_ref, c0_ref, mix_ref, dk_ref, s_ref, a_deg, b_deg, da_deg)

    if with_q:
        zeros[...] = jnp.zeros_like(zeros)
        for g in range(EARLY):
            load_q(g).start()
            clear_q(g).start()
    for i in range(count + LAST_LAG):
        if i < count:
            for step in quarters(max(start_of(i, SUM_ENDS) - 1, 0), SUM_ENDS[i] - 1):
                compute(*step)
            to_sibling(i).start()
        if 0 < i <= count:
            chip_sum(i - 1)
        if HALF_LAG <= i < count + HALF_LAG:
            half_sum(i - HALF_LAG)
        if i >= LAST_LAG:
            last_sum(i - LAST_LAG)
            if i - LAST_LAG in MIX_AFTER:
                n = MIX_AFTER.index(i - LAST_LAG)
                mixed(start_of(n, [SUM_ENDS[m] for m in MIX_AFTER]), SUM_ENDS[i - LAST_LAG])
    if with_q:
        mix_ref[STAT:] = jnp.zeros((ROWS - STAT, LANES), F32)
    else:
        mix_ref[STAT:GRAD] = s_ref[...]
        mix_ref[GRAD:] = out_ref[STAT:GRAD]
    for i in range(count):
        for copy in (to_sibling, to_x, to_y, forward_x, forward_y):
            copy(i).wait_send()
    if with_q:
        for g in range(EARLY):
            give_q(g).wait()
            clear_q(g).wait()


HALF_LAG, LAST_LAG = 2, 4
MOST = 8


def analyze(table, z, cid, kern, q_own=None, back=()):
    with_q = q_own is not None
    share = 13 if with_q else 8
    piece = (EARLY, *HALF_TABLE[1:])
    half = vmem(ROWS, LANES)
    pair = vmem(2, ROWS, LANES)
    degrees = vmem(SUB, NB * MOST * SUB, LN)
    if with_q:
        ins, places, outs = (q_own, kern), [ANY, VMEM], [(ROWS, LANES), (ROWS, LANES), piece]
        out_places, more = (VMEM, VMEM, ANY), [vmem(*piece), vmem(PAIRS, CH, LN), dma_sems(EARLY)]
    else:
        ext, a, c0 = back
        ins, places, outs = (ext, kern, a, c0), [VMEM] * 4, [(ROWS, LANES), (2, SUB, CH, LN)]
        out_places, more = (VMEM, VMEM), [half, vmem(SUB, LANES), degrees]
    return call(
        lambda *refs: analyze_kernel(share, with_q, *refs),
        outs,
        [degrees, degrees] + more + [
            vmem(GROUPS, *HALF_TABLE[1:]), vmem(GROUPS, NT, SUB, LANES), vmem(SUB, NT, LANES), vmem(*SLOTS, ROWS + SPARE, LANES),
            vmem(*SLOTS[1:], ROWS, LANES), pair, pair, half, half,
            dma_sems(GROUPS), dma_sems(GROUPS), dma_sems(3, EARLY),
        ] + [dma_sems(2, len(SUM_ENDS))] * 5,
        cid=cid,
        in_specs=[ANY] * len(table) + [ANY] + places,
        out_specs=out_places,
        name=f"analyze_{cid}",
    )(*table, z, *ins)


class Gather:
    def __init__(self, p, own_ref, ball, sems):
        self.p, self.own_ref, self.ball, self.sems = p, own_ref, ball, sems

    def relay(self, piece, n, to, a, b, part, src=None):
        i, lo, mid, hi, lanes = piece
        at = (rows(lo, hi), rows(lo, mid), rows(mid, hi))[part]
        here = self.ball.at[a, self.p.c, b, at, lanes]
        return send(here if src is None else src.at[at, lanes], here, self.sems[n], i, to)

    def own(self, piece, n, to):
        return self.relay(piece, n, to, self.p.x, self.p.y, 0, self.own_ref)

    def own_x(self, piece):
        return self.own(piece, 0, self.p.xn)

    def own_y(self, piece):
        return self.own(piece, 1, self.p.yn)

    def own_s(self, piece):
        return self.own(piece, 2, self.p.sibling)

    def diagonal_y(self, piece):
        return self.relay(piece, 3, self.p.yn, self.p.ox, self.p.y, 1)

    def diagonal_x(self, piece):
        return self.relay(piece, 4, self.p.xn, self.p.x, self.p.oy, 2)

    def sibling_x(self, piece):
        return self.relay(piece, 5, self.p.sibling, self.p.ox, self.p.y, 0)

    def sibling_y(self, piece):
        return self.relay(piece, 6, self.p.sibling, self.p.x, self.p.oy, 0)

    def sibling_d(self, piece):
        return self.relay(piece, 7, self.p.sibling, self.p.ox, self.p.oy, 0)

    def give(self, piece):
        for copy in (self.own_x, self.own_y, self.own_s):
            copy(piece).start()

    def pass_on(self, piece):
        self.own_x(piece).wait_recv()
        self.diagonal_y(piece).start()
        self.own_y(piece).wait_recv()
        self.diagonal_x(piece).start()
        self.sibling_x(piece).start()
        self.sibling_y(piece).start()

    def collect(self, piece):
        self.diagonal_y(piece).wait_recv()
        self.diagonal_x(piece).wait_recv()
        self.sibling_d(piece).start()

    def complete(self, piece):
        for copy in (self.own_s, self.sibling_x, self.sibling_y, self.sibling_d):
            copy(piece).wait_recv()

    def finish(self, piece):
        for copy in (
            self.own_x, self.own_y, self.own_s, self.diagonal_y, self.diagonal_x,
            self.sibling_x, self.sibling_y, self.sibling_d,
        ):
            copy(piece).wait_send()


def inverse_sums(table, ball, turned, g, k, lanes, at_once):
    @pl.loop(0, SUB, step=at_once)
    def _(some):
        for m in range(at_once):
            odd, m = m % 2, some + m
            if not odd:
                both = table(g, m // 2)
            tiles = []
            for n in range(GROUPS - 4 * k):
                j = 4 * k + n
                row = (GROUPS - sum_position(j, g)) * BLOCK + SUB * m
                if n < 4:
                    row = jnp.where(j >= g, row, ROWS)
                xj, cj, yj = place_of_block(j)
                tiles.append(ball[xj, cj, yj, pl.ds(pl.multiple_of(row, SUB), SUB), lanes])
            turned[m] = dot(both[NT * odd:NT * (odd + 1), 4 * SUB * k:], jnp.concatenate(tiles, axis=ROW))


ALL = pl.ds(0, LANES)


def synth_kernel(t_own, t_peer, own_ref, dk_ref, u_hbm, ext_ref, spec_ref, tbuf, ubuf, turned, ball, zin, kin, zg,
                 s_t, s_u, s_zk, s_zg, s_kin, s_kz, *sems):
    p = Place()
    x, c, y = p.x, p.c, p.y
    start_t, wait_t = table_loader(t_own, [(t_peer, SUB)], tbuf, s_t, y)
    count = len(GATHER_ENDS)

    def store_u(g):
        return pltpu.make_async_copy(ubuf.at[g], u_hbm.at[:, pl.ds(pl.multiple_of(SUB * g, SUB), SUB)], s_u.at[g])

    @pl.loop(0, GROUPS)
    def _(g):
        start_t(g)

    above = [{"dp": (p.z + r) % Z} for r in range(1, Z)]
    partner = [{"h": 3 - p.h}, {"h": 3 - p.h, "w": p.oy}]
    p.greet([p.sibling, p.xn, p.yn, *above, *partner])

    others = range(Z - 1)
    early = Gather(p, own_ref, ball, sems)
    late = Gather(p, ball.at[x, c, y], ball, sems)

    def piece(i):
        return i, *chunk(i, SUB, GATHER_ENDS), ALL

    def gather(i):
        return late if i == count - 1 else early

    quarter = pl.ds(2 * p.z, 2)

    def grads_z(r):
        return send(own_ref.at[GRAD:ROWS], zg.at[r], s_zg, r, above[r])

    def dk_z(r):
        return send(dk_ref.at[:, pl.ds(2 * ((p.z + 1 + r) % Z), 2)], zin.at[r], s_zk, r, above[r])

    stay = jnp.where(p.low, 0, 1)
    kept = jnp.where(p.low, p.pair, GROUPS - 1 - p.pair) % 4
    given = jnp.where(p.low, GROUPS - 1 - p.pair, p.pair) % 4

    def dk_plane(r):
        to = (p.yn, *partner)[r]
        src = kin.at[stay] if r == 0 else kin.at[1 - stay]
        return send(src, spec_ref.at[kept if r == 0 else given, quarter], s_kin, r, to)

    def dk_up(r):
        return send(spec_ref.at[:, quarter], spec_ref.at[:, quarter], s_kz, r, above[r])

    def compute(lo, hi, k):
        @pl.loop(0, hi - lo)
        def _(n):
            g = hi - 1 - n
            wait_t(g)
            inverse_sums(lambda g, i: tbuf[g, i].T, ball, turned, g, k, ALL, SUB if k > 0 else AT_ONCE)
            ubuf[g] = turn(turned[...])
            store_u(g).start()

    for r in others:
        grads_z(r).start()
        dk_z(r).start()
    for i in range(2):
        gather(i).give(piece(i))
    ball[x, c, y, 0:ROWS] = own_ref[...]
    for d in range(PLANE):
        ball[*slot_index(d), ROWS:] = jnp.zeros((SPARE, LANES), F32)
    for i in range(count + 2):
        if i < count:
            gather(i).pass_on(piece(i))
        if i == 1:
            for r in others:
                grads_z(r).wait_recv()
                ball[x, c, y, GRAD:ROWS] += zg[r]
        if i == 2:
            for r in others:
                dk_z(r).wait_recv()
            kin[...] = dk_ref[:, quarter] + zin[0] + zin[1] + zin[2]
            for r in others:
                dk_plane(r).start()
            spec_ref[kept, quarter] = kin[stay]
        if i == 3:
            for r in others:
                dk_plane(r).wait_recv()
            for r in others:
                dk_up(r).start()
        if i < count - 2:
            gather(i + 2).give(piece(i + 2))
        if 0 < i < count:
            gather(i - 1).collect(piece(i - 1))
        if i > 1:
            gather(i - 2).complete(piece(i - 2))
            for step in reversed(quarters(max(GROUPS - GATHER_ENDS[i - 2], 0), GROUPS - start_of(i - 2, GATHER_ENDS))):
                compute(*step)
        if i == count:
            gather(i - 1).collect(piece(i - 1))
    for d in range(PLANE):
        ext_ref[d] = ball[*slot_index(d), STAT:ROWS]
    for i in range(count):
        gather(i).finish(piece(i))
    for r in others:
        grads_z(r).wait_send()
        dk_z(r).wait_send()
        dk_plane(r).wait_send()
        dk_up(r).wait()

    @pl.loop(0, GROUPS)
    def _(g):
        store_u(g).wait()


def synth(table, own, cid, dk):
    quarter = (*SLOTS[1:], CH, LN)
    return call(
        synth_kernel,
        [(NT, NM, LANES), (PLANE, 2 * SUB, LANES), (4, SUB, CH, LN)],
        [
            vmem(GROUPS, *HALF_TABLE[1:]), vmem(GROUPS, NT, SUB, LANES), vmem(SUB, NT, LANES), vmem(*SLOTS, ROWS + SPARE, LANES),
            vmem(NB, *quarter), vmem(*quarter), vmem(NB, SUB, LANES), dma_sems(GROUPS), dma_sems(GROUPS),
        ] + [dma_sems(2, NB)] * 4 + [dma_sems(2, len(GATHER_ENDS))] * 8,
        cid=cid,
        in_specs=[ANY, ANY, VMEM, VMEM],
        out_specs=(ANY, VMEM, VMEM),
        name=f"synth_{cid}",
    )(*table, own, dk)


WIDE = SUB * NN
BT = 2 * SUB
PER = NT // BT
FIRST = 9 * BLOCK


def grid_stage(n, orders, x, tgt, q_ref, weights, dout, dz, grads_ref, scratch):
    g_ref, gt_ref, w1_ref, w2t_ref = weights
    some = range(BT // SUB)
    ts = [slice(SUB * k, SUB * (k + 1)) for k in some]

    def columns(t):
        return slice(NN * t, NN * (t + 1))

    def wide(v):
        return jnp.concatenate([v[t] for t in range(SUB)], axis=COL)

    line, yb, hid, act, db, dh = ([ref.at[k] for k in some] for ref in scratch)
    for k in some:
        y = to_grid(orders[k][...], g_ref[...]).reshape(SUB, CH, NN)
        r0 = turn(x[:, ts[k]] - tgt[:, ts[k]])
        line[k][...] = wide(r0 + y)
        yb[k][...] = wide(y).astype(BF16)
    for k in some:
        hid[k][...] = mxu(w1_ref[...], yb[k][...], TN_DIMS)
        for t in range(SUB):
            h = hid[k][:, columns(t)]
            h2 = h * h
            th = jnp.tanh(h * (GELU_A + (GELU_A * GELU_B) * h2))
            cdf = HALF + HALF * th
            act[k][:, columns(t)] = (h * cdf).astype(BF16)
            hid[k][:, columns(t)] = cdf + (HALF * h) * (1.0 - th * th) * (GELU_A + (3.0 * GELU_A * GELU_B) * h2)
    for k in some:
        res = line[k][...] + mxu(w2t_ref[...], act[k][...])
        first = n % PER * BT + SUB * k
        d = jnp.concatenate([jnp.full((1, NN), q_ref[first + t], F32) for t in range(SUB)], axis=COL) * res
        line[k][...] = d
        db[k][...] = d.astype(BF16)
        loss = jnp.sum((d * res).reshape(SUB, SUB, WIDE), axis=ROW)
        grads_ref[:SUB, 2 * LN:] += sum(loss[:, LN * i:LN * (i + 1)] for i in range(WIDE // LN))
        for t in range(SUB):
            dout[SUB * k + t] = line[k][:, columns(t)]
    for k in some:
        dh[k][...] = (mxu(w2t_ref[...], db[k][...], TN_DIMS) * hid[k][...]).astype(BF16)
        grads_ref[:, :LN] += mxu(yb[k][...], dh[k][...], NT_DIMS)
        grads_ref[:, LN:2 * LN] += mxu(db[k][...], act[k][...], NT_DIMS)
    for k in some:
        dy = line[k][...] + mxu(w1_ref[...], dh[k][...])
        dys = jnp.concatenate([dy[:, columns(t)] for t in range(SUB)], axis=ROW)
        dz[ts[k]] = to_orders(dys, gt_ref[...])


def forward_kernel(t_own, t_high, own_ref, x_hbm, tgt_hbm, q_ref, base_ref, w1_ref, w2t_ref, dout_hbm, dz_hbm, q_low, grads_ref,
                   tbuf, across, ubuf, turned, ball, xbuf, tgtbuf, dbuf, zbuf, g_ref, gt_ref, line, yb, hid, act, db, dh,
                   s_t, s_in, s_out, s_q, s_low, *sems):
    p = Place()
    y = p.y
    start_t, wait_local = table_loader(t_own, [(None, LATE), (t_high, EARLY)], tbuf, s_t, y)
    gather = Gather(p, own_ref, ball, sems)
    share = 2

    def lanes(s):
        return pl.ds(pl.multiple_of(LN * s, LN), LN)

    def piece(s, half):
        lo, hi = ((0, FIRST), (FIRST, DATA))[half]
        return 2 * s + half, lo, lo + (hi - lo) * share // BLOCK * SUB, hi, lanes(s)

    def each(step, s):
        for half in range(2):
            step(piece(s, half))

    def block(n):
        return n // PER, pl.ds(pl.multiple_of(n % PER * BT, BT), BT)

    def loads(n):
        b, t = block(n)
        return [
            pltpu.make_async_copy(src.at[b, :, t], dst.at[n % BUFFERS], s_in.at[i, n % BUFFERS])
            for i, (src, dst) in enumerate(((x_hbm, xbuf), (tgt_hbm, tgtbuf)))
        ]

    def stores(n):
        b, t = block(n)
        return [
            pltpu.make_async_copy(dbuf.at[n % BUFFERS], dout_hbm.at[b, t], s_out.at[0, n % BUFFERS]),
            pltpu.make_async_copy(zbuf.at[n % BUFFERS], dz_hbm.at[t, :, lanes(b)], s_out.at[1, n % BUFFERS]),
        ]

    def give_q(g):
        return send(tbuf.at[SUB * y + g], tbuf.at[SUB * y + g], s_q, g, p.yn)

    def store_low(g):
        return pltpu.make_async_copy(tbuf.at[SUB * p.oy + g], q_low.at[g], s_low.at[g])

    @pl.loop(0, GROUPS)
    def _(g):
        start_t(g)

    p.greet([p.sibling, p.xn, p.yn])
    each(gather.give, 0)
    for copy in loads(0):
        copy.start()
    ball[p.x, p.c, y, :ROWS] = own_ref[...]
    for d in range(PLANE):
        ball[*slot_index(d), ROWS:] = jnp.zeros((SPARE, LANES), F32)
    grads_ref[...] = jnp.zeros_like(grads_ref)
    gt_ref[...] = signed(base_ref, y, 2)
    g_ref[...] = gt_ref[...].T
    def across_table(g):
        for i in range(PAIRS):
            across[g, i] = tbuf[g, i].T

    @pl.loop(0, GROUPS)
    def _(g):
        at = g % SUB

        @pl.when((at >= LATE) | (g // SUB == y))
        def _():
            wait_local(g)
            across_table(g)

    each(gather.pass_on, 0)
    for g in reversed(range(LATE)):
        give_q(g).start()
    each(gather.give, 1)
    each(gather.collect, 0)

    @pl.loop(0, NB)
    def _(s):
        each(gather.complete, s)
        for k in reversed(range(4)):
            @pl.loop(0, 4)
            def _(n):
                g = 4 * k + 3 - n
                at = g % SUB

                @pl.when((s == 0) & (at < LATE) & (g // SUB != y))
                def _():
                    give_q(at).wait_recv()
                    store_low(at).start()
                    across_table(g)

                inverse_sums(lambda g, i: across[g, i], ball, turned, g, k, lanes(s), SUB)
                ubuf[:, pl.ds(pl.multiple_of(SUB * g, SUB), SUB)] = turn(turned[...])

        @pl.loop(0, PER)
        def _(i):
            n = s * PER + i
            for copy in loads(n):
                copy.wait()

            @pl.when(n + 1 < NB * PER)
            def _():
                for copy in loads(n + 1):
                    copy.start()

            @pl.when(n >= BUFFERS)
            def _():
                for copy in stores(n - BUFFERS):
                    copy.wait()

            orders = [ubuf.at[pl.ds(pl.multiple_of(i * BT + SUB * k, SUB), SUB)] for k in range(BT // SUB)]
            grid_stage(
                n, orders, xbuf.at[n % BUFFERS], tgtbuf.at[n % BUFFERS], q_ref, (g_ref, gt_ref, w1_ref, w2t_ref),
                dbuf.at[n % BUFFERS], zbuf.at[n % BUFFERS], grads_ref, (line, yb, hid, act, db, dh),
            )
            for copy in stores(n):
                copy.start()

            @pl.when((i == 0) & (s + 1 < NB))
            def _():
                each(gather.pass_on, s + 1)

            @pl.when((i == 0) & (s + 2 < NB))
            def _():
                each(gather.give, s + 2)

            @pl.when((i == 2) & (s + 1 < NB))
            def _():
                each(gather.collect, s + 1)

    for n in range(BUFFERS):
        for copy in stores(NB * PER - BUFFERS + n):
            copy.wait()

    @pl.loop(0, NB)
    def _(s):
        each(gather.finish, s)

    for g in range(LATE):
        give_q(g).wait_send()
        store_low(g).wait()


def forward(table, own, x, target, q, base, w1, w2t, cid):
    hid = 2 * CH
    grid, two = (BUFFERS, CH, BT, NN), BT // SUB
    return call(
        forward_kernel,
        [(NB, NT, CH, NN), (NT, NM, LANES), (LATE, *HALF_TABLE[1:]), (CH, LANES)],
        [
            vmem(GROUPS, *HALF_TABLE[1:]), vmem(GROUPS, *HALF_TABLE[1:]), vmem(NT, NM, LN), vmem(SUB, NT, LN), vmem(*SLOTS, ROWS + SPARE, LANES),
            vmem(*grid), vmem(*grid), vmem(BUFFERS, BT, CH, NN), vmem(BUFFERS, BT, NM, LN), vmem(NN, NN), vmem(NN, NN),
            vmem(two, CH, WIDE), vmem(two, CH, WIDE, dtype=BF16), vmem(two, hid, WIDE), vmem(two, hid, WIDE, dtype=BF16),
            vmem(two, CH, WIDE, dtype=BF16), vmem(two, hid, WIDE, dtype=BF16),
            dma_sems(GROUPS), dma_sems(2, BUFFERS), dma_sems(2, BUFFERS), dma_sems(2, LATE), dma_sems(LATE),
        ] + [dma_sems(2, 2 * NB)] * 8,
        cid=cid,
        in_specs=[ANY, ANY, VMEM, ANY, ANY, SMEM, VMEM, VMEM, VMEM],
        out_specs=(ANY, ANY, ANY, VMEM),
        name="forward",
    )(*table, own, x, target, q, base, w1, w2t)


def blocks(nt):
    return (
        pl.BlockSpec((1, CH, nt, NN), lambda b, t: (b, 0, t, 0)),
        pl.BlockSpec((1, nt, CH, NN), lambda b, t: (b, t, 0, 0)),
        pl.BlockSpec((nt, NM, LN), lambda b, t: (t, 0, b)),
    )


CHAN_SPEC = pl.BlockSpec((CH, LN), lambda b, t: (b, 0))
FINAL_T = 4 * SUB

def whole(*shape):
    return pl.BlockSpec(shape, lambda b, t: (0,) * len(shape))


def first_step():
    return (pl.program_id(0) == 0) & (pl.program_id(1) == 0)


def final_kernel(u_ref, x_ref, dout_ref, mu_ref, inv_ref, ext_ref, spec_ref, base_ref, out_ref, gspec_ref, gw1_ref, gw2t_ref, loss_ref,
                 g_ref, s0_ref, s1_ref):
    @pl.when(first_step())
    def _():
        g_ref[...] = signed(base_ref, Place().y, 1).T
        gspec_ref[0] = spec_ref[:, :, :CH]
        gspec_ref[1] = spec_ref[:, :, CH:]
        grads = ext_ref[:, SUB:].reshape(CH, LANES)
        gw1_ref[...] = grads[:, :LN]
        gw2t_ref[...] = grads[:, LN:2 * LN]
        loss = block_sum(grads[None, :SUB, 2 * LN:])[0] / TOTAL
        loss_ref[...] = loss
        sums = sum(ext_ref[n, :SUB] for n in range(PLANE)) / POINTS
        for b in range(NB):
            chans, lanes = slice(CH * b, CH * (b + 1)), slice(LN * b, LN * (b + 1))
            s0, s1 = (jnp.broadcast_to(sums[n:n + 1, lanes], (LN, LN)).T for n in range(2))
            s0_ref[chans] = s0[:CH]
            s1_ref[chans] = s1[:CH] + s1[CH:]

    chans = pl.ds(pl.multiple_of(pl.program_id(0) * CH, CH), CH)
    inv = col(inv_ref[...])
    slope = inv_ref[...] * inv_ref[...] * s1_ref[chans]

    @pl.loop(0, FINAL_T // SUB)
    def _(k):
        ts = pl.ds(pl.multiple_of(SUB * k, SUB), SUB)
        dn = to_grid(u_ref[ts], g_ref[...]).reshape(SUB, CH, NN)
        r = turn(dout_ref[0, ts] + inv * (dn - col(s0_ref[chans])))
        for c in range(CH):
            for n in range(NN // LN):
                lanes = slice(LN * n, LN * (n + 1))
                out_ref[0, c, ts, lanes] = r[c, :, lanes] - (x_ref[0, c, ts, lanes] - mu_ref[c:c + 1]) * slope[c:c + 1]


def final(u, x, dout, mu, inv, ext, spec, base):
    hid = 2 * CH
    degrees = NL // 4
    grid, lines, orders = blocks(FINAL_T)
    return call(
        final_kernel,
        [(NB, CH, NT, NN), (2, degrees, CH, CH), (CH, hid), (CH, hid), (1, 1)],
        [vmem(NN, NN), vmem(NB * CH, LN), vmem(NB * CH, LN)],
        grid=(NB, NT // FINAL_T),
        in_specs=[
            orders, grid, lines, CHAN_SPEC, CHAN_SPEC,
            whole(PLANE, 2 * SUB, LANES), whole(degrees, CH, LN), whole(4, DFT_STEP, NM),
        ],
        out_specs=(grid, whole(2, degrees, CH, CH), whole(CH, hid), whole(CH, hid), whole(1, 1)),
        name="final",
    )(u, x, dout, mu, inv, ext, spec.reshape(degrees, CH, LN), base)


def solution(mesh):
    def local_step(x, target, q, leg_fwd, leg_inv, spec_w, w1, w2):
        base = jnp.asarray(dft_tables())
        p_raw, q_raw = (jnp.swapaxes(v, 1, 2).reshape(RAW_TABLE) for v in (leg_fwd, leg_inv))
        z, p_own, p_peer, q_own, mu, inv, c0, kern = front(x, p_raw, q_raw, jnp.moveaxis(spec_w, 1, 3), base, 0)
        a, b, q_high = analyze((p_own, p_peer), z, 1, kern, q_own=q_own)
        dout, dz, q_low, grads = forward((q_own, q_high), b, x, target, q, base, w1, w2.T, 2)
        da, dk = analyze((q_own, q_low, q_high), dz, 3, kern, back=(grads, a, c0))
        du, ext, spec = synth((p_own, p_peer), da, 4, dk)
        d_field, grad_spec, gw1, gw2t, loss = final(du, x, dout, mu, inv, ext, spec, base)
        return loss.reshape(()), d_field, grad_spec, gw1, gw2t.T

    grid_spec = P("dp", None, "h", "w")
    table_spec = P("w", None, "h")
    return jax.shard_map(
        local_step,
        mesh=mesh,
        in_specs=(grid_spec, grid_spec, P("h"), table_spec, table_spec, P(), P(), P()),
        out_specs=(P(), grid_spec, P(None, "h"), P(), P()),
        check_vma=False,
    )
```

```python
import math
import numpy as np
import jax
import jax.numpy as jnp
from jax import lax
from jax.experimental import pallas as pl
from jax.experimental.pallas import tpu as pltpu
from jax.sharding import PartitionSpec as P

NORM_EPS = 1e-5
HI = lax.Precision.HIGHEST
F32 = jnp.float32
BF16 = jnp.bfloat16
MESH = pl.DeviceIdType.MESH
GELU_A = math.sqrt(2.0 / math.pi)
GELU_B = 0.044715

ROW, COL = 0, 1
NB, CH, NT, NN = 3, 64, 64, 256
NM, NL = 128, 128
DFT_STEP = 16
BUFFERS = 2
HALF = 0.5
LON, LAT, BATCH = 512, 256, 12
POINTS = LON * LAT
TOTAL = POINTS * BATCH * CH
LANES = NB * 2 * CH
SUB, LN = 8, 128
T8 = NT // SUB
GROUPS = NM // SUB
PLANE, Z = 8, 4
PAIRS = SUB // 2
FIRST_GROUPS = 3
H_OF_PAIR = (0, 0, 3, 3, 1, 1, 2, 2)
BLOCK = SUB * SUB
PLACES = GROUPS + 1
DATA = PLACES * BLOCK
STAT = DATA
GRAD = DATA + SUB
ROWS = GRAD + SUB
SPARE = BLOCK
SLOTS = (2, 2, 2)
AT_ONCE = 4
UNROLL = 2
LATE = 2
EARLY = SUB - LATE
NN_DIMS, NT_DIMS, TN_DIMS = ((1,), (0,)), ((1,), (1,)), ((0,), (0,))
SUM_ENDS = (2, 5, 8, 11, 14, 16, 17)
GATHER_ENDS = (3, 6, 9, 12, 15, 17)
MIX_AFTER = (2, 3, 4, 6)

SMEM = pl.BlockSpec(memory_space=pltpu.SMEM)
VMEM = pl.BlockSpec(memory_space=pltpu.VMEM)
ANY = pl.BlockSpec(memory_space=pl.ANY)


def dot(a, b, dims=NN_DIMS):
    return lax.dot_general(a, b, (dims, ((), ())), precision=HI, preferred_element_type=F32)


def mxu(a, b, dims=NN_DIMS):
    return lax.dot_general(a, b, (dims, ((), ())), preferred_element_type=F32)


def call(kernel, outs, scratch=(), cid=None, **kw):
    extra = {} if cid is None else {"collective_id": cid, "has_side_effects": True}
    return pl.pallas_call(
        kernel,
        out_shape=tuple(jax.ShapeDtypeStruct(s, F32) for s in outs),
        scratch_shapes=list(scratch),
        compiler_params=pltpu.CompilerParams(vmem_limit_bytes=62 << 20, **extra),
        **kw,
    )


def vmem(*shape, dtype=F32):
    return pltpu.VMEM(shape, dtype)


def dma_sems(*shape):
    return pltpu.SemaphoreType.DMA(shape)


def row_sum(v):
    return jnp.sum(v, axis=ROW, keepdims=True)


def block_sum(v):
    return jnp.sum(jnp.sum(v, axis=COL, keepdims=True), axis=COL + 1, keepdims=True)


def col(v):
    return v[:, :1]


def turn(v):
    return jnp.swapaxes(v, ROW, COL)


def rows(lo, hi):
    return pl.ds(lo, hi - lo)


def dft_tables():
    small = np.arange(DFT_STEP)[:, None] * np.arange(NM)[None]
    coarse, fine = (np.exp(-2j * np.pi * (v % LON) / LON) for v in (DFT_STEP * small, small))
    coarse = coarse / math.sqrt(LON)
    return np.stack([coarse.real, coarse.imag, fine.real, fine.imag]).astype(np.float32)


def signed(tables, half, weight):
    fine_re, fine_im = tables[2], tables[3]
    lines = []
    for n in range(DFT_STEP):
        re, im = tables[0, n:n + 1], tables[1, n:n + 1]
        lines.append(jnp.concatenate([re * fine_re - im * fine_im, re * fine_im + im * fine_re], axis=COL))
    out = jnp.concatenate(lines, axis=ROW)
    m = lax.broadcasted_iota(jnp.int32, out.shape, 1) % NM
    out = jnp.where((m % 2) * half == 1, -out, out)
    return jnp.where(m == 0, out, weight * out) if weight > 1 else out


def to_orders(lines, ft):
    z = dot(lines, ft).reshape(SUB, CH, NN)
    z = jnp.concatenate([z[:, :, :NM], z[:, :, NM:]], axis=COL)
    return jnp.swapaxes(z, 1, 2)


def to_grid(orders, ft):
    u = jnp.swapaxes(orders, 1, 2)
    u = jnp.concatenate([u[:, :CH, :], u[:, CH:, :]], axis=2).reshape(SUB * CH, NN)
    return dot(u, ft)


def place_of_block(j):
    k = min(j, GROUPS - 1 - j)
    return H_OF_PAIR[k] // 2, H_OF_PAIR[k] % 2, k % 2


def slot_index(d):
    return d // 4, d // 2 % 2, d % 2


def sum_position(j, g):
    k = min(j, GROUPS - 1 - j)
    return 2 * g + 1 if j < SUB else jnp.where(g <= k, 2 * g, k + 1 + g)


def start_of(i, ends):
    return ends[i - 1] if i > 0 else 0


def chunk(i, share, ends, last=ROWS):
    lo = start_of(i, ends) * BLOCK
    hi = ends[i] * BLOCK if ends[i] < PLACES else last
    return lo, lo + (hi - lo) * share // (2 * BLOCK) * SUB, hi


class Place:
    def __init__(self):
        self.h, self.y, self.z = lax.axis_index("h"), lax.axis_index("w"), lax.axis_index("dp")
        self.x, self.c = self.h // 2, self.h % 2
        self.slot = 2 * self.h + self.y
        self.low = self.h < 2
        self.pair = jnp.where(self.low, 4 * self.h, 14 - 4 * self.h) + self.y
        self.ox, self.oy = 1 - self.x, 1 - self.y
        self.sibling = {"h": 2 * self.x + 1 - self.c}
        self.xn = {"h": 2 * self.ox + self.c}
        self.yn = {"w": self.oy}

    def plane(self, r):
        s = (self.slot + r) % PLANE
        return {"h": s // 2, "w": s % 2}

    def greet(self, others):
        barrier = pltpu.get_barrier_semaphore()
        for other in others:
            pl.semaphore_signal(barrier, inc=1, device_id=other, device_id_type=MESH)
        pl.semaphore_wait(barrier, len(others))


def send(src, dst, sems, i, to):
    return pltpu.make_async_remote_copy(
        src_ref=src, dst_ref=dst, send_sem=sems.at[0, i], recv_sem=sems.at[1, i], device_id=to, device_id_type=MESH
    )


CB = 16
PIECES = CH // CB
RAW_TABLE = (SUB, SUB, NT, NL)
HALF_TABLE = (SUB, PAIRS, NL, LN)


def near_far(k):
    return pl.ds(pl.multiple_of(SUB * k, SUB), SUB), pl.ds(pl.multiple_of(SUB * (GROUPS - 1 - k), SUB), SUB)


def front_kernel(x_hbm, p_hbm, q_hbm, w_hbm, base_ref, z_hbm, p_own, p_peer, q_own, mu_ref, inv_ref, c0_ref, kern_ref,
                 xbuf, wbuf, pbuf, qbuf, ppack, qpack, zeros, cols, pay, sbuf, zbuf, ftbuf, turned, own, s_x, s_w, s_z, s_p, s_q, s_st):
    place = Place()
    near, far = near_far(place.pair)

    def load_x(n):
        b, part = n // PIECES, pl.ds(n % PIECES * CB, CB)
        return pltpu.make_async_copy(x_hbm.at[b, part], xbuf.at[b, part], s_x.at[n])

    def load_w(i):
        return pltpu.make_async_copy(w_hbm.at[i], wbuf.at[i], s_w.at[i])

    def load_p(g):
        return pltpu.make_async_copy(p_hbm.at[g], pbuf.at[g], s_p.at[2, g])

    def load_q(g):
        return pltpu.make_async_copy(q_hbm.at[g], qbuf.at[g], s_q.at[0, g])

    def store_p(g):
        return pltpu.make_async_copy(ppack.at[g], p_own.at[g], s_q.at[1, g])

    def store_q(g):
        return pltpu.make_async_copy(qpack.at[g], q_own.at[g], s_q.at[2, g])

    def give_p(g):
        return send(ppack.at[g, :, used(g)], p_peer.at[g, :, used(g)], s_p, g, place.yn)

    def clear_p(g):
        return pltpu.make_async_copy(zeros.at[:, unused(g)], p_peer.at[g, :, unused(g)], s_q.at[3, g])

    def pack(src, dst, g):
        for i in range(PAIRS):
            dst[g, i] = jnp.concatenate([src[g, 2 * i + n] for n in range(2)], axis=ROW).T

    @pl.loop(0, SUB)
    def _(g):
        load_p(g).start()

    @pl.loop(0, NB * PIECES)
    def _(n):
        load_x(n).start()

    for i in range(2):
        load_w(i).start()

    @pl.loop(0, SUB)
    def _(g):
        load_q(g).start()

    others = range(1, PLANE)
    place.greet([place.plane(r) for r in others])

    zeros[...] = jnp.zeros_like(zeros)
    for g in range(1, SUB):
        clear_p(g).start()

    def offer(lo, hi):
        @pl.loop(lo, hi)
        def _(g):
            load_p(g).wait()
            pack(pbuf, ppack, g)
            store_p(g).start()

        for g in range(lo, hi):
            give_p(g).start()

    offer(0, 1)
    cols[...] = jnp.zeros_like(cols)

    @pl.loop(0, NB * PIECES)
    def _(n):
        load_x(n).wait()
        v = xbuf[n // PIECES, pl.ds(n % PIECES * CB, CB)]
        mean = block_sum(v) / (NT * NN)
        diff = v - mean
        m2 = block_sum(diff * diff)
        lane = lax.broadcasted_iota(jnp.int32, (CB, 1, LN), 2)
        cols[pl.ds(pl.multiple_of(n * CB, CB), CB)] = jnp.where(lane < CH, mean, m2).reshape(CB, LN)
    wide = cols[...].T
    p1 = jnp.where(place.y == 0, row_sum(pbuf[0, 0]), 0.0)
    pay[...] = jnp.concatenate([
        *(wide[n:n + 1] for n in (0, CH)), jnp.concatenate([p1, p1], axis=COL), jnp.zeros((SUB - 3, NN), F32)
    ], axis=ROW)

    def give_stats(r):
        return send(pay, sbuf.at[place.slot], s_st, r, place.plane(r))

    for r in others:
        give_stats(r).start()
    offer(1, SUB)
    sbuf[place.slot] = pay[...]
    ftbuf[...] = signed(base_ref, place.y, 1)

    @pl.loop(0, SUB)
    def _(g):
        load_q(g).wait()
        pack(qbuf, qpack, g)
        store_q(g).start()

    for i in range(2):
        load_w(i).wait()

    @pl.loop(0, CH)
    def _(i):
        turned[...] = jnp.concatenate([wbuf[n, i] for n in range(2)], axis=ROW).T
        own[i, :SUB] = turned[near]
        own[i, SUB:] = turned[far]

    top = turn(own[...])
    kern_ref[:, :CH] = top
    kern_ref[:, CH:] = jnp.concatenate([-top[:, :, CH:], top[:, :, :CH]], axis=2)

    for r in others:
        give_stats(r).wait_recv()
    means, m2s, p1s = (jnp.concatenate([sbuf[s, n:n + 1] for s in range(PLANE)], axis=ROW) for n in range(3))
    mu = row_sum(means) / PLANE
    dev = means - mu
    var = (row_sum(m2s) + (NT * NN) * row_sum(dev * dev)) / POINTS
    c0 = math.sqrt(LON) * row_sum(p1s)
    mu_ref[...], inv_ref[...], turned[...] = (
        jnp.broadcast_to(v, (LN, NN)).T[:n] for v, n in ((mu, NB * CH), (lax.rsqrt(var + NORM_EPS), NB * CH), (c0, NL))
    )
    c0_ref[:SUB] = turned[near]
    c0_ref[SUB:] = turned[far]

    def store_z(n):
        t = pl.multiple_of(n % T8 * SUB, SUB)
        lanes = pl.multiple_of(n // T8 * LN, LN)
        return pltpu.make_async_copy(zbuf.at[n % BUFFERS], z_hbm.at[pl.ds(t, SUB), :, pl.ds(lanes, LN)], s_z.at[n % BUFFERS])

    @pl.loop(0, NB * T8)
    def _(n):
        @pl.when(n >= BUFFERS)
        def _():
            store_z(n - BUFFERS).wait()

        b = n // T8
        xt = turn(xbuf[b, :, pl.ds(pl.multiple_of(n % T8 * SUB, SUB), SUB), :])
        chans = pl.ds(pl.multiple_of(b * CH, CH), CH)
        xn = (xt - col(mu_ref[chans])) * col(inv_ref[chans])
        zbuf[n % BUFFERS] = to_orders(xn.reshape(SUB * CH, NN), ftbuf[...])
        store_z(n).start()

    for n in range(BUFFERS):
        store_z(NB * T8 - BUFFERS + n).wait()
    for r in others:
        give_stats(r).wait_send()

    @pl.loop(0, SUB)
    def _(g):
        store_p(g).wait()
        store_q(g).wait()

    for g in range(SUB):
        give_p(g).wait()
        if g > 0:
            clear_p(g).wait()


def used(g):
    return rows(SUB * g, NL)


def unused(g):
    return rows(0, SUB * g)


def front(x, p_raw, q_raw, spec_w, base, cid):
    return call(
        front_kernel,
        [(NT, NM, LANES), HALF_TABLE, HALF_TABLE, HALF_TABLE, (NB * CH, LN), (NB * CH, LN), (2 * SUB, LN), (2 * SUB, LN, LN)],
        [
            vmem(NB, CH, NT, NN), vmem(2, CH, CH, NL), vmem(*RAW_TABLE), vmem(*RAW_TABLE), vmem(*HALF_TABLE), vmem(*HALF_TABLE),
            vmem(PAIRS, CH, LN), vmem(NN, LN), vmem(SUB, NN), vmem(PLANE, SUB, NN),
            vmem(BUFFERS, SUB, NM, LN), vmem(NN, NN), vmem(NL, LN), vmem(CH, 2 * SUB, LN),
            dma_sems(NB * PIECES), dma_sems(2), dma_sems(2), dma_sems(3, SUB), dma_sems(4, SUB), dma_sems(2, PLANE),
        ],
        cid=cid,
        in_specs=[ANY, ANY, ANY, ANY, VMEM],
        out_specs=(ANY, ANY, ANY, ANY, VMEM, VMEM, VMEM, VMEM),
        name="front",
    )(x, p_raw, q_raw, spec_w, base)


def table_loader(own, peers, tbuf, sems, y):
    def copy(src, at, g):
        return pltpu.make_async_copy(src.at[at], tbuf.at[g], sems.at[g])

    def start(g):
        at = g % SUB
        away = g // SUB != y

        @pl.when(g // SUB == y)
        def _():
            copy(own, at, g).start()

        first = 0
        for src, count in peers:
            if src is not None:
                @pl.when(away & (at >= first) & (at < first + count))
                def _(src=src, first=first):
                    copy(src, at - first, g).start()
            first += count

    def wait(g):
        copy(own, 0, g).wait()

    return start, wait


def quarters(lo, hi):
    return [(max(lo, 4 * k), min(hi, 4 * k + 4), k) for k in range(4) if max(lo, 4 * k) < min(hi, 4 * k + 4)]


def by_degree(ref, v):
    n = v.shape[0] // SUB
    t = turn(v.reshape(n, SUB, LANES))
    for b in range(NB):
        ref[:, n * b:n * (b + 1)] = t[:, :, LN * b:LN * (b + 1)]


def put_degrees(ref, parts, first, count):
    n = count * SUB
    t = jnp.concatenate([parts[:, n * b:n * (b + 1)] for b in range(NB)], axis=2)
    t = turn(t)
    for i in range(count):
        to = BLOCK * (GROUPS - first - i)
        ref[to:to + BLOCK] = t[SUB * i:SUB * (i + 1)].reshape(BLOCK, LANES)


def near_mask(first, count, pair):
    place = first + lax.broadcasted_iota(jnp.int32, (NB * count * SUB, LN), 0) % (count * SUB) // SUB
    return (place % 2 == 1) & (place < 2 * (pair + 1))


def mix_places(first, count, pair, a_ref, kern_ref, b_ref, a, b):
    rows_in = a_ref[BLOCK * first:BLOCK * (first + count)]
    n = NB * count * SUB
    by_degree(a, rows_in)
    near = near_mask(first, count, pair)

    @pl.loop(0, SUB)
    def _(l):
        al = a[l, :n]
        b[l, :n] = jnp.where(near, dot(al, kern_ref[l]), dot(al, kern_ref[SUB + l]))

    put_degrees(b_ref, b, first, count)


def mix_back_places(first, count, pair, a_ref, db_ref, kern_ref, c0_ref, da_ref, dk_ref, s_ref, a, db, da):
    at = slice(BLOCK * first, BLOCK * (first + count))
    n = count * SUB
    by_degree(a, a_ref[at])
    by_degree(db, db_ref[at])
    near = near_mask(first, count, pair)

    @pl.loop(0, SUB, unroll=UNROLL)
    def _(l):
        al, dl = a[l, :NB * n], db[l, :NB * n]
        v = jnp.where(near, dot(dl, kern_ref[l], NT_DIMS), dot(dl, kern_ref[SUB + l], NT_DIMS))
        da[l, :NB * n] = v
        product = v * al
        s_ref[1:2] += jnp.concatenate([row_sum(product[n * i:n * (i + 1)]) for i in range(NB)], axis=COL)
        if first == 0:
            for row, c0 in ((SUB, l), (0, SUB + l)):
                c0 = jnp.concatenate([c0_ref[pl.ds(c0, 1)]] * NB, axis=COL)
                s_ref[0:1] += c0 * jnp.concatenate([v[n * i + row:n * i + row + 1] for i in range(NB)], axis=COL)
        for i, part in enumerate((jnp.where(near, al, 0.0), jnp.where(near, 0.0, al))):
            g = dot(part, dl, TN_DIMS)
            low = g[CH:]
            dk_ref[i, l] += g[:CH] + jnp.concatenate([low[:, CH:], -low[:, :CH]], axis=COL)

    put_degrees(da_ref, da, first, count)


def analyze_kernel(share, with_q, *refs):
    if with_q:
        t_own, t_peer, z_hbm, q_own, kern_ref, out_ref, mix_ref, q_peer, a_deg, b_deg, qbuf, zeros, s_clear, *rest = refs
        peers = [(t_peer, SUB)]
    else:
        t_own, t_low, t_high, z_hbm, ext_ref, kern_ref, a_ref, c0_ref, mix_ref, dk_ref, a_deg, b_deg, out_ref, s_ref, da_deg, *rest = refs
        peers = [(t_low, LATE), (t_high, EARLY)]
        dk_ref[...] = jnp.zeros_like(dk_ref)
        s_ref[...] = jnp.zeros_like(s_ref)
    tbuf, zbuf, turned, part, sib, rx, ry, fx, fy, s_t, s_z, s_q, s_sib, s_x, s_y, s_fx, s_fy = rest
    count = len(SUM_ENDS)
    end = DATA if with_q else ROWS
    p = Place()
    x, c, y = p.x, p.c, p.y
    start_t, wait_t = table_loader(t_own, peers, tbuf, s_t, y)

    def load_z(g):
        return pltpu.make_async_copy(z_hbm.at[:, pl.ds(pl.multiple_of(SUB * g, SUB), SUB)], zbuf.at[g], s_z.at[g])

    def loads(lo, hi):
        @pl.loop(lo, hi)
        def _(g):
            start_t(g)
            load_z(g).start()

    loads(0, FIRST_GROUPS)
    p.greet([p.sibling, p.xn, p.yn])
    loads(FIRST_GROUPS, GROUPS)
    for d in range(PLANE):
        if not with_q:
            part[*slot_index(d), STAT:GRAD] = ext_ref[SUB * d:SUB * (d + 1)]
            part[*slot_index(d), GRAD:ROWS] = jnp.zeros((SUB, LANES), F32)

    def load_q(g):
        return pltpu.make_async_copy(q_own.at[LATE + g], qbuf.at[g], s_q.at[2, g])

    def give_q(g):
        at = used(LATE + g)
        return send(qbuf.at[g, :, at], q_peer.at[g, :, at], s_q, g, p.yn)

    def clear_q(g):
        at = unused(LATE + g)
        return pltpu.make_async_copy(zeros.at[:, at], q_peer.at[g, :, at], s_clear.at[g])

    def compute(lo, hi, k):
        @pl.loop(lo, hi)
        def _(g):
            wait_t(g)
            load_z(g).wait()
            turned[...] = turn(zbuf[g])

            at_once = AT_ONCE if k < 2 else 2

            @pl.loop(0, SUB, step=at_once)
            def _(some):
                for m in range(at_once):
                    odd, m = m % 2, some + m
                    r = dot(tbuf[g, m // 2][4 * SUB * k:, NT * odd:NT * (odd + 1)], turned[m])
                    for n in range(GROUPS - 4 * k):
                        j = 4 * k + n
                        row = sum_position(j, g) * BLOCK + SUB * m
                        if n < 4:
                            row = jnp.where(j >= g, row, ROWS)
                        xj, cj, yj = place_of_block(j)
                        part[xj, cj, yj, pl.ds(pl.multiple_of(row, SUB), SUB), :] = r[SUB * n:SUB * (n + 1)]

    def to_sibling(i):
        lo, _, hi = chunk(i, share, SUM_ENDS, end)
        return send(part.at[:, 1 - c, :, rows(lo, hi)], sib.at[:, :, rows(lo, hi)], s_sib, i, p.sibling)

    def to_x(i):
        lo, mid, _ = chunk(i, share, SUM_ENDS, end)
        return send(part.at[p.ox, c, :, rows(lo, mid)], rx.at[:, rows(lo, mid)], s_x, i, p.xn)

    def to_y(i):
        _, mid, hi = chunk(i, share, SUM_ENDS, end)
        return send(part.at[:, c, p.oy, rows(mid, hi)], ry.at[:, rows(mid, hi)], s_y, i, p.yn)

    def forward_y(i):
        lo, mid, _ = chunk(i, share, SUM_ENDS, end)
        return send(part.at[x, c, p.oy, rows(lo, mid)], fy.at[rows(lo, mid)], s_fy, i, p.yn)

    def forward_x(i):
        _, mid, hi = chunk(i, share, SUM_ENDS, end)
        return send(part.at[p.ox, c, y, rows(mid, hi)], fx.at[rows(mid, hi)], s_fx, i, p.xn)

    def chip_sum(i):
        lo, _, hi = chunk(i, share, SUM_ENDS, end)
        to_sibling(i).wait_recv()

        @pl.loop(lo, hi, step=2 * SUB)
        def _(row):
            some = pl.ds(pl.multiple_of(row, SUB), 2 * SUB)
            for a in range(2):
                for b in range(2):
                    part[a, c, b, some] += sib[a, b, some]

        to_x(i).start()
        to_y(i).start()
        if with_q and i < EARLY:
            load_q(i).wait()
            give_q(i).start()

    def add(lo, hi, *sums):
        @pl.loop(lo, hi, step=SUB)
        def _(row):
            some = pl.ds(pl.multiple_of(row, SUB), SUB)
            for to, a, b in sums:
                to[some] = a[some] + b[some]

    def half_sum(i):
        lo, mid, hi = chunk(i, share, SUM_ENDS, end)
        to_x(i).wait_recv()
        other = part.at[x, c, p.oy]
        add(lo, mid, (other, other, rx.at[p.oy]))
        forward_y(i).start()
        to_y(i).wait_recv()
        other = part.at[p.ox, c, y]
        add(mid, hi, (other, other, ry.at[p.ox]))
        forward_x(i).start()
        mine = part.at[x, c, y]
        add(lo, mid, (out_ref, mine, rx.at[y]))
        add(mid, hi, (out_ref, mine, ry.at[x]))

    def last_sum(i):
        lo, mid, hi = chunk(i, share, SUM_ENDS, end)
        forward_y(i).wait_recv()
        add(lo, mid, (out_ref, out_ref, fy))
        forward_x(i).wait_recv()
        add(mid, hi, (out_ref, out_ref, fx))

    def mixed(first, end):
        places = end - first
        if with_q:
            mix_places(first, places, p.pair, out_ref, kern_ref, mix_ref, a_deg, b_deg)
        else:
            mix_back_places(first, places, p.pair, a_ref, out_ref, kern_ref, c0_ref, mix_ref, dk_ref, s_ref, a_deg, b_deg, da_deg)

    if with_q:
        zeros[...] = jnp.zeros_like(zeros)
        for g in range(EARLY):
            load_q(g).start()
            clear_q(g).start()
    for i in range(count + LAST_LAG):
        if i < count:
            for step in quarters(max(start_of(i, SUM_ENDS) - 1, 0), SUM_ENDS[i] - 1):
                compute(*step)
            to_sibling(i).start()
        if 0 < i <= count:
            chip_sum(i - 1)
        if HALF_LAG <= i < count + HALF_LAG:
            half_sum(i - HALF_LAG)
        if i >= LAST_LAG:
            last_sum(i - LAST_LAG)
            if i - LAST_LAG in MIX_AFTER:
                n = MIX_AFTER.index(i - LAST_LAG)
                mixed(start_of(n, [SUM_ENDS[m] for m in MIX_AFTER]), SUM_ENDS[i - LAST_LAG])
    if with_q:
        mix_ref[STAT:] = jnp.zeros((ROWS - STAT, LANES), F32)
    else:
        mix_ref[STAT:GRAD] = s_ref[...]
        mix_ref[GRAD:] = out_ref[STAT:GRAD]
    for i in range(count):
        for copy in (to_sibling, to_x, to_y, forward_x, forward_y):
            copy(i).wait_send()
    if with_q:
        for g in range(EARLY):
            give_q(g).wait()
            clear_q(g).wait()


HALF_LAG, LAST_LAG = 2, 4
MOST = 8


def analyze(table, z, cid, kern, q_own=None, back=()):
    with_q = q_own is not None
    share = 13 if with_q else 8
    piece = (EARLY, *HALF_TABLE[1:])
    half = vmem(ROWS, LANES)
    pair = vmem(2, ROWS, LANES)
    degrees = vmem(SUB, NB * MOST * SUB, LN)
    if with_q:
        ins, places, outs = (q_own, kern), [ANY, VMEM], [(ROWS, LANES), (ROWS, LANES), piece]
        out_places, more = (VMEM, VMEM, ANY), [vmem(*piece), vmem(PAIRS, CH, LN), dma_sems(EARLY)]
    else:
        ext, a, c0 = back
        ins, places, outs = (ext, kern, a, c0), [VMEM] * 4, [(ROWS, LANES), (2, SUB, CH, LN)]
        out_places, more = (VMEM, VMEM), [half, vmem(SUB, LANES), degrees]
    return call(
        lambda *refs: analyze_kernel(share, with_q, *refs),
        outs,
        [degrees, degrees] + more + [
            vmem(GROUPS, *HALF_TABLE[1:]), vmem(GROUPS, NT, SUB, LANES), vmem(SUB, NT, LANES), vmem(*SLOTS, ROWS + SPARE, LANES),
            vmem(*SLOTS[1:], ROWS, LANES), pair, pair, half, half,
            dma_sems(GROUPS), dma_sems(GROUPS), dma_sems(3, EARLY),
        ] + [dma_sems(2, len(SUM_ENDS))] * 5,
        cid=cid,
        in_specs=[ANY] * len(table) + [ANY] + places,
        out_specs=out_places,
        name=f"analyze_{cid}",
    )(*table, z, *ins)


class Gather:
    def __init__(self, p, own_ref, ball, sems):
        self.p, self.own_ref, self.ball, self.sems = p, own_ref, ball, sems

    def relay(self, piece, n, to, a, b, part, src=None):
        i, lo, mid, hi, lanes = piece
        at = (rows(lo, hi), rows(lo, mid), rows(mid, hi))[part]
        here = self.ball.at[a, self.p.c, b, at, lanes]
        return send(here if src is None else src.at[at, lanes], here, self.sems[n], i, to)

    def own(self, piece, n, to):
        return self.relay(piece, n, to, self.p.x, self.p.y, 0, self.own_ref)

    def own_x(self, piece):
        return self.own(piece, 0, self.p.xn)

    def own_y(self, piece):
        return self.own(piece, 1, self.p.yn)

    def own_s(self, piece):
        return self.own(piece, 2, self.p.sibling)

    def diagonal_y(self, piece):
        return self.relay(piece, 3, self.p.yn, self.p.ox, self.p.y, 1)

    def diagonal_x(self, piece):
        return self.relay(piece, 4, self.p.xn, self.p.x, self.p.oy, 2)

    def sibling_x(self, piece):
        return self.relay(piece, 5, self.p.sibling, self.p.ox, self.p.y, 0)

    def sibling_y(self, piece):
        return self.relay(piece, 6, self.p.sibling, self.p.x, self.p.oy, 0)

    def sibling_d(self, piece):
        return self.relay(piece, 7, self.p.sibling, self.p.ox, self.p.oy, 0)

    def give(self, piece):
        for copy in (self.own_x, self.own_y, self.own_s):
            copy(piece).start()

    def pass_on(self, piece):
        self.own_x(piece).wait_recv()
        self.diagonal_y(piece).start()
        self.own_y(piece).wait_recv()
        self.diagonal_x(piece).start()
        self.sibling_x(piece).start()
        self.sibling_y(piece).start()

    def collect(self, piece):
        self.diagonal_y(piece).wait_recv()
        self.diagonal_x(piece).wait_recv()
        self.sibling_d(piece).start()

    def complete(self, piece):
        for copy in (self.own_s, self.sibling_x, self.sibling_y, self.sibling_d):
            copy(piece).wait_recv()

    def finish(self, piece):
        for copy in (
            self.own_x, self.own_y, self.own_s, self.diagonal_y, self.diagonal_x,
            self.sibling_x, self.sibling_y, self.sibling_d,
        ):
            copy(piece).wait_send()


def inverse_sums(table, ball, turned, g, k, lanes, at_once):
    @pl.loop(0, SUB, step=at_once)
    def _(some):
        for m in range(at_once):
            odd, m = m % 2, some + m
            if not odd:
                both = table(g, m // 2)
            tiles = []
            for n in range(GROUPS - 4 * k):
                j = 4 * k + n
                row = (GROUPS - sum_position(j, g)) * BLOCK + SUB * m
                if n < 4:
                    row = jnp.where(j >= g, row, ROWS)
                xj, cj, yj = place_of_block(j)
                tiles.append(ball[xj, cj, yj, pl.ds(pl.multiple_of(row, SUB), SUB), lanes])
            turned[m] = dot(both[NT * odd:NT * (odd + 1), 4 * SUB * k:], jnp.concatenate(tiles, axis=ROW))


ALL = pl.ds(0, LANES)


def synth_kernel(t_own, t_peer, own_ref, dk_ref, u_hbm, ext_ref, spec_ref, tbuf, ubuf, turned, ball, zin, kin, zg,
                 s_t, s_u, s_zk, s_zg, s_kin, s_kz, *sems):
    p = Place()
    x, c, y = p.x, p.c, p.y
    start_t, wait_t = table_loader(t_own, [(t_peer, SUB)], tbuf, s_t, y)
    count = len(GATHER_ENDS)

    def store_u(g):
        return pltpu.make_async_copy(ubuf.at[g], u_hbm.at[:, pl.ds(pl.multiple_of(SUB * g, SUB), SUB)], s_u.at[g])

    @pl.loop(0, GROUPS)
    def _(g):
        start_t(g)

    above = [{"dp": (p.z + r) % Z} for r in range(1, Z)]
    partner = [{"h": 3 - p.h}, {"h": 3 - p.h, "w": p.oy}]
    p.greet([p.sibling, p.xn, p.yn, *above, *partner])

    others = range(Z - 1)
    early = Gather(p, own_ref, ball, sems)
    late = Gather(p, ball.at[x, c, y], ball, sems)

    def piece(i):
        return i, *chunk(i, SUB, GATHER_ENDS), ALL

    def gather(i):
        return late if i == count - 1 else early

    quarter = pl.ds(2 * p.z, 2)

    def grads_z(r):
        return send(own_ref.at[GRAD:ROWS], zg.at[r], s_zg, r, above[r])

    def dk_z(r):
        return send(dk_ref.at[:, pl.ds(2 * ((p.z + 1 + r) % Z), 2)], zin.at[r], s_zk, r, above[r])

    stay = jnp.where(p.low, 0, 1)
    kept = jnp.where(p.low, p.pair, GROUPS - 1 - p.pair) % 4
    given = jnp.where(p.low, GROUPS - 1 - p.pair, p.pair) % 4

    def dk_plane(r):
        to = (p.yn, *partner)[r]
        src = kin.at[stay] if r == 0 else kin.at[1 - stay]
        return send(src, spec_ref.at[kept if r == 0 else given, quarter], s_kin, r, to)

    def dk_up(r):
        return send(spec_ref.at[:, quarter], spec_ref.at[:, quarter], s_kz, r, above[r])

    def compute(lo, hi, k):
        @pl.loop(0, hi - lo)
        def _(n):
            g = hi - 1 - n
            wait_t(g)
            inverse_sums(lambda g, i: tbuf[g, i].T, ball, turned, g, k, ALL, SUB if k > 0 else AT_ONCE)
            ubuf[g] = turn(turned[...])
            store_u(g).start()

    for r in others:
        grads_z(r).start()
        dk_z(r).start()
    for i in range(2):
        gather(i).give(piece(i))
    ball[x, c, y, 0:ROWS] = own_ref[...]
    for d in range(PLANE):
        ball[*slot_index(d), ROWS:] = jnp.zeros((SPARE, LANES), F32)
    for i in range(count + 2):
        if i < count:
            gather(i).pass_on(piece(i))
        if i == 1:
            for r in others:
                grads_z(r).wait_recv()
                ball[x, c, y, GRAD:ROWS] += zg[r]
        if i == 2:
            for r in others:
                dk_z(r).wait_recv()
            kin[...] = dk_ref[:, quarter] + zin[0] + zin[1] + zin[2]
            for r in others:
                dk_plane(r).start()
            spec_ref[kept, quarter] = kin[stay]
        if i == 3:
            for r in others:
                dk_plane(r).wait_recv()
            for r in others:
                dk_up(r).start()
        if i < count - 2:
            gather(i + 2).give(piece(i + 2))
        if 0 < i < count:
            gather(i - 1).collect(piece(i - 1))
        if i > 1:
            gather(i - 2).complete(piece(i - 2))
            for step in reversed(quarters(max(GROUPS - GATHER_ENDS[i - 2], 0), GROUPS - start_of(i - 2, GATHER_ENDS))):
                compute(*step)
        if i == count:
            gather(i - 1).collect(piece(i - 1))
    for d in range(PLANE):
        ext_ref[d] = ball[*slot_index(d), STAT:ROWS]
    for i in range(count):
        gather(i).finish(piece(i))
    for r in others:
        grads_z(r).wait_send()
        dk_z(r).wait_send()
        dk_plane(r).wait_send()
        dk_up(r).wait()

    @pl.loop(0, GROUPS)
    def _(g):
        store_u(g).wait()


def synth(table, own, cid, dk):
    quarter = (*SLOTS[1:], CH, LN)
    return call(
        synth_kernel,
        [(NT, NM, LANES), (PLANE, 2 * SUB, LANES), (4, SUB, CH, LN)],
        [
            vmem(GROUPS, *HALF_TABLE[1:]), vmem(GROUPS, NT, SUB, LANES), vmem(SUB, NT, LANES), vmem(*SLOTS, ROWS + SPARE, LANES),
            vmem(NB, *quarter), vmem(*quarter), vmem(NB, SUB, LANES), dma_sems(GROUPS), dma_sems(GROUPS),
        ] + [dma_sems(2, NB)] * 4 + [dma_sems(2, len(GATHER_ENDS))] * 8,
        cid=cid,
        in_specs=[ANY, ANY, VMEM, VMEM],
        out_specs=(ANY, VMEM, VMEM),
        name=f"synth_{cid}",
    )(*table, own, dk)


WIDE = SUB * NN
BT = 2 * SUB
PER = NT // BT
FIRST = 9 * BLOCK


def grid_stage(n, orders, x, tgt, q_ref, weights, dout, dz, grads_ref, scratch):
    g_ref, gt_ref, w1_ref, w2t_ref = weights
    some = range(BT // SUB)
    ts = [slice(SUB * k, SUB * (k + 1)) for k in some]

    def columns(t):
        return slice(NN * t, NN * (t + 1))

    def wide(v):
        return jnp.concatenate([v[t] for t in range(SUB)], axis=COL)

    line, yb, hid, act, db, dh = ([ref.at[k] for k in some] for ref in scratch)
    for k in some:
        y = to_grid(orders[k][...], g_ref[...]).reshape(SUB, CH, NN)
        r0 = turn(x[:, ts[k]] - tgt[:, ts[k]])
        line[k][...] = wide(r0 + y)
        yb[k][...] = wide(y).astype(BF16)
    for k in some:
        for t in range(SUB):
            h = mxu(w1_ref[...], yb[k][:, columns(t)], TN_DIMS)
            h2 = h * h
            th = jnp.tanh(h * (GELU_A + (GELU_A * GELU_B) * h2))
            cdf = HALF + HALF * th
            act[k][:, columns(t)] = (h * cdf).astype(BF16)
            hid[k][:, columns(t)] = cdf + (HALF * h) * (1.0 - th * th) * (GELU_A + (3.0 * GELU_A * GELU_B) * h2)
    for k in some:
        res = line[k][...] + mxu(w2t_ref[...], act[k][...])
        first = n % PER * BT + SUB * k
        d = jnp.concatenate([jnp.full((1, NN), q_ref[first + t], F32) for t in range(SUB)], axis=COL) * res
        line[k][...] = d
        db[k][...] = d.astype(BF16)
        loss = jnp.sum((d * res).reshape(SUB, SUB, WIDE), axis=ROW)
        grads_ref[:SUB, 2 * LN:] += sum(loss[:, LN * i:LN * (i + 1)] for i in range(WIDE // LN))
        for t in range(SUB):
            dout[SUB * k + t] = line[k][:, columns(t)]
    for k in some:
        dh[k][...] = (mxu(w2t_ref[...], db[k][...], TN_DIMS) * hid[k][...]).astype(BF16)
        grads_ref[:, :LN] += mxu(dh[k][...], yb[k][...], NT_DIMS).T
        grads_ref[:, LN:2 * LN] += mxu(act[k][...], db[k][...], NT_DIMS).T
    for k in some:
        dy = line[k][...] + mxu(w1_ref[...], dh[k][...])
        dys = jnp.concatenate([dy[:, columns(t)] for t in range(SUB)], axis=ROW)
        dz[ts[k]] = to_orders(dys, gt_ref[...])


def forward_kernel(t_own, t_high, own_ref, x_hbm, tgt_hbm, q_ref, base_ref, w1_ref, w2t_ref, dout_hbm, dz_hbm, q_low, grads_ref,
                   tbuf, across, ubuf, turned, ball, xbuf, tgtbuf, dbuf, zbuf, g_ref, gt_ref, line, yb, hid, act, db, dh,
                   s_t, s_in, s_out, s_q, s_low, *sems):
    p = Place()
    y = p.y
    start_t, wait_local = table_loader(t_own, [(None, LATE), (t_high, EARLY)], tbuf, s_t, y)
    gather = Gather(p, own_ref, ball, sems)
    share = 2

    def lanes(s):
        return pl.ds(pl.multiple_of(LN * s, LN), LN)

    def piece(s, half):
        lo, hi = ((0, FIRST), (FIRST, DATA))[half]
        return 2 * s + half, lo, lo + (hi - lo) * share // BLOCK * SUB, hi, lanes(s)

    def each(step, s):
        for half in range(2):
            step(piece(s, half))

    def block(n):
        return n // PER, pl.ds(pl.multiple_of(n % PER * BT, BT), BT)

    def loads(n):
        b, t = block(n)
        return [
            pltpu.make_async_copy(src.at[b, :, t], dst.at[n % BUFFERS], s_in.at[i, n % BUFFERS])
            for i, (src, dst) in enumerate(((x_hbm, xbuf), (tgt_hbm, tgtbuf)))
        ]

    def stores(n):
        b, t = block(n)
        return [
            pltpu.make_async_copy(dbuf.at[n % BUFFERS], dout_hbm.at[b, t], s_out.at[0, n % BUFFERS]),
            pltpu.make_async_copy(zbuf.at[n % BUFFERS], dz_hbm.at[t, :, lanes(b)], s_out.at[1, n % BUFFERS]),
        ]

    def give_q(g):
        return send(tbuf.at[SUB * y + g], tbuf.at[SUB * y + g], s_q, g, p.yn)

    def store_low(g):
        return pltpu.make_async_copy(tbuf.at[SUB * p.oy + g], q_low.at[g], s_low.at[g])

    @pl.loop(0, GROUPS)
    def _(g):
        start_t(g)

    p.greet([p.sibling, p.xn, p.yn])
    each(gather.give, 0)
    for copy in loads(0):
        copy.start()
    ball[p.x, p.c, y, :ROWS] = own_ref[...]
    for d in range(PLANE):
        ball[*slot_index(d), ROWS:] = jnp.zeros((SPARE, LANES), F32)
    grads_ref[...] = jnp.zeros_like(grads_ref)
    gt_ref[...] = signed(base_ref, y, 2)
    g_ref[...] = gt_ref[...].T
    def across_table(g):
        for i in range(PAIRS):
            across[g, i] = tbuf[g, i].T

    @pl.loop(0, GROUPS)
    def _(g):
        at = g % SUB

        @pl.when((at >= LATE) | (g // SUB == y))
        def _():
            wait_local(g)
            across_table(g)

    each(gather.pass_on, 0)
    for g in reversed(range(LATE)):
        give_q(g).start()
    each(gather.give, 1)
    each(gather.collect, 0)

    @pl.loop(0, NB)
    def _(s):
        each(gather.complete, s)
        for k in reversed(range(4)):
            @pl.loop(0, 4)
            def _(n):
                g = 4 * k + 3 - n
                at = g % SUB

                @pl.when((s == 0) & (at < LATE) & (g // SUB != y))
                def _():
                    give_q(at).wait_recv()
                    store_low(at).start()
                    across_table(g)

                inverse_sums(lambda g, i: across[g, i], ball, turned, g, k, lanes(s), SUB)
                ubuf[:, pl.ds(pl.multiple_of(SUB * g, SUB), SUB)] = turn(turned[...])

        @pl.loop(0, PER)
        def _(i):
            n = s * PER + i
            for copy in loads(n):
                copy.wait()

            @pl.when(n + 1 < NB * PER)
            def _():
                for copy in loads(n + 1):
                    copy.start()

            @pl.when(n >= BUFFERS)
            def _():
                for copy in stores(n - BUFFERS):
                    copy.wait()

            orders = [ubuf.at[pl.ds(pl.multiple_of(i * BT + SUB * k, SUB), SUB)] for k in range(BT // SUB)]
            grid_stage(
                n, orders, xbuf.at[n % BUFFERS], tgtbuf.at[n % BUFFERS], q_ref, (g_ref, gt_ref, w1_ref, w2t_ref),
                dbuf.at[n % BUFFERS], zbuf.at[n % BUFFERS], grads_ref, (line, yb, hid, act, db, dh),
            )
            for copy in stores(n):
                copy.start()

            @pl.when((i == 0) & (s + 1 < NB))
            def _():
                each(gather.pass_on, s + 1)

            @pl.when((i == 0) & (s + 2 < NB))
            def _():
                each(gather.give, s + 2)

            @pl.when((i == 2) & (s + 1 < NB))
            def _():
                each(gather.collect, s + 1)

    for n in range(BUFFERS):
        for copy in stores(NB * PER - BUFFERS + n):
            copy.wait()

    @pl.loop(0, NB)
    def _(s):
        each(gather.finish, s)

    for g in range(LATE):
        give_q(g).wait_send()
        store_low(g).wait()


def forward(table, own, x, target, q, base, w1, w2t, cid):
    hid = 2 * CH
    grid, two = (BUFFERS, CH, BT, NN), BT // SUB
    return call(
        forward_kernel,
        [(NB, NT, CH, NN), (NT, NM, LANES), (LATE, *HALF_TABLE[1:]), (CH, LANES)],
        [
            vmem(GROUPS, *HALF_TABLE[1:]), vmem(GROUPS, *HALF_TABLE[1:]), vmem(NT, NM, LN), vmem(SUB, NT, LN), vmem(*SLOTS, ROWS + SPARE, LANES),
            vmem(*grid), vmem(*grid), vmem(BUFFERS, BT, CH, NN), vmem(BUFFERS, BT, NM, LN), vmem(NN, NN), vmem(NN, NN),
            vmem(two, CH, WIDE), vmem(two, CH, WIDE, dtype=BF16), vmem(two, hid, WIDE), vmem(two, hid, WIDE, dtype=BF16),
            vmem(two, CH, WIDE, dtype=BF16), vmem(two, hid, WIDE, dtype=BF16),
            dma_sems(GROUPS), dma_sems(2, BUFFERS), dma_sems(2, BUFFERS), dma_sems(2, LATE), dma_sems(LATE),
        ] + [dma_sems(2, 2 * NB)] * 8,
        cid=cid,
        in_specs=[ANY, ANY, VMEM, ANY, ANY, SMEM, VMEM, VMEM, VMEM],
        out_specs=(ANY, ANY, ANY, VMEM),
        name="forward",
    )(*table, own, x, target, q, base, w1, w2t)


def blocks(nt):
    return (
        pl.BlockSpec((1, CH, nt, NN), lambda b, t: (b, 0, t, 0)),
        pl.BlockSpec((1, nt, CH, NN), lambda b, t: (b, t, 0, 0)),
        pl.BlockSpec((nt, NM, LN), lambda b, t: (t, 0, b)),
    )


CHAN_SPEC = pl.BlockSpec((CH, LN), lambda b, t: (b, 0))
FINAL_T = 4 * SUB

def whole(*shape):
    return pl.BlockSpec(shape, lambda b, t: (0,) * len(shape))


def first_step():
    return (pl.program_id(0) == 0) & (pl.program_id(1) == 0)


def final_kernel(u_ref, x_ref, dout_ref, mu_ref, inv_ref, ext_ref, spec_ref, base_ref, out_ref, gspec_ref, gw1_ref, gw2t_ref, loss_ref,
                 g_ref, s0_ref, s1_ref):
    @pl.when(first_step())
    def _():
        g_ref[...] = signed(base_ref, Place().y, 1).T
        gspec_ref[0] = spec_ref[:, :, :CH]
        gspec_ref[1] = spec_ref[:, :, CH:]
        grads = ext_ref[:, SUB:].reshape(CH, LANES)
        gw1_ref[...] = grads[:, :LN]
        gw2t_ref[...] = grads[:, LN:2 * LN]
        loss = block_sum(grads[None, :SUB, 2 * LN:])[0] / TOTAL
        loss_ref[...] = loss
        sums = sum(ext_ref[n, :SUB] for n in range(PLANE)) / POINTS
        for b in range(NB):
            chans, lanes = slice(CH * b, CH * (b + 1)), slice(LN * b, LN * (b + 1))
            s0, s1 = (jnp.broadcast_to(sums[n:n + 1, lanes], (LN, LN)).T for n in range(2))
            s0_ref[chans] = s0[:CH]
            s1_ref[chans] = s1[:CH] + s1[CH:]

    chans = pl.ds(pl.multiple_of(pl.program_id(0) * CH, CH), CH)
    inv = col(inv_ref[...])
    slope = inv_ref[...] * inv_ref[...] * s1_ref[chans]

    @pl.loop(0, FINAL_T // SUB)
    def _(k):
        ts = pl.ds(pl.multiple_of(SUB * k, SUB), SUB)
        dn = to_grid(u_ref[ts], g_ref[...]).reshape(SUB, CH, NN)
        r = turn(dout_ref[0, ts] + inv * (dn - col(s0_ref[chans])))
        for c in range(CH):
            for n in range(NN // LN):
                lanes = slice(LN * n, LN * (n + 1))
                out_ref[0, c, ts, lanes] = r[c, :, lanes] - (x_ref[0, c, ts, lanes] - mu_ref[c:c + 1]) * slope[c:c + 1]


def final(u, x, dout, mu, inv, ext, spec, base):
    hid = 2 * CH
    degrees = NL // 4
    grid, lines, orders = blocks(FINAL_T)
    return call(
        final_kernel,
        [(NB, CH, NT, NN), (2, degrees, CH, CH), (CH, hid), (CH, hid), (1, 1)],
        [vmem(NN, NN), vmem(NB * CH, LN), vmem(NB * CH, LN)],
        grid=(NB, NT // FINAL_T),
        in_specs=[
            orders, grid, lines, CHAN_SPEC, CHAN_SPEC,
            whole(PLANE, 2 * SUB, LANES), whole(degrees, CH, LN), whole(4, DFT_STEP, NM),
        ],
        out_specs=(grid, whole(2, degrees, CH, CH), whole(CH, hid), whole(CH, hid), whole(1, 1)),
        name="final",
    )(u, x, dout, mu, inv, ext, spec.reshape(degrees, CH, LN), base)


def solution(mesh):
    def local_step(x, target, q, leg_fwd, leg_inv, spec_w, w1, w2):
        base = jnp.asarray(dft_tables())
        p_raw, q_raw = (jnp.swapaxes(v, 1, 2).reshape(RAW_TABLE) for v in (leg_fwd, leg_inv))
        z, p_own, p_peer, q_own, mu, inv, c0, kern = front(x, p_raw, q_raw, jnp.moveaxis(spec_w, 1, 3), base, 0)
        a, b, q_high = analyze((p_own, p_peer), z, 1, kern, q_own=q_own)
        dout, dz, q_low, grads = forward((q_own, q_high), b, x, target, q, base, w1, w2.T, 2)
        da, dk = analyze((q_own, q_low, q_high), dz, 3, kern, back=(grads, a, c0))
        du, ext, spec = synth((p_own, p_peer), da, 4, dk)
        d_field, grad_spec, gw1, gw2t, loss = final(du, x, dout, mu, inv, ext, spec, base)
        return loss.reshape(()), d_field, grad_spec, gw1, gw2t.T

    grid_spec = P("dp", None, "h", "w")
    table_spec = P("w", None, "h")
    return jax.shard_map(
        local_step,
        mesh=mesh,
        in_specs=(grid_spec, grid_spec, P("h"), table_spec, table_spec, P(), P(), P()),
        out_specs=(P(), grid_spec, P(None, "h"), P(), P()),
        check_vma=False,
    )
```
